32 devices in a mesh: box: 16 (over z, y, core), lev: 2 (over x).
Axes of the slice: x: 2, y: 2, z: 4, core: 2. Of those that a mesh axis runs over, the one named last changes fastest.
Arguments:
- fine: float32 [96, 5, 32, 1024], P(('box', 'lev')), may hold values from -12 to 12
- coarse: float32 [5, 256, 32, 128], P(None, 'box', 'lev'), may hold values from -6 to 6
- owner_map: int32 [96, 2], P(('box', 'lev')), may hold values from -2 to 7, as said below
- patch_count: int32 [32], P(('box', 'lev')), may hold values from 1 to 3, as said below
- face_mask: int32 [96, 6], P(('box', 'lev')), may hold values 0 or 1
Outputs:
- updated: float32 [5, 256, 32, 128], P(None, 'box', 'lev')
- ghost: float32 [96, 6, 5, 2048], P(('box', 'lev'))
The draws below stay inside these ranges and needn't reach their ends.
Inputs may be any that keep to these rules, and one draw needn't show every extreme that they name: `owner_map`: row p is fine patch p of device j = p // 3: column 0 is the offset k of its coarse owner, device (j + k) mod 32, one of -2, -1, 1, 2 and different for the 3 rows of one device; column 1 is a region r of that owner's block, 0 to 7. Rows of patches that are not live carry entries of the same kind and are ignored. No two live patches name the same owner and region. Device j holds live patches j * 3 to j * 3 + patch_count[j] - 1. Some device holds 3 live patches.
All inputs are finite; a program needn't handle non-finite values. No bound on the sum of `face_mask` on one device may be relied on, other than what follows from the above.
Results may differ from the reference program's by a relative error of at most 0.0003.
Values sent between devices are 32-bit elements; how exact they have to be, the bound alone decides.
A program may use at most 128 MiB of HBM per device.

```python
import jax
import jax.numpy as jnp
from jax import lax

FIELDS = 5
F = 32
FPD = 3
R = 8
CZ = 128
NBLOCKS = 32
NFINE = 96
NX = 256
NY = 32
N_LEV = 2


def owner_table(key):
    first_key = jax.random.fold_in(key, 101)
    second_key = jax.random.fold_in(key, 202)
    base_offsets = jnp.tile(jnp.arange(4, dtype=jnp.int32), (NBLOCKS, 1))
    ordering = jax.random.permutation(first_key, base_offsets, axis=1, independent=True)[:, :FPD]
    delta_table = jnp.array([-2, -1, 1, 2], dtype=jnp.int32)
    offsets = delta_table[ordering]
    region_base = jnp.tile(jnp.arange(R, dtype=jnp.int32), (NBLOCKS, 1))
    region_perm = jax.random.permutation(second_key, region_base, axis=1, independent=True)
    target = (jnp.arange(NBLOCKS, dtype=jnp.int32)[:, None] + offsets) % NBLOCKS
    regions = region_perm[target, ordering]
    return jnp.stack([offsets.reshape(-1), regions.reshape(-1)], axis=1).astype(jnp.int32)


def draw_owner_map(key, part):
    return owner_table(key)


def draw_patch_count(key, part):
    counts = jax.random.randint(jax.random.fold_in(key, 7), (NBLOCKS,), 1, FPD + 1)
    fullest = jax.random.randint(jax.random.fold_in(key, 9), (), 0, NBLOCKS)
    return jnp.where(jnp.arange(NBLOCKS) == fullest, FPD, counts).astype(jnp.int32)


def touch_ends(values, own_key, smallest, top_value):
    spot = [jax.random.randint(jax.random.fold_in(own_key, axis), (), 0, length) for axis, length in enumerate(values.shape)]
    longest = values.shape.index(max(values.shape))
    next_to = spot[:longest] + [(spot[longest] + 1) % values.shape[longest]] + spot[longest + 1:]
    return values.at[tuple(spot)].set(smallest).at[tuple(next_to)].set(top_value)


def level_of(key, shape, cuts, low, high):
    def one(dim, blocks):
        draws = jax.random.uniform(jax.random.fold_in(jax.random.fold_in(key, 6), dim), (blocks,), jnp.float32, low / len(cuts), high / len(cuts))
        return jnp.repeat(jnp.exp(draws), shape[dim] // blocks).reshape((-1,) + (1,) * (len(shape) - dim - 1))

    level = one(*cuts[0])
    for cut in cuts[1:]:
        level = level * one(*cut)
    return level


def centred(stream_key, dims, scale, reach, shards=(), kind=jnp.bfloat16):
    factor_of = level_of(stream_key, dims, shards, -0.22, 0.18) if shards else 1.0
    entries = jax.random.normal(stream_key, dims, jnp.float32) * scale * factor_of
    return jnp.minimum(jnp.maximum(entries, -reach), reach).astype(kind)


def setup_inputs(seed: int = 0) -> dict:
    streams_of = jax.random.split(jax.random.key(seed), 6)
    fine = centred(streams_of[0], (NFINE, FIELDS, F, F * F), 2.0, 12.0, ((0, 32),), jnp.float32)
    coarse = centred(streams_of[1], (FIELDS, NX, NY, CZ), 1.0, 6.0, ((1, 16), (2, 2)), jnp.float32)
    owner_map = draw_owner_map(jax.random.fold_in(streams_of[5], 71), 0)
    patch_count = draw_patch_count(jax.random.fold_in(streams_of[5], 71), 0)
    face_mask = touch_ends((jax.random.randint(streams_of[4], (NFINE, 6), 0, 4) < 3).astype(jnp.int32), jax.random.fold_in(streams_of[4], 1), 0, 1)
    return {"fine": fine, "coarse": coarse, "owner_map": owner_map, "patch_count": patch_count, "face_mask": face_mask}


def restrict(fine):
    coarse_edge = fine.shape[2] // 2
    grouped = fine.reshape(fine.shape[0], fine.shape[1], coarse_edge, 2, coarse_edge, 2, coarse_edge, 2)
    return jnp.sum(grouped, axis=(3, 5, 7)) * 0.125


def widen(values):
    return jnp.repeat(jnp.repeat(jnp.repeat(values, 2, axis=1), 2, axis=2), 2, axis=3)


def interpolate(window):
    edge_cells = window.shape[1] - 4
    fine_width = 2 * edge_cells
    centre = window[:, 1:-1, 1:-1, 1:-1]
    slope_x = 0.5 * (window[:, 2:, 1:-1, 1:-1] - window[:, :-2, 1:-1, 1:-1])
    slope_y = 0.5 * (window[:, 1:-1, 2:, 1:-1] - window[:, 1:-1, :-2, 1:-1])
    slope_z = 0.5 * (window[:, 1:-1, 1:-1, 2:] - window[:, 1:-1, 1:-1, :-2])
    offset_sign = jnp.tile(jnp.array([-0.25, 0.25], dtype=window.dtype), edge_cells + 2)
    fine_value = (widen(centre) + offset_sign[None, :, None, None] * widen(slope_x)
                  + offset_sign[None, None, :, None] * widen(slope_y)
                  + offset_sign[None, None, None, :] * widen(slope_z))
    middle = slice(2, fine_width + 2)
    lower_rim = slice(0, 2)
    upper_rim = slice(fine_width + 2, fine_width + 4)
    face_list = [fine_value[:, lower_rim, middle, middle], fine_value[:, upper_rim, middle, middle],
                 fine_value[:, middle, lower_rim, middle], fine_value[:, middle, upper_rim, middle],
                 fine_value[:, middle, middle, lower_rim], fine_value[:, middle, middle, upper_rim]]
    return jnp.stack([each_face.reshape(each_face.shape[0], -1) for each_face in face_list])


def reference(fine, coarse, owner_map, patch_count, face_mask):
    coarse_edge = F // 2
    patch_total = fine.shape[0]
    per_device = patch_total // NBLOCKS
    averaged = restrict(fine)
    patch_ids = jnp.arange(patch_total, dtype=jnp.int32)
    holder = patch_ids // per_device
    is_live = (patch_ids % per_device) < patch_count[holder]
    target = (holder + owner_map[:, 0]) % NBLOCKS
    starts = jnp.stack([jnp.zeros_like(target), (target // N_LEV) * coarse_edge,
                        (target % N_LEV) * coarse_edge, owner_map[:, 1] * coarse_edge], axis=1).astype(jnp.int32)
    extent = (coarse.shape[0], coarse_edge, coarse_edge, coarse_edge)

    def write_patch(position, field):
        corner = [starts[position, 0], starts[position, 1], starts[position, 2], starts[position, 3]]
        present = lax.dynamic_slice(field, corner, extent)
        placed = jnp.where(is_live[position], averaged[position], present)
        return lax.dynamic_update_slice(field, placed, corner)

    updated = lax.fori_loop(0, patch_total, write_patch, coarse)
    padded = jnp.pad(updated, ((0, 0), (2, 2), (2, 2), (2, 2)), mode="wrap")
    window_extent = (coarse.shape[0], coarse_edge + 4, coarse_edge + 4, coarse_edge + 4)

    def ghost_of(position):
        corner = [starts[position, 0], starts[position, 1], starts[position, 2], starts[position, 3]]
        window = lax.dynamic_slice(padded, corner, window_extent)
        keep_mask = (is_live[position] & (face_mask[position] > 0)).astype(coarse.dtype)
        return interpolate(window) * keep_mask[:, None, None]

    ghosts = lax.map(ghost_of, patch_ids)
    return updated, ghosts
```

```python
import functools

import jax
import jax.numpy as jnp
from jax import lax
from jax.experimental import pallas as pl
from jax.experimental.pallas import tpu as pltpu
from jax.sharding import PartitionSpec as P

DELTAS = (-2, -1, 1, 2)
LANES = 128
SUB = 8
F32 = jnp.float32
BF16 = jnp.bfloat16
MESH_ID = pl.DeviceIdType.MESH


def iota(shape, dim):
    return lax.broadcasted_iota(jnp.int32, shape, dim)


def split(values):
    high = values.astype(BF16)
    return high, (values - high.astype(F32)).astype(BF16)


def split_lanes(values):
    return jnp.concatenate(split(values), axis=1)


def times_transposed(left, right):
    return lax.dot_general(left, right, (((1,), (1,)), ((), ())), preferred_element_type=F32)


def both(table):
    return jnp.concatenate([table, table], axis=0)


def window_rows(edge):
    return 14 * edge, 0, 8 * edge, 2 * edge, 12 * edge, 13 * edge


def kernel(
    n_box, n_lev, slots, fields, edge,
    owner, count, fine_far, coarse_far, updated, window,
    fine, coarse, half_a, half_b, send1, recv1, halo_out, halo_in, corner_out, corner_in,
    planes, zrows, send3, recv3, place_table,
    load, s1, r1, s2, r2, s3, r3,
):
    fine_edge = 2 * edge
    block = fields * edge
    ext = edge + SUB
    rows3, z_at, d_at, zd_at, c_at, e_at = window_rows(edge)
    frows = fields * fine_edge
    cut = (fields + 1) // 2
    chunks = ((0, cut), (cut, fields))
    loads = {}
    for part, (f0, f1) in enumerate(chunks):
        for s in range(slots):
            rows = pl.ds(s * frows + f0 * fine_edge, (f1 - f0) * fine_edge)
            loads[part, s] = pltpu.make_async_copy(
                fine_far.at[rows], fine.at[rows], load.at[part * slots + s]
            )
            loads[part, s].start()
    coarse_load = pltpu.make_async_copy(coarse_far, coarse, load.at[2 * slots])
    coarse_load.start()
    n_dev = n_box * n_lev
    box = lax.axis_index("box")
    lev = lax.axis_index("lev")
    me = box * n_lev + lev

    def shifted(by):
        other = lax.rem(me + (by + n_dev), n_dev)
        return (lax.div(other, n_lev), lax.rem(other, n_lev))

    def beside(dx, dy):
        return (lax.rem(box + (dx + n_box), n_box), lax.rem(lev + (dy + n_lev), n_lev))

    sides = (beside(-1, 0), beside(1, 0), beside(0, -1), beside(0, 1))
    corners = tuple(beside(2 * cx - 1, 2 * cy - 1) for cx in (0, 1) for cy in (0, 1))
    barrier = pltpu.get_barrier_semaphore()
    peers = [shifted(delta) for delta in DELTAS] + list(sides) + list(corners)
    for peer in peers:
        pl.semaphore_signal(barrier, inc=1, device_id=peer, device_id_type=MESH_ID)

    live_count = count[0]
    chosen = [
        [(s < live_count) & (owner[0, s] == delta) for delta in DELTAS] for s in range(slots)
    ]
    weight = [[jnp.where(c, 1.0, 0.0).astype(F32) for c in row] for row in chosen]

    q = iota((fine_edge * fine_edge, edge * edge), 0)
    c = iota((fine_edge * fine_edge, edge * edge), 1)
    goal = (q // (2 * fine_edge)) * edge + (q % fine_edge) // 2
    table = jnp.where(goal == c, 0.125, 0.0).astype(BF16)
    for k in range(4):
        region = jnp.int32(-1)
        for s in range(slots):
            region = jnp.where(chosen[s][k], owner[1, s], region)
        send1[k, 0:SUB, :] = jnp.full((SUB, 2 * LANES), 1.0, F32) * region.astype(F32)
    first = []
    for part, (f0, f1) in enumerate(chunks):
        size = (f1 - f0) * edge
        for s in range(slots):
            loads[part, s].wait()
            rows = slice(s * frows + f0 * fine_edge, s * frows + f1 * fine_edge)
            high, low = split(fine[rows, :])
            got = jnp.dot(high, table, preferred_element_type=F32) + jnp.dot(
                low, table, preferred_element_type=F32
            )
            half_a[rows, :] = got[:, :LANES]
            half_b[rows, :] = got[:, LANES:]
        for h, half in enumerate((half_a, half_b)):
            averaged = []
            for s in range(slots):
                at = s * frows + f0 * fine_edge
                averaged.append(
                    half[pl.ds(at, size, stride=2), :] + half[pl.ds(at + 1, size, stride=2), :]
                )
            for k in range(4):
                total = averaged[0] * weight[0][k]
                for s in range(1, slots):
                    total = total + averaged[s] * weight[s][k]
                at = SUB + f0 * edge
                send1[k, at:at + size, h * LANES:(h + 1) * LANES] = total
        if part == 0:
            pl.semaphore_wait(barrier, len(peers))
        start = 0 if part == 0 else SUB + f0 * edge
        rows = pl.ds(start, SUB + f1 * edge - start)
        for k, delta in enumerate(DELTAS):
            copy = pltpu.make_async_remote_copy(
                src_ref=send1.at[k, rows], dst_ref=recv1.at[k, rows],
                send_sem=s1.at[part * 4 + k], recv_sem=r1.at[part * 4 + k],
                device_id=shifted(delta), device_id_type=MESH_ID,
            )
            copy.start()
            first.append(copy)

    for pair in range(4):
        row = iota((LANES, 2 * LANES), 0)
        col = iota((LANES, 2 * LANES), 1)
        hit = (row // edge == 2 * pair + col // LANES) & (row % edge == col % edge)
        place_table[pair] = both(jnp.where(hit, 1.0, 0.0).astype(BF16))
    planes[...] = jnp.zeros_like(planes)
    zrows[...] = jnp.zeros_like(zrows)
    corner_out[...] = jnp.zeros_like(corner_out)
    for k in range(4):
        send3[k * rows3 + e_at:k * rows3 + rows3, :] = jnp.zeros((edge, LANES), F32)
    coarse_load.wait()

    group = (iota((1, LANES), 1) // edge).astype(F32)
    second = []
    for part, (f0, f1) in enumerate(chunks):
        size = (f1 - f0) * edge
        for k in range(4):
            first[part * 4 + k].wait_recv()
        if part == 0:
            region_rows = [recv1[k, 0:1, 0:LANES] for k in range(4)]
            here = [group == region_rows[k] for k in range(4)]
        at = SUB + f0 * edge
        for h in range(2):
            stacked = split_lanes(jnp.concatenate(
                [recv1[k, at:at + size, h * LANES:(h + 1) * LANES] for k in range(4)], axis=0
            ))
            for pair in range(4):
                spread = jnp.dot(stacked, place_table[pair], preferred_element_type=F32)
                for odd in range(2):
                    y = h * SUB + 2 * pair + odd
                    rows = pl.ds(f0 * edge * edge + y, size, stride=edge)
                    merged = coarse[rows, :]
                    for k in range(4):
                        merged = jnp.where(
                            here[k], spread[k * size:(k + 1) * size, odd * LANES:(odd + 1) * LANES], merged
                        )
                    updated[rows, :] = merged
                    if y < 2:
                        halo_out[2, y, f0 * edge:f1 * edge, :] = merged
                    if y >= edge - 2:
                        halo_out[3, edge - 1 - y, f0 * edge:f1 * edge, :] = merged
        for f in range(f0, f1):
            for layer in range(2):
                for side, x in ((0, layer), (1, edge - 1 - layer)):
                    at = f * edge * edge + x * edge
                    halo_out[side, layer, f * edge:(f + 1) * edge, :] = updated[at:at + edge, :]
            for cx in (0, 1):
                for cy in (0, 1):
                    at = f * edge * edge + cx * (edge - 1) * edge + cy * (edge - 1)
                    corner_out[2 * cx + cy, f:f + 1, :] = updated[at:at + 1, :]
        rows = pl.ds(f0 * edge, size)
        for side in (2, 3, 0, 1):
            copy = pltpu.make_async_remote_copy(
                src_ref=halo_out.at[side, :, rows], dst_ref=halo_in.at[side ^ 1, :, rows],
                send_sem=s2.at[part * 4 + side], recv_sem=r2.at[part * 4 + (side ^ 1)],
                device_id=sides[side], device_id_type=MESH_ID,
            )
            copy.start()
            second.append(copy)
    for corner in range(4):
        copy = pltpu.make_async_remote_copy(
            src_ref=corner_out.at[corner], dst_ref=corner_in.at[3 - corner],
            send_sem=s2.at[8 + corner], recv_sem=r2.at[8 + 3 - corner],
            device_id=corners[corner], device_id_type=MESH_ID,
        )
        copy.start()
        second.append(copy)

    lane = iota((1, LANES), 1).astype(F32)

    def pick(k, place):
        t = lane - edge * region_rows[k] - place
        return jnp.where((t == 0.0) | (t == LANES) | (t == -LANES), 1.0, 0.0)

    i_side = iota((ext, 1), 0)
    place = jnp.where(i_side == edge, -1, jnp.where(i_side == edge + 1, edge, i_side)).astype(F32)
    used = i_side < edge + 2
    side_table = jnp.concatenate(
        [jnp.where(used, pick(k, place), 0.0) for k in range(4)], axis=0
    ).astype(BF16)
    side_table = jnp.concatenate([side_table, side_table], axis=1)
    i_z = iota((SUB, 1), 0)
    plus = jnp.where(i_z == 0, -1, jnp.where(i_z == 2, 0, jnp.where(i_z == 1, edge, edge + 1)))
    minus = jnp.where(i_z == 2, -2, edge - 1)
    z_list = []
    for k in range(4):
        up = pick(k, plus.astype(F32))
        down = jnp.where((i_z == 2) | (i_z == 3), pick(k, minus.astype(F32)), 0.0)
        z_list.append(jnp.where(i_z < 4, up - down, 0.0))
    z_table = jnp.concatenate(z_list, axis=0).astype(BF16)
    z_table = jnp.concatenate([z_table, z_table], axis=1)

    def z_store(v, values):
        for k in range(4):
            at = k * rows3
            level = values[k * SUB:k * SUB + 2, :]
            if v < edge:
                send3[pl.ds(at + z_at + v, 2, stride=edge), :] = level
                send3[pl.ds(at + zd_at + v, 2, stride=edge), :] = values[k * SUB + 2:k * SUB + 4, :]
            else:
                send3[pl.ds(at + e_at + 8 + v - edge, 2, stride=2), :] = level

    for v in range(edge):
        for f in range(fields):
            zrows[pl.ds(v * LANES + f, edge, stride=SUB), :] = updated[
                pl.ds(f * edge * edge + v, edge, stride=edge), :
            ]
    for v in range(0, edge, 2):
        got = times_transposed(z_table, split_lanes(zrows[v * LANES:(v + 2) * LANES, :]))
        z_store(v, got[:, :LANES])
        z_store(v + 1, got[:, LANES:])

    third = []

    def send_back(part):
        start, size = ((0, 4 * edge), (4 * edge, rows3 - 4 * edge))[part]
        for k, delta in enumerate(DELTAS):
            copy = pltpu.make_async_remote_copy(
                src_ref=send3.at[pl.ds(k * rows3 + start, size)], dst_ref=recv3.at[k, pl.ds(start, size)],
                send_sem=s3.at[part * 4 + k], recv_sem=r3.at[part * 4 + k],
                device_id=shifted(-delta), device_id_type=MESH_ID,
            )
            copy.start()
            third.append(copy)

    send_back(0)
    for copy in second:
        copy.wait_recv()

    for side in range(4):
        near = 1.0 if side % 2 == 0 else -1.0
        for f in range(fields):
            a = f * edge
            adjacent = halo_in[side, 0, a:a + edge, :]
            far = halo_in[side, 1, a:a + edge, :]
            own = halo_out[side, 0, a:a + edge, :]
            planes[pl.ds(2 * side * LANES + f, edge, stride=SUB), :] = adjacent
            planes[pl.ds((2 * side + 1) * LANES + f, edge, stride=SUB), :] = (own - far) * near
    for corner in range(4):
        planes[8 * LANES + corner * SUB:8 * LANES + (corner + 1) * SUB, :] = corner_in[corner]
    for side in range(4):
        both_planes = split_lanes(planes[2 * side * LANES:(2 * side + 2) * LANES, :])
        got = times_transposed(side_table, both_planes)
        for k in range(4):
            at = k * rows3
            send3[at + (4 + side) * edge:at + (5 + side) * edge, :] = got[k * ext:k * ext + edge, :LANES]
            send3[at + e_at + 2 * side:at + e_at + 2 * side + 2, :] = (
                got[k * ext + edge:k * ext + edge + 2, :LANES]
            )
            to = at + d_at + side * edge
            send3[to:to + edge, :] = got[k * ext:k * ext + edge, LANES:]
        if side >= 2:
            z_store(edge + side - 2, times_transposed(z_table, both_planes[:LANES, :]))
    got = times_transposed(side_table, split_lanes(planes[8 * LANES:9 * LANES, :]))
    for k in range(4):
        send3[k * rows3 + c_at:k * rows3 + c_at + edge, :] = got[k * ext:k * ext + edge, :]

    send_back(1)
    for copy in third:
        copy.wait_recv()

    for s in range(slots):
        total = recv3[0] * weight[s][0]
        for k in range(1, 4):
            total = total + recv3[k] * weight[s][k]
        window[s] = total

    for copy in first + second + third:
        copy.wait_send()


def ghost_kernel(
    slots, fields, edge, count, mask, window, updated_in, updated_out, ghost_out,
    ghost, pass_sem, out_sem,
):
    fine_edge = 2 * edge
    rows3, z_at, d_at, zd_at, c_at, e_at = window_rows(edge)
    live_count = count[0]
    outs = [pltpu.make_async_copy(updated_in, updated_out, pass_sem.at[0])]
    outs[0].start()

    def line_tables(cell, odd, pair):
        i = iota((2 * edge, LANES), 0)
        at = jnp.where(i == edge + pair, -1, jnp.where(i == edge + pair + 1, edge, i))
        at = jnp.where((i < edge) | (at != i), at, -9)
        plain = jnp.where(at == cell, 1.0, 0.0)
        sign = jnp.where(odd, 0.125, -0.125)
        slope = jnp.where(at == cell + 1, sign, jnp.where(at == cell - 1, -sign, 0.0))
        full = both(jnp.concatenate([plain, plain + slope], axis=1)).astype(BF16)
        return full, both((plain[:edge] * 0.125)).astype(BF16)

    l2 = iota((2 * edge, LANES), 1)
    side_tables = []
    for side in range(4):
        full, w_diff = line_tables((l2 % fine_edge) // 2, l2 % 2 == 1, 2 * side)
        side_tables.append(full)
    z_tables = []
    for z in range(2):
        full, v_diff = line_tables(
            (l2 % (2 * fine_edge)) // 4, (l2 // 2) % 2 == 1, 8 + 2 * z
        )
        z_tables.append(full)
    row = iota((LANES, LANES), 0)
    col = iota((LANES, LANES), 1)
    line_v = both(jnp.where(row // SUB == (col % (2 * fine_edge)) // 4, 1.0, 0.0).astype(BF16))

    lanes8 = iota((SUB, LANES), 1)
    low_half = lanes8 < 2 * fine_edge
    half_sign = jnp.where(low_half, -0.125, 0.125)
    quarter = (lanes8 // fine_edge) % 2 == 1
    quarter_slope = jnp.where(quarter, 0.125, -0.125)
    quarter_sign = jnp.where(quarter, 1.0, -1.0)
    last_sign = jnp.where(lanes8 % 2 == 1, 1.0, -1.0)
    own_field = lanes8 % SUB == iota((SUB, LANES), 0)

    def spread_plane(s, at, table, ends=None):
        total = window[s, at:at + edge, :]
        if ends is not None:
            total = jnp.concatenate([total, ends], axis=0)
        high = total.astype(BF16).astype(F32)
        tall = jnp.concatenate([high, total - high], axis=0)
        return jnp.dot(tall.T.astype(BF16), table, preferred_element_type=F32)

    def cut(values, m):
        return values[m * SUB:(m + 1) * SUB, :]

    for s in range(slots):
        keep = [
            jnp.where((s < live_count) & (mask[s, face] > 0), 1.0, 0.0).astype(F32)
            for face in range(6)
        ]
        ends_all = window[s, e_at:e_at + edge, :]
        lines = spread_plane(s, c_at, w_diff)
        line = [cut(lines, corner) * 8.0 for corner in range(4)]
        edges = []
        for side in range(4):
            centre = spread_plane(s, (4 + side) * edge, side_tables[side], ends_all)
            diff = spread_plane(s, d_at + side * edge, w_diff)
            plain = [cut(centre, m)[:, :LANES] for m in range(edge)]
            full = [cut(centre, m)[:, LANES:] for m in range(edge)]
            high_side = side % 2
            if side < 2:
                edges.append(ends_all[2 * side:2 * side + 1, :])
                edges.append(ends_all[2 * side + 1:2 * side + 2, :])
                around = [line[2 * high_side]] + plain + [line[2 * high_side + 1]]
                for t in range(edge // 2):
                    base = jnp.where(low_half, full[2 * t], full[2 * t + 1])
                    slope = jnp.where(
                        low_half, around[2 * t + 2] - around[2 * t], around[2 * t + 3] - around[2 * t + 1]
                    )
                    across = jnp.where(low_half, cut(diff, 2 * t), cut(diff, 2 * t + 1))
                    base = base + slope * quarter_slope
                    at = t * LANES
                    ghost[s, :, side, at:at + LANES] = ((base - across) * keep[side])[:fields]
                    at = at + fine_edge * fine_edge
                    ghost[s, :, side, at:at + LANES] = ((base + across) * keep[side])[:fields]
            else:
                around = [line[high_side]] + plain + [line[2 + high_side]]
                for t in range(edge):
                    value = (
                        full[t] + (around[t + 2] - around[t]) * half_sign + cut(diff, t) * quarter_sign
                    )
                    ghost[s, :, side, t * LANES:(t + 1) * LANES] = (value * keep[side])[:fields]
        tall = jnp.concatenate([jnp.where(own_field, e, 0.0) for e in edges], axis=0)
        ends = jnp.dot(split_lanes(tall), line_v, preferred_element_type=F32)
        for z in range(2):
            centre = spread_plane(s, z_at + z * edge, z_tables[z], ends_all)
            diff = spread_plane(s, zd_at + z * edge, v_diff)
            around = (
                [cut(ends, z)] + [cut(centre, m)[:, :LANES] for m in range(edge)] + [cut(ends, 2 + z)]
            )
            for t in range(edge):
                value = (
                    cut(centre, t)[:, LANES:]
                    + (around[t + 2] - around[t]) * half_sign
                    + cut(diff, t) * last_sign
                )
                ghost[s, :, 4 + z, t * LANES:(t + 1) * LANES] = (value * keep[4 + z])[:fields]
        outs.append(pltpu.make_async_copy(ghost.at[s], ghost_out.at[s], out_sem.at[s]))
        outs[-1].start()
    for copy in outs:
        copy.wait()


def body(n_box, n_lev, fine, coarse, owner_map, patch_count, face_mask):
    slots, fields, fine_edge, _ = fine.shape
    edge = fine_edge // 2
    block = fields * edge
    rows3 = window_rows(edge)[0]
    vmem = pl.BlockSpec(memory_space=pltpu.VMEM)
    smem = pl.BlockSpec(memory_space=pltpu.SMEM)
    hbm = pl.BlockSpec(memory_space=pltpu.HBM)
    flat = jax.ShapeDtypeStruct((block * edge, LANES), F32)
    updated, window = pl.pallas_call(
        functools.partial(kernel, n_box, n_lev, slots, fields, edge),
        out_shape=(flat, jax.ShapeDtypeStruct((slots, rows3, LANES), F32)),
        in_specs=[smem, smem, hbm, hbm],
        out_specs=(vmem, vmem),
        scratch_shapes=[
            pltpu.VMEM((slots * fields * fine_edge, fine_edge * fine_edge), F32),
            pltpu.VMEM((block * edge, LANES), F32),
            pltpu.VMEM((slots * fields * fine_edge, LANES), F32),
            pltpu.VMEM((slots * fields * fine_edge, LANES), F32),
            pltpu.VMEM((4, block + SUB, 2 * LANES), F32),
            pltpu.VMEM((4, block + SUB, 2 * LANES), F32),
            pltpu.VMEM((4, 2, block, LANES), F32),
            pltpu.VMEM((4, 2, block, LANES), F32),
            pltpu.VMEM((4, SUB, LANES), F32),
            pltpu.VMEM((4, SUB, LANES), F32),
            pltpu.VMEM((9 * LANES, LANES), F32),
            pltpu.VMEM((edge * LANES, LANES), F32),
            pltpu.VMEM((4 * rows3, LANES), F32),
            pltpu.VMEM((4, rows3, LANES), F32),
            pltpu.VMEM((4, 2 * LANES, 2 * LANES), BF16),
            pltpu.SemaphoreType.DMA((2 * slots + 1,)),
            pltpu.SemaphoreType.DMA((8,)),
            pltpu.SemaphoreType.DMA((8,)),
            pltpu.SemaphoreType.DMA((12,)),
            pltpu.SemaphoreType.DMA((12,)),
            pltpu.SemaphoreType.DMA((8,)),
            pltpu.SemaphoreType.DMA((8,)),
        ],
        compiler_params=pltpu.CompilerParams(collective_id=0, has_side_effects=True, vmem_limit_bytes=55000000),
    )(
        owner_map.T, patch_count,
        fine.reshape(slots * fields * fine_edge, fine_edge * fine_edge),
        coarse.reshape(block * edge, LANES),
    )
    ghost_shape = (slots, fields, 6, 2 * fine_edge * fine_edge)
    updated, ghost = pl.pallas_call(
        functools.partial(ghost_kernel, slots, fields, edge),
        out_shape=(flat, jax.ShapeDtypeStruct(ghost_shape, F32)),
        in_specs=[smem, smem, vmem, vmem],
        out_specs=(hbm, hbm),
        scratch_shapes=[
            pltpu.VMEM(ghost_shape, F32),
            pltpu.SemaphoreType.DMA((1,)),
            pltpu.SemaphoreType.DMA((slots,)),
        ],
        compiler_params=pltpu.CompilerParams(vmem_limit_bytes=16777216),
    )(patch_count, face_mask, window, updated)
    return updated.reshape(coarse.shape), ghost.transpose(0, 2, 1, 3)


def solution(mesh):
    return jax.shard_map(
        functools.partial(body, mesh.shape["box"], mesh.shape["lev"]),
        mesh=mesh,
        in_specs=(
            P(("box", "lev"), None, None, None),
            P(None, "box", "lev", None),
            P(("box", "lev"), None),
            P(("box", "lev")),
            P(("box", "lev"), None),
        ),
        out_specs=(P(None, "box", "lev", None), P(("box", "lev"), None, None, None)),
        check_vma=False,
    )
```

```python
import functools

import jax
import jax.numpy as jnp
from jax import lax
from jax.experimental import pallas as pl
from jax.experimental.pallas import tpu as pltpu
from jax.sharding import PartitionSpec as P

DELTAS = (-2, -1, 1, 2)
LANES = 128
SUB = 8
F32 = jnp.float32
BF16 = jnp.bfloat16
MESH_ID = pl.DeviceIdType.MESH


def iota(shape, dim):
    return lax.broadcasted_iota(jnp.int32, shape, dim)


def split(values):
    high = values.astype(BF16)
    return high, (values - high.astype(F32)).astype(BF16)


def split_lanes(values):
    return jnp.concatenate(split(values), axis=1)


def times_transposed(left, right):
    return lax.dot_general(left, right, (((1,), (1,)), ((), ())), preferred_element_type=F32)


def both(table):
    return jnp.concatenate([table, table], axis=0)


def transposed_groups(arrays, edge):
    out = list(arrays)
    group = iota(out[0].shape, 1) // edge
    for bit in (4, 2, 1):
        low = (group // bit) % 2 == 0
        for i in range(8):
            if i & bit == 0:
                a, b = out[i], out[i + bit]
                out[i] = jnp.where(low, a, pltpu.roll(b, bit * edge, 1))
                out[i + bit] = jnp.where(low, pltpu.roll(a, LANES - bit * edge, 1), b)
    return out


class Layout:
    def __init__(self, fields, edge):
        self.ends = 4 * fields
        self.side = 4 * fields + 4
        self.z = 4 * self.side
        self.corner = self.z + 8 * fields
        self.own = self.corner + 8
        self.rows = self.own + 12 * fields + 8
        self.rows = self.rows + (-self.rows) % SUB


DIRECTIONS = ((-1, 0), (1, 0), (0, -1), (0, 1), (-1, -1), (-1, 1), (1, -1), (1, 1))


def opposite(d):
    return d ^ 1 if d < 4 else 11 - d


def relations(n_box, n_lev):
    n_dev = n_box * n_lev
    offsets, same = set(), {}
    for me in range(n_dev):
        box, lev = divmod(me, n_lev)

        def add(other):
            db, dl = (other // n_lev - box) % n_box, (other % n_lev - lev) % n_lev
            offsets.add((db, dl))
            offsets.add((-db % n_box, -dl % n_lev))

        for delta in DELTAS:
            add((me + delta) % n_dev)
        for d, (dx, dy) in enumerate(DIRECTIONS):
            owner = ((box - dx) % n_box) * n_lev + (lev - dy) % n_lev
            add(owner)
            for k, delta in enumerate(DELTAS):
                target = (owner - delta) % n_dev
                add(target)
                same.setdefault((d, k), set()).add(target == me)
    offsets.discard((0, 0))
    return sorted(offsets), same


def kernel(
    n_box, n_lev, slots, fields, edge,
    owner, count, fine_far, coarse_far, updated, window,
    fine, coarse, half_a, half_b, avg, own_got, send1, recv1, region_out, region_in, near_in,
    upd, corner_lines, corner_region, side_out, side_in, z_out, z_in, corner_out, corner_in,
    place_table,
    load, s1, r1, sh, rh, s3, r3,
):
    fine_edge = 2 * edge
    block = fields * edge
    plane = edge * edge
    lay = Layout(fields, edge)
    frows = fields * fine_edge
    cut = (fields + 1) // 2
    chunks = ((0, cut), (cut, fields))
    loads = {}
    for part, (f0, f1) in enumerate(chunks):
        for s in range(slots):
            rows = pl.ds(s * frows + f0 * fine_edge, (f1 - f0) * fine_edge)
            loads[part, s] = pltpu.make_async_copy(
                fine_far.at[rows], fine.at[rows], load.at[part * slots + s]
            )
            loads[part, s].start()
    coarse_load = pltpu.make_async_copy(coarse_far, coarse, load.at[2 * slots])
    coarse_load.start()
    n_dev = n_box * n_lev
    offsets, same = relations(n_box, n_lev)
    box = lax.axis_index("box")
    lev = lax.axis_index("lev")
    me = box * n_lev + lev

    def at(linear):
        return (lax.div(linear, n_lev), lax.rem(linear, n_lev))

    def shifted(by):
        return at(lax.rem(me + (by + n_dev), n_dev))

    def beside(dx, dy):
        return (lax.rem(box + (dx + n_box), n_box), lax.rem(lev + (dy + n_lev), n_lev))

    around = [beside(dx, dy) for dx, dy in DIRECTIONS]
    barrier = pltpu.get_barrier_semaphore()
    for db, dl in offsets:
        pl.semaphore_signal(barrier, inc=1, device_id=beside(db, dl), device_id_type=MESH_ID)

    live_count = count[0]
    chosen = [
        [(s < live_count) & (owner[0, s] == delta) for delta in DELTAS] for s in range(slots)
    ]
    weight = [[jnp.where(c, 1.0, 0.0).astype(F32) for c in row] for row in chosen]
    for k in range(4):
        region = jnp.int32(-1)
        for s in range(slots):
            region = jnp.where(chosen[s][k], owner[1, s], region)
        region_out[k] = jnp.full((1, LANES), 1.0, F32) * region.astype(F32)

    q = iota((fine_edge * fine_edge, plane), 0)
    c = iota((fine_edge * fine_edge, plane), 1)
    goal = (q // (2 * fine_edge)) * edge + (q % fine_edge) // 2
    table = jnp.where(goal == c, 0.125, 0.0).astype(BF16)
    first, told = [], []
    order = (1, 2, 0, 3)
    for part, (f0, f1) in enumerate(chunks):
        size = (f1 - f0) * edge
        for s in range(slots):
            loads[part, s].wait()
            rows = slice(s * frows + f0 * fine_edge, s * frows + f1 * fine_edge)
            high, low = split(fine[rows, :])
            got = jnp.dot(high, table, preferred_element_type=F32) + jnp.dot(
                low, table, preferred_element_type=F32
            )
            half_a[rows, :] = got[:, :LANES]
            half_b[rows, :] = got[:, LANES:]
        to = f0 * edge
        for h, half in enumerate((half_a, half_b)):
            averaged = []
            for s in range(slots):
                start = s * frows + f0 * fine_edge
                mean = half[pl.ds(start, size, stride=2), :] + half[pl.ds(start + 1, size, stride=2), :]
                start = (h * slots + s) * block + to
                avg[start:start + size, :] = mean
                averaged.append(mean)
            for k in range(4):
                total = averaged[0] * weight[0][k]
                for s in range(1, slots):
                    total = total + averaged[s] * weight[s][k]
                send1[k, to:to + size, h * LANES:(h + 1) * LANES] = total
        if part == 0:
            pl.semaphore_wait(barrier, len(offsets))
            for k in order:
                copy = pltpu.make_async_remote_copy(
                    src_ref=region_out.at[k], dst_ref=region_in.at[k],
                    send_sem=sh.at[k], recv_sem=rh.at[k],
                    device_id=shifted(DELTAS[k]), device_id_type=MESH_ID,
                )
                copy.start()
                told.append(copy)
        for k in order:
            copy = pltpu.make_async_remote_copy(
                src_ref=send1.at[k, pl.ds(to, size)], dst_ref=recv1.at[k, pl.ds(to, size)],
                send_sem=s1.at[part * 4 + k], recv_sem=r1.at[part * 4 + k],
                device_id=shifted(DELTAS[k]), device_id_type=MESH_ID,
            )
            copy.start()
            first.append(copy)

    for copy in told:
        copy.wait_recv()
    passed = []
    for d in range(8):
        copy = pltpu.make_async_remote_copy(
            src_ref=region_in, dst_ref=near_in.at[opposite(d)],
            send_sem=sh.at[4 + d], recv_sem=rh.at[4 + opposite(d)],
            device_id=around[d], device_id_type=MESH_ID,
        )
        copy.start()
        passed.append(copy)

    for pair in range(4):
        row = iota((LANES, 2 * LANES), 0)
        col = iota((LANES, 2 * LANES), 1)
        hit = (row // edge == 2 * pair + col // LANES) & (row % edge == col % edge)
        place_table[pair] = both(jnp.where(hit, 1.0, 0.0).astype(BF16))

    row = iota((plane, 4 * LANES), 0)
    col = iota((plane, 4 * LANES), 1)
    kind = col // LANES
    inner = col % edge
    fixed = jnp.where(kind % 2 == 0, 0, edge - 1)
    hit = jnp.where(kind < 2, fixed * edge + inner, inner * edge + fixed) == row
    own_table = jnp.where(hit, 1.0, 0.0).astype(BF16)
    high, low = split(jnp.concatenate(
        [avg[:slots * block, :], avg[slots * block:, :]], axis=1
    ))
    got = jnp.dot(high, own_table, preferred_element_type=F32) + jnp.dot(
        low, own_table, preferred_element_type=F32
    )
    for kind in range(4):
        own_got[kind * slots * block:(kind + 1) * slots * block, :] = got[
            :, kind * LANES:(kind + 1) * LANES
        ]
    group_f = iota((fields, LANES), 1) // edge
    for s in range(slots):
        for h in range(2):
            for side in range(2):
                start = (h * slots + s) * block + side * (edge - 1)
                to = lay.own + (2 * side + h) * fields
                window[s, to:to + fields, :] = avg[pl.ds(start, fields, stride=edge), :]
            for kind in range(4):
                total = jnp.zeros((fields, LANES), F32)
                for i in range(8):
                    start = (kind * slots + s) * block + h * 8 + i
                    part = own_got[pl.ds(start, fields, stride=edge), :]
                    total = jnp.where(group_f == i, part, total)
                to = lay.own + (2 * (2 + kind) + h) * fields
                window[s, to:to + fields, :] = total

    corner_lines[...] = jnp.zeros_like(corner_lines)
    coarse_load.wait()
    for copy in passed:
        copy.wait_recv()

    lane = iota((1, LANES), 1).astype(F32)
    here_rows = [region_in[k] for k in range(4)]

    def pick(region, place):
        t = lane - edge * region - place
        return jnp.where((t == 0.0) | (t == LANES) | (t == -LANES), 1.0, 0.0)

    z_rows = []
    for depth in range(2):
        for k in range(4):
            for place in (-1 - depth, edge + depth):
                z_rows.append(pick(here_rows[k], place))
    for d in (1, 0):
        for place in (-1, edge):
            for k in range(4):
                z_rows.append(pick(near_in[d, k], place))
    z_table = jnp.concatenate(z_rows, axis=0).astype(BF16)
    z_table = jnp.concatenate([z_table, z_table], axis=1)
    for corner in range(4):
        for k in range(4):
            corner_region[k, corner:corner + 1, :] = near_in[opposite(4 + corner), k]

    group = (iota((1, LANES), 1) // edge).astype(F32)
    here = [group == region for region in here_rows]
    group8 = iota((SUB, LANES), 1) // edge
    end_lines = [jnp.zeros((SUB, LANES), F32) for _ in range(2)]
    for part, (f0, f1) in enumerate(chunks):
        size = (f1 - f0) * edge
        for k in range(4):
            first[part * 4 + k].wait_recv()
        to = f0 * edge
        for h in range(2):
            stacked = split_lanes(jnp.concatenate(
                [recv1[k, to:to + size, h * LANES:(h + 1) * LANES] for k in range(4)], axis=0
            ))
            for pair in range(4):
                spread = jnp.dot(stacked, place_table[pair], preferred_element_type=F32)
                for odd in range(2):
                    y = h * SUB + 2 * pair + odd
                    rows = pl.ds(f0 * plane + y, size, stride=edge)
                    merged = coarse[rows, :]
                    for k in range(4):
                        merged = jnp.where(
                            here[k], spread[k * size:(k + 1) * size, odd * LANES:(odd + 1) * LANES], merged
                        )
                    upd[rows, :] = merged
                    updated[rows, :] = merged
        for f in range(f0, f1):
            got = times_transposed(z_table, split_lanes(upd[f * plane:(f + 1) * plane, :]))
            for depth in range(2):
                for h in range(2):
                    z_out[pl.ds((2 * depth + h) * fields + f, 8, stride=4 * fields), :] = got[
                        depth * 8:(depth + 1) * 8, h * LANES:(h + 1) * LANES
                    ]
            high_end = got[16:24, LANES:]
            if f:
                high_end = pltpu.roll(high_end, LANES - f * edge, 1)
            low_end = pltpu.roll(got[24:32, :LANES], LANES - (f + 1) * edge, 1)
            end_lines[0] = jnp.where(group8 == 7 - f, high_end, end_lines[0])
            end_lines[1] = jnp.where(group8 == 7 - f, low_end, end_lines[1])

    third = []

    def send(src, dst, slot, d, k, target):
        kinds = {False} if d is None else same[d, k]
        remote = local = itself = None
        if False in kinds:
            remote = pltpu.make_async_remote_copy(
                src_ref=src, dst_ref=dst, send_sem=s3.at[slot], recv_sem=r3.at[slot],
                device_id=target, device_id_type=MESH_ID,
            )
        if True in kinds:
            local = pltpu.make_async_copy(src, dst, r3.at[slot])
        if local is None:
            remote.start()
        elif remote is None:
            local.start()
        else:
            itself = (target[0] == box) & (target[1] == lev)
            pl.when(itself)(local.start)
            pl.when(jnp.logical_not(itself))(remote.start)
        third.append((remote, local, itself))

    def target_of(d, k):
        other = around[opposite(d)]
        linear = other[0] * n_lev + other[1]
        return at(lax.rem(linear + (n_dev - DELTAS[k]), n_dev))

    z_size = 8 * fields
    for k in order:
        send(z_out.at[pl.ds(k * z_size, z_size)], z_in.at[k], k, None, k, shifted(-DELTAS[k]))

    field_step = plane
    sublane = iota((SUB, LANES), 0)
    in_group = iota((SUB, LANES), 1) % edge
    for d in (0, 1, 2, 3):
        outer, inner = (edge, 1) if d < 2 else (1, edge)
        adjacent = edge - 1 if d % 2 == 0 else 0
        far = edge - 2 if d % 2 == 0 else 1
        lines = []
        for i in range(8):
            lines.append(jnp.concatenate([
                upd[pl.ds(level * outer + (h * 8 + i) * inner, SUB, stride=field_step), :]
                for level in (adjacent, far) for h in range(2)
            ], axis=0))
        by_region = transposed_groups(lines, edge)
        ends = []
        for g in range(8):
            before = by_region[(g + 7) % 8][:2 * SUB]
            after = by_region[(g + 1) % 8][:2 * SUB]
            ends.append(jnp.where(iota((2 * SUB, LANES), 1) % edge == 0, after, before))
        for k in range(4):
            region = near_in[opposite(d), k]
            total = by_region[0]
            end = ends[0]
            for g in range(1, 8):
                hit = region == float(g)
                total = jnp.where(hit, by_region[g], total)
                end = jnp.where(hit, ends[g], end)
            base = (d * 4 + k) * lay.side
            for part in range(4):
                side_out[base + part * fields:base + (part + 1) * fields, :] = total[
                    part * SUB:part * SUB + fields, :
                ]
            for h in range(2):
                used = (sublane < fields) & ((in_group == 0) | (in_group == edge - 1))
                one = jnp.where(used, end[h * SUB:(h + 1) * SUB, :], 0.0)
                for bit in (1, 2, 4):
                    moved = pltpu.roll(one, LANES - 2 * bit, 1)
                    one = jnp.where((sublane // bit) % 2 == 1, moved, one)
                side_out[base + lay.ends + h:base + lay.ends + h + 1, :] = jnp.sum(
                    one, axis=0, keepdims=True
                )
        if d < 2:
            for e in range(2):
                side_out[pl.ds(d * 4 * lay.side + lay.ends + 2 + e, 4, stride=lay.side), :] = (
                    end_lines[d][e * 4:(e + 1) * 4, :]
                )
        else:
            for e in range(2):
                side_out[pl.ds(d * 4 * lay.side + lay.ends + 2 + e, 4, stride=lay.side), :] = (
                    jnp.zeros((4, LANES), F32)
                )
        for k in order:
            send(
                side_out.at[pl.ds((d * 4 + k) * lay.side, lay.side)], side_in.at[k, d],
                4 + d * 4 + k, d, k, target_of(d, k),
            )

    for f in range(fields):
        for corner in range(4):
            x = 0 if corner // 2 else edge - 1
            y = 0 if corner % 2 else edge - 1
            start = f * plane + x * edge + y
            corner_lines[7 - f, corner:corner + 1, :] = upd[start:start + 1, :]
    by_region = transposed_groups([corner_lines[f] for f in range(8)], edge)
    for k in range(4):
        region = corner_region[k]
        total = by_region[0]
        for g in range(1, 8):
            total = jnp.where(region == float(g), by_region[g], total)
        for corner in range(4):
            corner_out[corner, k] = total[corner:corner + 1, :]
    for corner in range(4):
        for k in order:
            send(
                corner_out.at[corner, k], corner_in.at[k, corner],
                20 + corner * 4 + k, 4 + corner, k, target_of(4 + corner, k),
            )

    for remote, local, itself in third:
        if local is None:
            remote.wait_recv()
        elif remote is None:
            local.wait()
        else:
            pl.when(itself)(local.wait)
            pl.when(jnp.logical_not(itself))(remote.wait_recv)

    for s in range(slots):
        delta = owner[0, s]
        k = delta + 2 - jnp.where(delta > 0, 1, 0)
        for d in range(4):
            window[s, d * lay.side:(d + 1) * lay.side, :] = side_in[k, d]
        window[s, lay.z:lay.z + z_size, :] = z_in[k]
        for corner in range(4):
            window[s, lay.corner + corner:lay.corner + corner + 1, :] = corner_in[k, corner]

    for copy in first + told + passed:
        copy.wait_send()
    for remote, local, itself in third:
        if local is None:
            remote.wait_send()
        elif remote is not None:
            pl.when(jnp.logical_not(itself))(remote.wait_send)


def ghost_kernel(
    slots, fields, edge, count, mask, window, updated_in, updated_out, ghost_out,
    ghost, pass_sem, out_sem,
):
    lay = Layout(fields, edge)
    live_count = count[0]
    outs = [pltpu.make_async_copy(updated_in, updated_out, pass_sem.at[0])]
    outs[0].start()

    def weights(width, target, along, within, normal):
        row = iota((LANES, width), 0)
        part = (row // edge) % 4
        signs = jnp.where(part == 1, along, jnp.where(part == 2, within, normal))
        value = jnp.where(part == 0, 1.0, jnp.where(signs == 1, 0.125, -0.125))
        return jnp.where(row % edge == target, value, 0.0).astype(BF16)

    lx = iota((LANES, 2 * LANES), 1)
    lz = iota((LANES, LANES), 1)
    quarter = 2 * edge
    tables = (
        weights(2 * LANES, (lx % quarter) // 2, (lx // quarter) % 2, lx % 2, lx // LANES),
        weights(LANES, (lz % quarter) // 2, lz // 64, lz % 2, (lz // quarter) % 2),
        weights(LANES, (lz % 64) // 4, lz // 64, (lz // 2) % 2, lz % 2),
    )
    lane = iota((SUB, LANES), 1)
    in_group = lane % edge
    last_lane, first_lane = lane >= LANES - edge, lane < edge
    low_half = lane < LANES // 2

    for s in range(slots):
        def rows(start):
            return window[s, start:start + SUB, :]

        def spread(start, shift, stride):
            row = jnp.broadcast_to(window[s, start:start + 1, :], (SUB, LANES))
            return pltpu.roll(row, shift % LANES, 1, stride=stride, stride_axis=0)

        for kind in range(3):
            parts = [[], [], [], []]
            for side in range(2):
                face = 2 * kind + side
                base = face * lay.side if kind < 2 else lay.z + side * 4 * fields
                centre = [rows(base + h * fields) for h in range(2)]
                far = [rows(base + (2 + h) * fields) for h in range(2)]
                own = [rows(lay.own + (2 * face + h) * fields) for h in range(2)]
                if kind == 0:
                    lines = [lay.corner + 2 * side, lay.corner + 2 * side + 1]
                elif kind == 1:
                    lines = [lay.corner + side, lay.corner + 2 + side]
                else:
                    lines = [d * lay.side + lay.ends + 2 + side for d in range(2)]
                below = spread(lines[0], edge, edge)
                above = spread(lines[1], 0, edge)
                up = [pltpu.roll(v, LANES - edge, 1) for v in centre]
                down = [pltpu.roll(v, edge, 1) for v in centre]
                along = [
                    jnp.where(last_lane, up[1], up[0]) - jnp.where(first_lane, below, down[0]),
                    jnp.where(last_lane, above, up[1]) - jnp.where(first_lane, down[0], down[1]),
                ]
                within = []
                for h in range(2):
                    if kind < 2:
                        before = spread(base + lay.ends + h, 1 - edge, 2)
                        after = spread(base + lay.ends + h, edge - 1, 2)
                    else:
                        low_row, high_row = 2 * lay.side + lay.ends + h, 3 * lay.side + lay.ends + h
                        before = spread(low_row, 0 if side else 1 - edge, 2)
                        after = spread(high_row, edge - 1 if side else 0, 2)
                    right = jnp.where(in_group == edge - 1, after, pltpu.roll(centre[h], LANES - 1, 1))
                    left = jnp.where(in_group == 0, before, pltpu.roll(centre[h], 1, 1))
                    within.append(right - left)
                normal = [(o - v) if side == 0 else (v - o) for o, v in zip(own, far)]
                for part, values in zip(parts, (centre, along, within, normal)):
                    part.extend(values)
            wide = [jnp.concatenate(part, axis=0) for part in parts]
            high = [v.astype(BF16).astype(F32) for v in wide]
            low = [v - u for v, u in zip(wide, high)]
            groups = transposed_groups(high + low, edge)
            spreads = jnp.dot(
                jnp.concatenate(groups, axis=0).astype(BF16), tables[kind], preferred_element_type=F32
            )
            for side in range(2):
                face = 2 * kind + side
                keep = jnp.where((s < live_count) & (mask[s, face] > 0), 1.0, 0.0).astype(F32)
                for h in range(2):
                    def cell(i):
                        start = (i * 4 + side * 2 + h) * SUB
                        return spreads[start:start + SUB, :]

                    if kind == 0:
                        for t in range(4):
                            for layer in range(2):
                                cols = slice(layer * LANES, (layer + 1) * LANES)
                                value = jnp.where(low_half, cell(2 * t)[:, cols], cell(2 * t + 1)[:, cols])
                                to = (layer * 8 + h * 4 + t) * LANES
                                ghost[s, :, face, to:to + LANES] = (value * keep)[:fields]
                    else:
                        for i in range(8):
                            to = (h * 8 + i) * LANES
                            ghost[s, :, face, to:to + LANES] = (cell(i) * keep)[:fields]
        outs.append(pltpu.make_async_copy(ghost.at[s], ghost_out.at[s], out_sem.at[s]))
        outs[-1].start()
    for copy in outs:
        copy.wait()


def body(n_box, n_lev, fine, coarse, owner_map, patch_count, face_mask):
    slots, fields, fine_edge, _ = fine.shape
    edge = fine_edge // 2
    block = fields * edge
    lay = Layout(fields, edge)
    vmem = pl.BlockSpec(memory_space=pltpu.VMEM)
    smem = pl.BlockSpec(memory_space=pltpu.SMEM)
    hbm = pl.BlockSpec(memory_space=pltpu.HBM)
    flat = jax.ShapeDtypeStruct((block * edge, LANES), F32)
    updated, window = pl.pallas_call(
        functools.partial(kernel, n_box, n_lev, slots, fields, edge),
        out_shape=(flat, jax.ShapeDtypeStruct((slots, lay.rows, LANES), F32)),
        in_specs=[smem, smem, hbm, hbm],
        out_specs=(vmem, vmem),
        scratch_shapes=[
            pltpu.VMEM((slots * fields * fine_edge, fine_edge * fine_edge), F32),
            pltpu.VMEM((block * edge, LANES), F32),
            pltpu.VMEM((slots * fields * fine_edge, LANES), F32),
            pltpu.VMEM((slots * fields * fine_edge, LANES), F32),
            pltpu.VMEM((2 * slots * block, LANES), F32),
            pltpu.VMEM((4 * slots * block, LANES), F32),
            pltpu.VMEM((4, block, 2 * LANES), F32),
            pltpu.VMEM((4, block, 2 * LANES), F32),
            pltpu.VMEM((4, 1, LANES), F32),
            pltpu.VMEM((4, 1, LANES), F32),
            pltpu.VMEM((8, 4, 1, LANES), F32),
            pltpu.VMEM((SUB * edge * edge, LANES), F32),
            pltpu.VMEM((SUB, SUB, LANES), F32),
            pltpu.VMEM((4, SUB, LANES), F32),
            pltpu.VMEM((16 * lay.side, LANES), F32),
            pltpu.VMEM((4, 4, lay.side, LANES), F32),
            pltpu.VMEM((4 * 8 * fields, LANES), F32),
            pltpu.VMEM((4, 8 * fields, LANES), F32),
            pltpu.VMEM((4, 4, 1, LANES), F32),
            pltpu.VMEM((4, 4, 1, LANES), F32),
            pltpu.VMEM((4, 2 * LANES, 2 * LANES), BF16),
            pltpu.SemaphoreType.DMA((2 * slots + 1,)),
            pltpu.SemaphoreType.DMA((8,)),
            pltpu.SemaphoreType.DMA((8,)),
            pltpu.SemaphoreType.DMA((12,)),
            pltpu.SemaphoreType.DMA((12,)),
            pltpu.SemaphoreType.DMA((36,)),
            pltpu.SemaphoreType.DMA((36,)),
        ],
        compiler_params=pltpu.CompilerParams(
            collective_id=0, has_side_effects=True, vmem_limit_bytes=55000000
        ),
    )(
        owner_map.T, patch_count,
        fine.reshape(slots * fields * fine_edge, fine_edge * fine_edge),
        coarse.reshape(block * edge, LANES),
    )
    ghost_shape = (slots, fields, 6, 2 * fine_edge * fine_edge)
    updated, ghost = pl.pallas_call(
        functools.partial(ghost_kernel, slots, fields, edge),
        out_shape=(flat, jax.ShapeDtypeStruct(ghost_shape, F32)),
        in_specs=[smem, smem, vmem, vmem],
        out_specs=(hbm, hbm),
        scratch_shapes=[
            pltpu.VMEM(ghost_shape, F32),
            pltpu.SemaphoreType.DMA((1,)),
            pltpu.SemaphoreType.DMA((slots,)),
        ],
        compiler_params=pltpu.CompilerParams(vmem_limit_bytes=16777216),
    )(patch_count, face_mask, window, updated)
    return updated.reshape(coarse.shape), ghost.transpose(0, 2, 1, 3)


def solution(mesh):
    return jax.shard_map(
        functools.partial(body, mesh.shape["box"], mesh.shape["lev"]),
        mesh=mesh,
        in_specs=(
            P(("box", "lev"), None, None, None),
            P(None, "box", "lev", None),
            P(("box", "lev"), None),
            P(("box", "lev")),
            P(("box", "lev"), None),
        ),
        out_specs=(P(None, "box", "lev", None), P(("box", "lev"), None, None, None)),
        check_vma=False,
    )
```

```python
import functools

import jax
import jax.numpy as jnp
from jax import lax
from jax.experimental import pallas as pl
from jax.experimental.pallas import tpu as pltpu
from jax.sharding import PartitionSpec as P

DELTAS = (-2, -1, 1, 2)
LANES = 128
SUB = 8
F32 = jnp.float32
BF16 = jnp.bfloat16
MESH_ID = pl.DeviceIdType.MESH
VMEM_FIRST = 56000000
VMEM_SECOND = 56000000


def iota(shape, dim):
    return lax.broadcasted_iota(jnp.int32, shape, dim)


def split(values):
    high = values.astype(BF16)
    return high, (values - high.astype(F32)).astype(BF16)


def split_lanes(values):
    return jnp.concatenate(split(values), axis=1)


def times_transposed(left, right):
    return lax.dot_general(left, right, (((1,), (1,)), ((), ())), preferred_element_type=F32)


def both(table):
    return jnp.concatenate([table, table], axis=0)


def transposed_groups(arrays, edge):
    out = list(arrays)
    group = iota(out[0].shape, 1) // edge
    for bit in (4, 2, 1):
        low = (group // bit) % 2 == 0
        for i in range(8):
            if i & bit == 0:
                a, b = out[i], out[i + bit]
                out[i] = jnp.where(low, a, pltpu.roll(b, bit * edge, 1))
                out[i + bit] = jnp.where(low, pltpu.roll(a, LANES - bit * edge, 1), b)
    return out


class Layout:
    def __init__(self, fields, edge):
        self.ends = 4 * fields
        self.side = 4 * fields + 4
        self.z_size = 8 * fields
        self.z = 4 * self.side
        self.corner = self.z + self.z_size
        self.own = self.corner + 4
        self.keep = self.own + 12 * fields
        self.rows = self.keep + 6
        self.rows = self.rows + (-self.rows) % SUB
        self.field = edge * edge + SUB


DIRECTIONS = ((-1, 0), (1, 0), (0, -1), (0, 1), (-1, -1), (-1, 1), (1, -1), (1, 1))


def relations(n_box, n_lev):
    n_dev = n_box * n_lev
    offsets, same = set(), {}
    for me in range(n_dev):
        box, lev = divmod(me, n_lev)

        def add(other):
            db, dl = (other // n_lev - box) % n_box, (other % n_lev - lev) % n_lev
            offsets.add((db, dl))
            offsets.add((-db % n_box, -dl % n_lev))

        for delta in DELTAS:
            add((me + delta) % n_dev)
        for d, (dx, dy) in enumerate(DIRECTIONS):
            owner = ((box - dx) % n_box) * n_lev + (lev - dy) % n_lev
            add(owner)
            for k, delta in enumerate(DELTAS):
                target = (owner - delta) % n_dev
                add(target)
                same.setdefault((d, k), set()).add(target == me)
    offsets.discard((0, 0))
    reach = max(min(db, n_box - db) for db, _ in offsets)
    return sorted(offsets), reach, same


def kernel(
    n_box, n_lev, slots, fields, edge,
    owner_far, count_far, mask_far, fine_far, coarse_far, updated, window,
    owner_of, count, mask, fine, coarse, avg, own_got, send1, recv1, region_out, near_in,
    upd, corner_lines, corner_region, side_out, side_in, z_out, z_in, corner_out, corner_in, place_table,
    small, load, put, s1, r1, sh, rh, s3, r3, mixed,
):
    fine_edge = 2 * edge
    block = fields * edge
    plane = edge * edge
    lay = Layout(fields, edge)
    frows = fields * fine_edge
    cut = (fields + 1) // 2
    chunks = ((0, cut), (cut, fields))
    small_loads = [
        pltpu.make_async_copy(src, dst, small.at[i])
        for i, (src, dst) in enumerate(((owner_far, owner_of), (count_far, count), (mask_far, mask)))
    ]
    for copy in small_loads:
        copy.start()
    all_rows = slots * frows
    loads = {}
    for part, (f0, f1) in enumerate(chunks):
        for s in range(slots):
            start, size = s * frows + f0 * fine_edge, (f1 - f0) * fine_edge
            for t in range(8):
                copy = pltpu.make_async_copy(
                    fine_far.at[pl.ds(start, size), pl.ds(t * LANES, LANES)],
                    fine.at[pl.ds(t * all_rows + start, size)],
                    load.at[part],
                )
                copy.start()
        rows = fine.at[pl.ds(0, 8 * slots * (f1 - f0) * fine_edge)]
        loads[part] = pltpu.make_async_copy(rows, rows, load.at[part])
    coarse_load = pltpu.make_async_copy(coarse_far, coarse, small.at[3])
    coarse_load.start()
    n_dev = n_box * n_lev
    offsets, reach, same = relations(n_box, n_lev)
    box = lax.axis_index("box")
    lev = lax.axis_index("lev")
    me = box * n_lev + lev

    def at(linear):
        return (lax.div(linear, n_lev), lax.rem(linear, n_lev))

    def shifted(by):
        return at(lax.rem(me + (by + n_dev), n_dev))

    def beside(dx, dy):
        return (lax.rem(box + (dx + n_box), n_box), lax.rem(lev + (dy + n_lev), n_lev))

    barrier = pltpu.get_barrier_semaphore()
    for db, dl in offsets:
        pl.semaphore_signal(barrier, inc=1, device_id=beside(db, dl), device_id_type=MESH_ID)

    q = iota((fine_edge * fine_edge, plane), 0)
    c = iota((fine_edge * fine_edge, plane), 1)
    goal = (q // (2 * fine_edge)) * edge + (q % fine_edge) // 2
    table = jnp.where(goal == c, 0.125, 0.0).astype(BF16)
    order = (1, 2, 0, 3)
    back = [shifted(-delta) for delta in DELTAS]

    def target_of(d, k):
        dx, dy = DIRECTIONS[d]
        other = beside(-dx, -dy)
        return at(lax.rem(other[0] * n_lev + other[1] + (n_dev - DELTAS[k]), n_dev))

    targets = [[target_of(d, k) for k in range(4)] for d in range(8)]

    def place_of(device):
        db = lax.rem(device[0] - box + (n_box + reach), n_box)
        return db * n_lev + lax.rem(device[1] - lev + n_lev, n_lev)

    for copy in small_loads:
        copy.wait()
    live_count = count[0]
    owner = [owner_of[0, s] for s in range(slots)]
    region_of = [owner_of[1, s] for s in range(slots)]
    chosen = [
        [(s < live_count) & (owner[s] == delta) for delta in DELTAS] for s in range(slots)
    ]
    weight = [[jnp.where(c, 1.0, 0.0).astype(F32) for c in row] for row in chosen]
    for k in range(4):
        region = jnp.int32(-1)
        for s in range(slots):
            region = jnp.where(chosen[s][k], region_of[s], region)
        region_out[k] = jnp.full((1, LANES), 1.0, F32) * region.astype(F32)

    near_in[reach * n_lev] = region_out[...]
    first = {}
    for part, (f0, f1) in enumerate(chunks):
        size = (f1 - f0) * edge
        loads[part].wait()
        columns = []
        for t in range(8):
            pieces = []
            for s in range(slots):
                start = t * all_rows + s * frows + f0 * fine_edge
                pieces.append(
                    fine[pl.ds(start, size, stride=2), :] + fine[pl.ds(start + 1, size, stride=2), :]
                )
            columns.append(jnp.concatenate(pieces, axis=0))
        high, low = split(jnp.concatenate(columns, axis=1))
        got = jnp.dot(jnp.concatenate([high, low], axis=0), table, preferred_element_type=F32)
        got = got[:slots * size] + got[slots * size:]
        to = f0 * edge
        for h in range(2):
            averaged = []
            for s in range(slots):
                mean = got[s * size:(s + 1) * size, h * LANES:(h + 1) * LANES]
                start = (h * slots + s) * block + to
                avg[start:start + size, :] = mean
                averaged.append(mean)
            for k in range(4):
                total = averaged[0] * weight[0][k]
                for s in range(1, slots):
                    total = total + averaged[s] * weight[s][k]
                send1[k, to:to + size, h * LANES:(h + 1) * LANES] = total
        if part == 0:
            pl.semaphore_wait(barrier, len(offsets))
            for db, dl in offsets:
                slot = ((reach - db) % n_box) * n_lev + (-dl) % n_lev
                copy = pltpu.make_async_remote_copy(
                    src_ref=region_out, dst_ref=near_in.at[slot],
                    send_sem=sh.at[0], recv_sem=rh.at[0],
                    device_id=beside(db, dl), device_id_type=MESH_ID,
                )
                copy.start()
        for k in order:
            copy = pltpu.make_async_remote_copy(
                src_ref=send1.at[k, pl.ds(to, size)], dst_ref=recv1.at[k, pl.ds(to, size)],
                send_sem=s1.at[0], recv_sem=r1.at[part],
                device_id=shifted(DELTAS[k]), device_id_type=MESH_ID,
            )
            copy.start()
        rows = recv1.at[:, pl.ds(to, size)]
        first[part] = pltpu.make_async_copy(rows, rows, r1.at[part])

    for pair in range(4):
        row = iota((LANES, 2 * LANES), 0)
        col = iota((LANES, 2 * LANES), 1)
        hit = (row // edge == 2 * pair + col // LANES) & (row % edge == col % edge)
        place_table[pair] = both(jnp.where(hit, 1.0, 0.0).astype(BF16))

    row = iota((plane, 4 * LANES), 0)
    col = iota((plane, 4 * LANES), 1)
    kind = col // LANES
    inner = col % edge
    fixed = jnp.where(kind % 2 == 0, 0, edge - 1)
    hit = jnp.where(kind < 2, fixed * edge + inner, inner * edge + fixed) == row
    own_table = jnp.where(hit, 1.0, 0.0).astype(BF16)
    high, low = split(jnp.concatenate(
        [avg[:slots * block, :], avg[slots * block:, :]], axis=1
    ))
    got = jnp.dot(high, own_table, preferred_element_type=F32) + jnp.dot(
        low, own_table, preferred_element_type=F32
    )
    for kind in range(4):
        own_got[kind * slots * block:(kind + 1) * slots * block, :] = got[
            :, kind * LANES:(kind + 1) * LANES
        ]
    group_f = iota((fields, LANES), 1) // edge
    for s in range(slots):
        for h in range(2):
            for side in range(2):
                start = (h * slots + s) * block + side * (edge - 1)
                to = lay.own + (2 * side + h) * fields
                window[s, to:to + fields, :] = avg[pl.ds(start, fields, stride=edge), :]
            for kind in range(4):
                total = jnp.zeros((fields, LANES), F32)
                for i in range(8):
                    start = (kind * slots + s) * block + h * 8 + i
                    part = own_got[pl.ds(start, fields, stride=edge), :]
                    total = jnp.where(group_f == i, part, total)
                to = lay.own + (2 * (2 + kind) + h) * fields
                window[s, to:to + fields, :] = total

        for face in range(6):
            keep = jnp.where((s < live_count) & (mask[s, face] > 0), 1.0, 0.0).astype(F32)
            window[s, lay.keep + face:lay.keep + face + 1, :] = jnp.full((1, LANES), 1.0, F32) * keep
    corner_lines[...] = jnp.zeros_like(corner_lines)
    coarse_load.wait()
    told = near_in.at[pl.ds(0, len(offsets))]
    pltpu.make_async_copy(told, told, rh.at[0]).wait()

    lane = iota((1, LANES), 1).astype(F32)
    here_rows = [near_in[place_of(back[k]), k] for k in range(4)]
    near = [[near_in[place_of(targets[d][k]), k] for k in range(4)] for d in range(8)]

    def pick(region, place):
        t = lane - edge * region - place
        return jnp.where((t == 0.0) | (t == LANES) | (t == -LANES), 1.0, 0.0)

    z_rows = []
    for depth in range(2):
        for k in range(4):
            for place in (-1 - depth, edge + depth):
                z_rows.append(pick(here_rows[k], place))
    for d in range(2):
        for place in (-1, edge):
            for k in range(4):
                z_rows.append(pick(near[d][k], place))
    z_table = jnp.concatenate(z_rows, axis=0).astype(BF16)
    z_table = jnp.concatenate([z_table, z_table], axis=1)
    for corner in range(4):
        for k in range(4):
            corner_region[k, corner:corner + 1, :] = near[4 + corner][k]

    group = (iota((1, LANES), 1) // edge).astype(F32)
    here = [group == region for region in here_rows]
    group8 = iota((SUB, LANES), 1) // edge
    end_lines = [jnp.zeros((SUB, LANES), F32) for _ in range(2)]
    for part, (f0, f1) in enumerate(chunks):
        size = (f1 - f0) * edge
        first[part].wait()
        to = f0 * edge
        for h in range(2):
            stacked = split_lanes(jnp.concatenate(
                [recv1[k, to:to + size, h * LANES:(h + 1) * LANES] for k in range(4)], axis=0
            ))
            for pair in range(4):
                spread = jnp.dot(stacked, place_table[pair], preferred_element_type=F32)
                for odd in range(2):
                    y = h * SUB + 2 * pair + odd
                    for f in range(f0, f1):
                        merged = coarse[pl.ds(f * plane + y, edge, stride=edge), :]
                        for k in range(4):
                            start = k * size + (f - f0) * edge
                            merged = jnp.where(
                                here[k],
                                spread[start:start + edge, odd * LANES:(odd + 1) * LANES],
                                merged,
                            )
                        upd[pl.ds(f * lay.field + y, edge, stride=edge), :] = merged
        for f in range(f0, f1):
            pltpu.make_async_copy(
                upd.at[pl.ds(f * lay.field, plane)], updated.at[pl.ds(f * plane, plane)], put.at[0]
            ).start()
        for f in range(f0, f1):
            start = f * lay.field
            got = times_transposed(z_table, split_lanes(upd[start:start + plane, :]))
            for depth in range(2):
                for h in range(2):
                    z_out[pl.ds((2 * depth + h) * fields + f, 8, stride=4 * fields), :] = got[
                        depth * 8:(depth + 1) * 8, h * LANES:(h + 1) * LANES
                    ]
            high_end = got[16:24, LANES:]
            if f:
                high_end = pltpu.roll(high_end, LANES - f * edge, 1)
            low_end = pltpu.roll(got[24:32, :LANES], LANES - (f + 1) * edge, 1)
            end_lines[0] = jnp.where(group8 == 7 - f, high_end, end_lines[0])
            end_lines[1] = jnp.where(group8 == 7 - f, low_end, end_lines[1])

    clear, unclear = [0, 0, 0], []

    def send(src, dst, sem, d, k, target):
        kinds = {False} if d is None else same[d, k]
        remote = local = None
        if False in kinds:
            remote = pltpu.make_async_remote_copy(
                src_ref=src, dst_ref=dst, recv_sem=r3.at[sem], device_id=target, device_id_type=MESH_ID,
                send_sem=s3.at[sem] if len(kinds) == 1 else mixed.at[len(unclear)],
            )
        if True in kinds:
            local = pltpu.make_async_copy(src, dst, r3.at[sem])
        if local is None:
            remote.start()
            clear[sem] += 1
        elif remote is None:
            local.start()
        else:
            itself = (target[0] == box) & (target[1] == lev)
            pl.when(itself)(local.start)
            pl.when(jnp.logical_not(itself))(remote.start)
            unclear.append((remote, itself))

    for k in order:
        send(z_out.at[pl.ds(k * lay.z_size, lay.z_size)], z_in.at[k], 0, None, k, back[k])

    field_step = lay.field
    sublane = iota((SUB, LANES), 0)
    in_group = iota((SUB, LANES), 1) % edge
    for d in (0, 1, 2, 3):
        outer, inner = (edge, 1) if d < 2 else (1, edge)
        adjacent = edge - 1 if d % 2 == 0 else 0
        far = edge - 2 if d % 2 == 0 else 1
        lines = []
        for i in range(8):
            lines.append(jnp.concatenate([
                upd[pl.ds(level * outer + (h * 8 + i) * inner, SUB, stride=field_step), :]
                for level in (adjacent, far) for h in range(2)
            ], axis=0))
        by_region = transposed_groups(lines, edge)
        ends = []
        for g in range(8):
            before = by_region[(g + 7) % 8][:2 * SUB]
            after = by_region[(g + 1) % 8][:2 * SUB]
            ends.append(jnp.where(iota((2 * SUB, LANES), 1) % edge == 0, after, before))
        for k in range(4):
            region = near[d][k]
            total = by_region[0]
            end = ends[0]
            for g in range(1, 8):
                hit = region == float(g)
                total = jnp.where(hit, by_region[g], total)
                end = jnp.where(hit, ends[g], end)
            base = (d * 4 + k) * lay.side
            for part in range(4):
                side_out[base + part * fields:base + (part + 1) * fields, :] = total[
                    part * SUB:part * SUB + fields, :
                ]
            for h in range(2):
                used = (sublane < fields) & ((in_group == 0) | (in_group == edge - 1))
                one = jnp.where(used, end[h * SUB:(h + 1) * SUB, :], 0.0)
                moved = one
                for f in range(1, fields):
                    moved = jnp.where(sublane == f, pltpu.roll(one, LANES - 2 * f, 1), moved)
                one = moved
                side_out[base + lay.ends + h:base + lay.ends + h + 1, :] = jnp.sum(
                    one, axis=0, keepdims=True
                )
        if d < 2:
            for e in range(2):
                side_out[pl.ds(d * 4 * lay.side + lay.ends + 2 + e, 4, stride=lay.side), :] = (
                    end_lines[d][e * 4:(e + 1) * 4, :]
                )
        else:
            for e in range(2):
                side_out[pl.ds(d * 4 * lay.side + lay.ends + 2 + e, 4, stride=lay.side), :] = (
                    jnp.zeros((4, LANES), F32)
                )

    for f in range(fields):
        for corner in range(4):
            x = 0 if corner // 2 else edge - 1
            y = 0 if corner % 2 else edge - 1
            start = f * lay.field + x * edge + y
            corner_lines[7 - f, corner:corner + 1, :] = upd[start:start + 1, :]
    by_region = transposed_groups([corner_lines[f] for f in range(8)], edge)
    for k in range(4):
        region = corner_region[k]
        total = by_region[0]
        for g in range(1, 8):
            total = jnp.where(region == float(g), by_region[g], total)
        for corner in range(4):
            corner_out[corner * 4 + k] = total[corner:corner + 1, :]
    for d in (0, 1, 2, 3):
        for k in order:
            send(
                side_out.at[pl.ds((d * 4 + k) * lay.side, lay.side)], side_in.at[k, d],
                1, d, k, targets[d][k],
            )
    for corner in range(4):
        for k in order:
            send(
                corner_out.at[corner * 4 + k], corner_in.at[k * 4 + corner],
                2, 4 + corner, k, targets[4 + corner][k],
            )

    for sem, ref in enumerate((z_in, side_in, corner_in)):
        pltpu.make_async_copy(ref, ref, r3.at[sem]).wait()
    for s in range(slots):
        k = owner[s] + 2 - jnp.where(owner[s] > 0, 1, 0)
        for d in range(4):
            window[s, d * lay.side:(d + 1) * lay.side, :] = side_in[k, d]
        window[s, lay.z:lay.z + lay.z_size, :] = z_in[k]
        for corner in range(4):
            window[s, lay.corner + corner:lay.corner + corner + 1, :] = corner_in[k * 4 + corner]

    pltpu.make_async_copy(updated, updated, put.at[0]).wait()
    pltpu.make_async_copy(send1, send1, s1.at[0]).wait()
    told = near_in.at[pl.ds(0, len(offsets))]
    pltpu.make_async_copy(told, told, sh.at[0]).wait()
    for sem, (ref, size) in enumerate(((z_out, lay.z_size), (side_out, lay.side), (corner_out, 1))):
        if clear[sem]:
            rows = ref.at[pl.ds(0, clear[sem] * size)]
            pltpu.make_async_copy(rows, rows, s3.at[sem]).wait()
    for remote, itself in unclear:
        pl.when(jnp.logical_not(itself))(remote.wait_send)


def ghost_kernel(
    slots, fields, edge, updated_in, window, updated_out, ghost_out, passing, ghost, lhs, pass_sem, out_sem
):
    lay = Layout(fields, edge)
    into = pltpu.make_async_copy(updated_in, passing, pass_sem.at[0])
    out = pltpu.make_async_copy(passing, updated_out, pass_sem.at[1])
    into.start()

    def weights(width, target, along, within, normal):
        row = iota((LANES, width), 0)
        part = (row // edge) % 4
        signs = jnp.where(part == 1, along, jnp.where(part == 2, within, normal))
        value = jnp.where(part == 0, 1.0, jnp.where(signs == 1, 0.125, -0.125))
        return jnp.where(row % edge == target, value, 0.0).astype(BF16)

    lx = iota((LANES, 2 * LANES), 1)
    lz = iota((LANES, LANES), 1)
    quarter = 2 * edge
    tables = (
        weights(2 * LANES, (lx % quarter) // 2, (lx // quarter) % 2, lx % 2, lx // LANES),
        weights(LANES, (lz % quarter) // 2, lz // 64, lz % 2, (lz // quarter) % 2),
        weights(LANES, (lz % 64) // 4, lz // 64, (lz // 2) % 2, lz % 2),
    )
    lane = iota((SUB, LANES), 1)
    in_group = lane % edge
    last_lane, first_lane = lane >= LANES - edge, lane < edge
    low_half = lane < LANES // 2

    for s in range(slots):
        def rows(start, size=SUB):
            return window[s, start:start + size, :]

        def spread(start, shift, stride):
            row = jnp.broadcast_to(rows(start, 1), (SUB, LANES))
            return pltpu.roll(row, shift % LANES, 1, stride=stride, stride_axis=0)

        for kind in range(3):
            parts = [[], [], [], []]
            for side in range(2):
                face = 2 * kind + side
                base = face * lay.side if kind < 2 else lay.z + side * 4 * fields
                layers = [rows(base + h * fields) for h in range(4)]
                centre, far = layers[:2], layers[2:]
                own = [rows(lay.own + (2 * face + h) * fields) for h in range(2)]
                if kind == 0:
                    lines = [lay.corner + 2 * side, lay.corner + 2 * side + 1]
                elif kind == 1:
                    lines = [lay.corner + side, lay.corner + 2 + side]
                else:
                    lines = [d * lay.side + lay.ends + 2 + side for d in range(2)]
                below = spread(lines[0], edge, edge)
                above = spread(lines[1], 0, edge)
                up = [pltpu.roll(v, LANES - edge, 1) for v in centre]
                down = [pltpu.roll(v, edge, 1) for v in centre]
                along = [
                    jnp.where(last_lane, up[1], up[0]) - jnp.where(first_lane, below, down[0]),
                    jnp.where(last_lane, above, up[1]) - jnp.where(first_lane, down[0], down[1]),
                ]
                within = []
                for h in range(2):
                    if kind < 2:
                        before = spread(base + lay.ends + h, 1 - edge, 2)
                        after = spread(base + lay.ends + h, edge - 1, 2)
                    else:
                        low_row, high_row = 2 * lay.side + lay.ends + h, 3 * lay.side + lay.ends + h
                        before = spread(low_row, 0 if side else 1 - edge, 2)
                        after = spread(high_row, edge - 1 if side else 0, 2)
                    right = jnp.where(in_group == edge - 1, after, pltpu.roll(centre[h], LANES - 1, 1))
                    left = jnp.where(in_group == 0, before, pltpu.roll(centre[h], 1, 1))
                    within.append(right - left)
                normal = [(o - v) if side == 0 else (v - o) for o, v in zip(own, far)]
                for part, values in zip(parts, (centre, along, within, normal)):
                    part.extend(values)
            wide = [jnp.concatenate(part, axis=0) for part in parts]
            high = [v.astype(BF16).astype(F32) for v in wide]
            low = [v - u for v, u in zip(wide, high)]
            groups = transposed_groups(high + low, edge)
            lhs[s * 3 + kind] = jnp.concatenate(groups, axis=0).astype(BF16)

    into.wait()
    out.start()
    for s in range(slots):
        for kind in range(3):
            spreads = jnp.dot(lhs[s * 3 + kind], tables[kind], preferred_element_type=F32)
            for side in range(2):
                face = 2 * kind + side
                keep = window[s, lay.keep + face:lay.keep + face + 1, :]
                for h in range(2):
                    def cell(i):
                        start = (i * 4 + side * 2 + h) * SUB
                        return spreads[start:start + SUB, :]

                    if kind == 0:
                        for t in range(4):
                            for layer in range(2):
                                cols = slice(layer * LANES, (layer + 1) * LANES)
                                value = jnp.where(low_half, cell(2 * t)[:, cols], cell(2 * t + 1)[:, cols])
                                to = (layer * 8 + h * 4 + t) * LANES
                                ghost[s, :, face, to:to + LANES] = (value * keep)[:fields]
                    else:
                        for i in range(8):
                            to = (h * 8 + i) * LANES
                            ghost[s, :, face, to:to + LANES] = (cell(i) * keep)[:fields]
        pltpu.make_async_copy(ghost.at[s], ghost_out.at[s], out_sem.at[0]).start()
    out.wait()
    pltpu.make_async_copy(ghost, ghost_out, out_sem.at[0]).wait()


def body(n_box, n_lev, fine, coarse, owner_map, patch_count, face_mask):
    slots, fields, fine_edge, _ = fine.shape
    edge = fine_edge // 2
    block = fields * edge
    lay = Layout(fields, edge)
    offsets, reach, same = relations(n_box, n_lev)
    far = pl.BlockSpec(memory_space=pl.ANY)
    vmem = pl.BlockSpec(memory_space=pltpu.VMEM)
    flat = jax.ShapeDtypeStruct((block * edge, LANES), F32)
    places = (2 * reach + 1) * n_lev
    owner_rows = owner_map.T
    updated, window = pl.pallas_call(
        functools.partial(kernel, n_box, n_lev, slots, fields, edge),
        out_shape=(
            flat,
            jax.ShapeDtypeStruct((slots, lay.rows, LANES), F32),
        ),
        in_specs=[far] * 5,
        out_specs=(far, vmem),
        scratch_shapes=[
            pltpu.SMEM(owner_rows.shape, jnp.int32),
            pltpu.SMEM(patch_count.shape, jnp.int32),
            pltpu.SMEM(face_mask.shape, jnp.int32),
            pltpu.VMEM((8 * slots * fields * fine_edge, LANES), F32),
            pltpu.VMEM((block * edge, LANES), F32),
            pltpu.VMEM((2 * slots * block, LANES), F32),
            pltpu.VMEM((4 * slots * block, LANES), F32),
            pltpu.VMEM((4, block, 2 * LANES), F32),
            pltpu.VMEM((4, block, 2 * LANES), F32),
            pltpu.VMEM((4, 1, LANES), F32),
            pltpu.VMEM((places, 4, 1, LANES), F32),
            pltpu.VMEM((SUB * lay.field, LANES), F32),
            pltpu.VMEM((SUB, SUB, LANES), F32),
            pltpu.VMEM((4, SUB, LANES), F32),
            pltpu.VMEM((16 * lay.side, LANES), F32),
            pltpu.VMEM((4, 4, lay.side, LANES), F32),
            pltpu.VMEM((4 * lay.z_size, LANES), F32),
            pltpu.VMEM((4, lay.z_size, LANES), F32),
            pltpu.VMEM((16, 1, LANES), F32),
            pltpu.VMEM((16, 1, LANES), F32),
            pltpu.VMEM((4, 2 * LANES, 2 * LANES), BF16),
            pltpu.SemaphoreType.DMA((4,)),
            pltpu.SemaphoreType.DMA((2,)),
            pltpu.SemaphoreType.DMA((1,)),
            pltpu.SemaphoreType.DMA((1,)),
            pltpu.SemaphoreType.DMA((2,)),
            pltpu.SemaphoreType.DMA((1,)),
            pltpu.SemaphoreType.DMA((1,)),
            pltpu.SemaphoreType.DMA((3,)),
            pltpu.SemaphoreType.DMA((3,)),
            pltpu.SemaphoreType.DMA((max(1, sum(len(v) > 1 for v in same.values())),)),
        ],
        compiler_params=pltpu.CompilerParams(
            collective_id=0, has_side_effects=True, vmem_limit_bytes=VMEM_FIRST
        ),
    )(
        owner_rows, patch_count, face_mask,
        fine.reshape(slots * fields * fine_edge, fine_edge * fine_edge),
        coarse.reshape(block * edge, LANES),
    )
    ghost_shape = (slots, fields, 6, 2 * fine_edge * fine_edge)
    updated, ghost = pl.pallas_call(
        functools.partial(ghost_kernel, slots, fields, edge),
        out_shape=(flat, jax.ShapeDtypeStruct(ghost_shape, F32)),
        in_specs=[far, vmem],
        out_specs=(far, far),
        scratch_shapes=[
            pltpu.VMEM((block * edge, LANES), F32),
            pltpu.VMEM(ghost_shape, F32),
            pltpu.VMEM((3 * slots, 2 * LANES, LANES), BF16),
            pltpu.SemaphoreType.DMA((2,)),
            pltpu.SemaphoreType.DMA((1,)),
        ],
        compiler_params=pltpu.CompilerParams(vmem_limit_bytes=VMEM_SECOND),
    )(updated, window)
    return updated.reshape(coarse.shape), ghost.transpose(0, 2, 1, 3)


def solution(mesh):
    return jax.shard_map(
        functools.partial(body, mesh.shape["box"], mesh.shape["lev"]),
        mesh=mesh,
        in_specs=(
            P(("box", "lev"), None, None, None),
            P(None, "box", "lev", None),
            P(("box", "lev"), None),
            P(("box", "lev")),
            P(("box", "lev"), None),
        ),
        out_specs=(P(None, "box", "lev", None), P(("box", "lev"), None, None, None)),
        check_vma=False,
    )
```

```python
import functools

import jax
import jax.numpy as jnp
from jax import lax
from jax.experimental import pallas as pl
from jax.experimental.pallas import tpu as pltpu
from jax.sharding import PartitionSpec as P

DELTAS = (-2, -1, 1, 2)
LANES = 128
SUB = 8
F32 = jnp.float32
BF16 = jnp.bfloat16
MESH_ID = pl.DeviceIdType.MESH
VMEM_FIRST = 56000000
VMEM_SECOND = 56000000


def iota(shape, dim):
    return lax.broadcasted_iota(jnp.int32, shape, dim)


def split(values):
    high = values.astype(BF16)
    return high, (values - high.astype(F32)).astype(BF16)


def split_lanes(values):
    return jnp.concatenate(split(values), axis=1)


def times_transposed(left, right):
    return lax.dot_general(left, right, (((1,), (1,)), ((), ())), preferred_element_type=F32)


def both(table):
    return jnp.concatenate([table, table], axis=0)


def transposed_groups(arrays, edge, bits=(4, 2, 1)):
    out = list(arrays)
    group = iota(out[0].shape, 1) // edge
    for bit in bits:
        low = (group // bit) % 2 == 0
        for i in range(8):
            if i & bit == 0:
                a, b = out[i], out[i + bit]
                out[i] = jnp.where(low, a, pltpu.roll(b, bit * edge, 1))
                out[i + bit] = jnp.where(low, pltpu.roll(a, LANES - bit * edge, 1), b)
    return out


class Layout:
    def __init__(self, fields, edge):
        self.ends = 4 * fields
        self.side = 4 * fields + 4
        self.z_size = 8 * fields
        self.z = 4 * self.side
        self.corner = self.z + self.z_size
        self.own = self.corner + 4
        self.keep = self.own + 12 * fields
        self.rows = self.keep + 1
        self.rows = self.rows + (-self.rows) % SUB
        self.field = edge * edge + SUB


DIRECTIONS = ((-1, 0), (1, 0), (0, -1), (0, 1), (-1, -1), (-1, 1), (1, -1), (1, 1))


def relations(n_box, n_lev):
    n_dev = n_box * n_lev
    offsets, same = set(), {}
    for me in range(n_dev):
        box, lev = divmod(me, n_lev)

        def add(other):
            db, dl = (other // n_lev - box) % n_box, (other % n_lev - lev) % n_lev
            offsets.add((db, dl))
            offsets.add((-db % n_box, -dl % n_lev))

        for delta in DELTAS:
            add((me + delta) % n_dev)
        for d, (dx, dy) in enumerate(DIRECTIONS):
            owner = ((box - dx) % n_box) * n_lev + (lev - dy) % n_lev
            add(owner)
            for k, delta in enumerate(DELTAS):
                target = (owner - delta) % n_dev
                add(target)
                same.setdefault((d, k), set()).add(target == me)
    offsets.discard((0, 0))
    reach = max(min(db, n_box - db) for db, _ in offsets)
    return sorted(offsets), reach, same


def kernel(
    n_box, n_lev, slots, fields, edge,
    owner_far, count_far, fine_far, coarse_far, updated, window,
    owner_of, count, fine, coarse, avg, own_got, send1, recv1, region_out, near_in,
    upd, corner_lines, corner_region, side_out, side_in, z_out, z_in, corner_out, corner_in, place_table,
    small, load, put, s1, r1, sh, rh, s3, r3, mixed,
):
    fine_edge = 2 * edge
    block = fields * edge
    plane = edge * edge
    lay = Layout(fields, edge)
    frows = fields * fine_edge
    cut = (fields + 1) // 2
    chunks = ((0, cut), (cut, fields))
    small_loads = [
        pltpu.make_async_copy(src, dst, small.at[i])
        for i, (src, dst) in enumerate(((owner_far, owner_of), (count_far, count)))
    ]
    for copy in small_loads:
        copy.start()
    all_rows = slots * frows
    loads = {}
    for part, (f0, f1) in enumerate(chunks):
        for s in range(slots):
            start, size = s * frows + f0 * fine_edge, (f1 - f0) * fine_edge
            for t in range(8):
                copy = pltpu.make_async_copy(
                    fine_far.at[pl.ds(start, size), pl.ds(t * LANES, LANES)],
                    fine.at[pl.ds(t * all_rows + start, size)],
                    load.at[part],
                )
                copy.start()
        rows = fine.at[pl.ds(0, 8 * slots * (f1 - f0) * fine_edge)]
        loads[part] = pltpu.make_async_copy(rows, rows, load.at[part])
    coarse_load = pltpu.make_async_copy(coarse_far, coarse, small.at[2])
    coarse_load.start()
    n_dev = n_box * n_lev
    offsets, reach, same = relations(n_box, n_lev)
    box = lax.axis_index("box")
    lev = lax.axis_index("lev")
    me = box * n_lev + lev

    def at(linear):
        return (lax.div(linear, n_lev), lax.rem(linear, n_lev))

    def shifted(by):
        return at(lax.rem(me + (by + n_dev), n_dev))

    def beside(dx, dy):
        return (lax.rem(box + (dx + n_box), n_box), lax.rem(lev + (dy + n_lev), n_lev))

    barrier = pltpu.get_barrier_semaphore()
    for db, dl in offsets:
        pl.semaphore_signal(barrier, inc=1, device_id=beside(db, dl), device_id_type=MESH_ID)

    q = iota((fine_edge * fine_edge, plane), 0)
    c = iota((fine_edge * fine_edge, plane), 1)
    goal = (q // (2 * fine_edge)) * edge + (q % fine_edge) // 2
    table = jnp.where(goal == c, 0.125, 0.0).astype(BF16)
    order = (1, 2, 0, 3)
    back = [shifted(-delta) for delta in DELTAS]

    def target_of(d, k):
        dx, dy = DIRECTIONS[d]
        other = beside(-dx, -dy)
        return at(lax.rem(other[0] * n_lev + other[1] + (n_dev - DELTAS[k]), n_dev))

    targets = [[target_of(d, k) for k in range(4)] for d in range(8)]

    def place_of(device):
        db = lax.rem(device[0] - box + (n_box + reach), n_box)
        return db * n_lev + lax.rem(device[1] - lev + n_lev, n_lev)

    for copy in small_loads:
        copy.wait()
    live_count = count[0]
    owner = [owner_of[0, s] for s in range(slots)]
    region_of = [owner_of[1, s] for s in range(slots)]
    chosen = [
        [(s < live_count) & (owner[s] == delta) for delta in DELTAS] for s in range(slots)
    ]
    weight = [[jnp.where(c, 1.0, 0.0).astype(F32) for c in row] for row in chosen]
    for k in range(4):
        region = jnp.int32(-1)
        for s in range(slots):
            region = jnp.where(chosen[s][k], region_of[s], region)
        region_out[k] = jnp.full((1, LANES), 1.0, F32) * region.astype(F32)

    near_in[reach * n_lev] = region_out[...]
    first = {}
    for part, (f0, f1) in enumerate(chunks):
        size = (f1 - f0) * edge
        loads[part].wait()
        columns = []
        for t in range(8):
            pieces = []
            for s in range(slots):
                start = t * all_rows + s * frows + f0 * fine_edge
                pieces.append(
                    fine[pl.ds(start, size, stride=2), :] + fine[pl.ds(start + 1, size, stride=2), :]
                )
            columns.append(jnp.concatenate(pieces, axis=0))
        high, low = split(jnp.concatenate(columns, axis=1))
        got = jnp.dot(jnp.concatenate([high, low], axis=0), table, preferred_element_type=F32)
        got = got[:slots * size] + got[slots * size:]
        to = f0 * edge
        for h in range(2):
            averaged = []
            for s in range(slots):
                mean = got[s * size:(s + 1) * size, h * LANES:(h + 1) * LANES]
                start = (h * slots + s) * block + to
                avg[start:start + size, :] = mean
                averaged.append(mean)
            for k in range(4):
                total = averaged[0] * weight[0][k]
                for s in range(1, slots):
                    total = total + averaged[s] * weight[s][k]
                send1[k, to:to + size, h * LANES:(h + 1) * LANES] = total
        if part == 0:
            pl.semaphore_wait(barrier, len(offsets))
            for db, dl in offsets:
                slot = ((reach - db) % n_box) * n_lev + (-dl) % n_lev
                copy = pltpu.make_async_remote_copy(
                    src_ref=region_out, dst_ref=near_in.at[slot],
                    send_sem=sh.at[0], recv_sem=rh.at[0],
                    device_id=beside(db, dl), device_id_type=MESH_ID,
                )
                copy.start()
        for k in order:
            copy = pltpu.make_async_remote_copy(
                src_ref=send1.at[k, pl.ds(to, size)], dst_ref=recv1.at[k, pl.ds(to, size)],
                send_sem=s1.at[0], recv_sem=r1.at[part],
                device_id=shifted(DELTAS[k]), device_id_type=MESH_ID,
            )
            copy.start()
        rows = recv1.at[:, pl.ds(to, size)]
        first[part] = pltpu.make_async_copy(rows, rows, r1.at[part])

    for pair in range(4):
        row = iota((LANES, 2 * LANES), 0)
        col = iota((LANES, 2 * LANES), 1)
        hit = (row // edge == 2 * pair + col // LANES) & (row % edge == col % edge)
        place_table[pair] = both(jnp.where(hit, 1.0, 0.0).astype(BF16))

    row = iota((plane, 4 * LANES), 0)
    col = iota((plane, 4 * LANES), 1)
    kind = col // LANES
    inner = col % edge
    fixed = jnp.where(kind % 2 == 0, 0, edge - 1)
    hit = jnp.where(kind < 2, fixed * edge + inner, inner * edge + fixed) == row
    own_table = jnp.where(hit, 1.0, 0.0).astype(BF16)
    high, low = split(jnp.concatenate(
        [avg[:slots * block, :], avg[slots * block:, :]], axis=1
    ))
    got = jnp.dot(high, own_table, preferred_element_type=F32) + jnp.dot(
        low, own_table, preferred_element_type=F32
    )
    for kind in range(4):
        own_got[kind * slots * block:(kind + 1) * slots * block, :] = got[
            :, kind * LANES:(kind + 1) * LANES
        ]
    group_f = iota((fields, LANES), 1) // edge
    for s in range(slots):
        for h in range(2):
            for side in range(2):
                start = (h * slots + s) * block + side * (edge - 1)
                to = lay.own + (2 * side + h) * fields
                window[s, to:to + fields, :] = avg[pl.ds(start, fields, stride=edge), :]
            for kind in range(4):
                total = jnp.zeros((fields, LANES), F32)
                for i in range(8):
                    start = (kind * slots + s) * block + h * 8 + i
                    part = own_got[pl.ds(start, fields, stride=edge), :]
                    total = jnp.where(group_f == i, part, total)
                to = lay.own + (2 * (2 + kind) + h) * fields
                window[s, to:to + fields, :] = total

        live = jnp.where(s < live_count, 1.0, 0.0).astype(F32)
        window[s, lay.keep:lay.keep + 1, :] = jnp.full((1, LANES), 1.0, F32) * live
    corner_lines[...] = jnp.zeros_like(corner_lines)
    coarse_load.wait()
    told = near_in.at[pl.ds(0, len(offsets))]
    pltpu.make_async_copy(told, told, rh.at[0]).wait()

    lane = iota((1, LANES), 1).astype(F32)
    here_rows = [near_in[place_of(back[k]), k] for k in range(4)]
    near = [[near_in[place_of(targets[d][k]), k] for k in range(4)] for d in range(8)]

    def pick(region, place):
        t = lane - edge * region - place
        return jnp.where((t == 0.0) | (t == LANES) | (t == -LANES), 1.0, 0.0)

    z_rows = []
    for depth in range(2):
        for k in range(4):
            for place in (-1 - depth, edge + depth):
                z_rows.append(pick(here_rows[k], place))
    for d in range(2):
        for place in (-1, edge):
            for k in range(4):
                z_rows.append(pick(near[d][k], place))
    z_table = jnp.concatenate(z_rows, axis=0).astype(BF16)
    z_table = jnp.concatenate([z_table, z_table], axis=1)
    for corner in range(4):
        for k in range(4):
            corner_region[k, corner:corner + 1, :] = near[4 + corner][k]

    group = (iota((1, LANES), 1) // edge).astype(F32)
    here = [group == region for region in here_rows]
    group8 = iota((SUB, LANES), 1) // edge
    end_lines = [jnp.zeros((SUB, LANES), F32) for _ in range(2)]
    for part, (f0, f1) in enumerate(chunks):
        size = (f1 - f0) * edge
        first[part].wait()
        to = f0 * edge
        for h in range(2):
            stacked = split_lanes(jnp.concatenate(
                [recv1[k, to:to + size, h * LANES:(h + 1) * LANES] for k in range(4)], axis=0
            ))
            for pair in range(4):
                spread = jnp.dot(stacked, place_table[pair], preferred_element_type=F32)
                for odd in range(2):
                    y = h * SUB + 2 * pair + odd
                    for f in range(f0, f1):
                        merged = coarse[pl.ds(f * plane + y, edge, stride=edge), :]
                        for k in range(4):
                            start = k * size + (f - f0) * edge
                            merged = jnp.where(
                                here[k],
                                spread[start:start + edge, odd * LANES:(odd + 1) * LANES],
                                merged,
                            )
                        upd[pl.ds(f * lay.field + y, edge, stride=edge), :] = merged
        for f in range(f0, f1):
            pltpu.make_async_copy(
                upd.at[pl.ds(f * lay.field, plane)], updated.at[pl.ds(f * plane, plane)], put.at[0]
            ).start()
        for f in range(f0, f1):
            start = f * lay.field
            got = times_transposed(z_table, split_lanes(upd[start:start + plane, :]))
            for depth in range(2):
                for h in range(2):
                    z_out[pl.ds((2 * depth + h) * fields + f, 8, stride=4 * fields), :] = got[
                        depth * 8:(depth + 1) * 8, h * LANES:(h + 1) * LANES
                    ]
            high_end = got[16:24, LANES:]
            if f:
                high_end = pltpu.roll(high_end, LANES - f * edge, 1)
            low_end = pltpu.roll(got[24:32, :LANES], LANES - (f + 1) * edge, 1)
            end_lines[0] = jnp.where(group8 == 7 - f, high_end, end_lines[0])
            end_lines[1] = jnp.where(group8 == 7 - f, low_end, end_lines[1])

    clear, unclear = [0, 0, 0], []

    def send(src, dst, sem, d, k, target):
        kinds = {False} if d is None else same[d, k]
        remote = local = None
        if False in kinds:
            remote = pltpu.make_async_remote_copy(
                src_ref=src, dst_ref=dst, recv_sem=r3.at[sem], device_id=target, device_id_type=MESH_ID,
                send_sem=s3.at[sem] if len(kinds) == 1 else mixed.at[len(unclear)],
            )
        if True in kinds:
            local = pltpu.make_async_copy(src, dst, r3.at[sem])
        if local is None:
            remote.start()
            clear[sem] += 1
        elif remote is None:
            local.start()
        else:
            itself = (target[0] == box) & (target[1] == lev)
            pl.when(itself)(local.start)
            pl.when(jnp.logical_not(itself))(remote.start)
            unclear.append((remote, itself))

    for k in order:
        send(z_out.at[pl.ds(k * lay.z_size, lay.z_size)], z_in.at[k], 0, None, k, back[k])

    field_step = lay.field
    sublane = iota((SUB, LANES), 0)
    in_group = iota((SUB, LANES), 1) % edge
    for d in (0, 1, 2, 3):
        outer, inner = (edge, 1) if d < 2 else (1, edge)
        adjacent = edge - 1 if d % 2 == 0 else 0
        far = edge - 2 if d % 2 == 0 else 1
        lines = []
        for i in range(8):
            lines.append(jnp.concatenate([
                upd[pl.ds(level * outer + (h * 8 + i) * inner, SUB, stride=field_step), :]
                for level in (adjacent, far) for h in range(2)
            ], axis=0))
        by_region = transposed_groups(lines, edge)
        ends = []
        for g in range(8):
            before = by_region[(g + 7) % 8][:2 * SUB]
            after = by_region[(g + 1) % 8][:2 * SUB]
            ends.append(jnp.where(iota((2 * SUB, LANES), 1) % edge == 0, after, before))
        for k in range(4):
            region = near[d][k]
            total = by_region[0]
            end = ends[0]
            for g in range(1, 8):
                hit = region == float(g)
                total = jnp.where(hit, by_region[g], total)
                end = jnp.where(hit, ends[g], end)
            base = (d * 4 + k) * lay.side
            for part in range(4):
                side_out[base + part * fields:base + (part + 1) * fields, :] = total[
                    part * SUB:part * SUB + fields, :
                ]
            for h in range(2):
                used = (sublane < fields) & ((in_group == 0) | (in_group == edge - 1))
                one = jnp.where(used, end[h * SUB:(h + 1) * SUB, :], 0.0)
                moved = one
                for f in range(1, fields):
                    moved = jnp.where(sublane == f, pltpu.roll(one, LANES - 2 * f, 1), moved)
                one = moved
                side_out[base + lay.ends + h:base + lay.ends + h + 1, :] = jnp.sum(
                    one, axis=0, keepdims=True
                )
        if d < 2:
            for e in range(2):
                side_out[pl.ds(d * 4 * lay.side + lay.ends + 2 + e, 4, stride=lay.side), :] = (
                    end_lines[d][e * 4:(e + 1) * 4, :]
                )
        else:
            for e in range(2):
                side_out[pl.ds(d * 4 * lay.side + lay.ends + 2 + e, 4, stride=lay.side), :] = (
                    jnp.zeros((4, LANES), F32)
                )

        if d % 2:
            for near_d in (d - 1, d):
                for k in order:
                    send(
                        side_out.at[pl.ds((near_d * 4 + k) * lay.side, lay.side)],
                        side_in.at[k, near_d], 1, near_d, k, targets[near_d][k],
                    )

    for f in range(fields):
        for corner in range(4):
            x = 0 if corner // 2 else edge - 1
            y = 0 if corner % 2 else edge - 1
            start = f * lay.field + x * edge + y
            corner_lines[7 - f, corner:corner + 1, :] = upd[start:start + 1, :]
    by_region = transposed_groups([corner_lines[f] for f in range(8)], edge)
    for k in range(4):
        region = corner_region[k]
        total = by_region[0]
        for g in range(1, 8):
            total = jnp.where(region == float(g), by_region[g], total)
        for corner in range(4):
            corner_out[corner * 4 + k] = total[corner:corner + 1, :]
    for corner in range(4):
        for k in order:
            send(
                corner_out.at[corner * 4 + k], corner_in.at[k * 4 + corner],
                2, 4 + corner, k, targets[4 + corner][k],
            )

    for sem, ref in enumerate((z_in, side_in, corner_in)):
        pltpu.make_async_copy(ref, ref, r3.at[sem]).wait()
    for s in range(slots):
        k = owner[s] + 2 - jnp.where(owner[s] > 0, 1, 0)
        for d in range(4):
            window[s, d * lay.side:(d + 1) * lay.side, :] = side_in[k, d]
        window[s, lay.z:lay.z + lay.z_size, :] = z_in[k]
        for corner in range(4):
            window[s, lay.corner + corner:lay.corner + corner + 1, :] = corner_in[k * 4 + corner]

    pltpu.make_async_copy(updated, updated, put.at[0]).wait()
    pltpu.make_async_copy(send1, send1, s1.at[0]).wait()
    told = near_in.at[pl.ds(0, len(offsets))]
    pltpu.make_async_copy(told, told, sh.at[0]).wait()
    for sem, (ref, size) in enumerate(((z_out, lay.z_size), (side_out, lay.side), (corner_out, 1))):
        if clear[sem]:
            rows = ref.at[pl.ds(0, clear[sem] * size)]
            pltpu.make_async_copy(rows, rows, s3.at[sem]).wait()
    for remote, itself in unclear:
        pl.when(jnp.logical_not(itself))(remote.wait_send)


def ghost_kernel(
    slots, fields, edge, mask_far, updated_in, window, updated_out, ghost_out,
    mask, passing, ghost, table, lhs, mask_sem, pass_sem, out_sem,
):
    lay = Layout(fields, edge)
    into = pltpu.make_async_copy(updated_in, passing, pass_sem.at[0])
    out = pltpu.make_async_copy(passing, updated_out, pass_sem.at[1])
    mask_load = pltpu.make_async_copy(mask_far, mask, mask_sem.at[0])
    mask_load.start()
    into.start()

    table[...] = jnp.zeros_like(table)
    cell_row = iota((edge, LANES), 0)
    col = iota((edge, LANES), 1)
    quarter = 2 * edge
    for kind in range(3):
        target = (col % 64) // 4 if kind == 2 else (col % quarter) // 2
        along = (col // quarter) % 2 if kind == 0 else col // 64
        within = (col // 2) % 2 if kind == 2 else col % 2
        step = cell_row - target
        alike = step == 0

        def signed(sign, where):
            return jnp.where(where, jnp.where(sign == 1, 0.125, -0.125), 0.0)

        centre = jnp.where(alike, 1.0, signed(within, step == 1) - signed(within, step == -1))
        ends = signed(within, step == 1 - edge) - signed(within, step == edge - 1)
        slope = signed(along, alike)
        for odd in range(2):
            for line in range(2):
                block = 2 * odd + line
                for column in range(2):
                    if kind == 0:
                        normal = jnp.where(alike, 0.125 if column else -0.125, 0.0)
                        used = col // 64 == line
                    else:
                        normal = signed(col % 2 if kind == 2 else (col // quarter) % 2, alike)
                        used = None if column == line else False
                    if used is False:
                        continue
                    for part, value in enumerate((centre, slope, normal, ends)):
                        if used is not None:
                            value = jnp.where(used, value, 0.0)
                        row = (part % 2) * LANES + (odd * 4 + (part // 2) * 2 + line) * edge
                        to = (2 * odd + column) * LANES
                        table[kind, row:row + edge, to:to + LANES] = value.astype(BF16)

    lane = iota((SUB, LANES), 1)
    in_group = lane % edge
    last_lane, first_lane = lane >= LANES - edge, lane < edge

    for s in range(slots):
        def rows(start, size=SUB):
            return window[s, start:start + size, :]

        def spread(start, shift, stride):
            row = jnp.broadcast_to(rows(start, 1), (SUB, LANES))
            return pltpu.roll(row, shift % LANES, 1, stride=stride, stride_axis=0)

        for kind in range(3):
            parts = [[] for _ in range(8)]
            for side in range(2):
                face = 2 * kind + side
                base = face * lay.side if kind < 2 else lay.z + side * 4 * fields
                layers = [rows(base + h * fields) for h in range(4)]
                centre, far = layers[:2], layers[2:]
                own = [rows(lay.own + (2 * face + h) * fields) for h in range(2)]
                if kind == 0:
                    lines = [lay.corner + 2 * side, lay.corner + 2 * side + 1]
                elif kind == 1:
                    lines = [lay.corner + side, lay.corner + 2 + side]
                else:
                    lines = [d * lay.side + lay.ends + 2 + side for d in range(2)]
                below = spread(lines[0], edge, edge)
                above = spread(lines[1], 0, edge)
                up = [pltpu.roll(v, LANES - edge, 1) for v in centre]
                down = [pltpu.roll(v, edge, 1) for v in centre]
                along = [
                    jnp.where(last_lane, up[1], up[0]) - jnp.where(first_lane, below, down[0]),
                    jnp.where(last_lane, above, up[1]) - jnp.where(first_lane, down[0], down[1]),
                ]
                for h in range(2):
                    if kind < 2:
                        before = after = spread(base + lay.ends + h, 0, 2)
                    else:
                        low_row, high_row = 2 * lay.side + lay.ends + h, 3 * lay.side + lay.ends + h
                        before = spread(low_row, edge - 1 if side else 0, 2)
                        after = spread(high_row, 0 if side else 1 - edge, 2)
                    end = jnp.where(in_group == edge - 1, before, jnp.where(in_group == 0, after, 0.0))
                    normal = own[h] - far[h] if side == 0 else far[h] - own[h]
                    for part, values in enumerate((centre[h], along[h], normal, end)):
                        parts[h * 4 + part].append(values)
            groups = transposed_groups([jnp.concatenate(v, axis=0) for v in parts], edge, (4, 2))
            for pair in range(4):
                high, low = split(jnp.concatenate(groups[2 * pair:2 * pair + 2], axis=1))
                lhs[s * 3 + kind, pair * 16:(pair + 1) * 16, :] = high
                lhs[s * 3 + kind, 64 + pair * 16:64 + (pair + 1) * 16, :] = low

    into.wait()
    out.start()
    mask_load.wait()
    for s in range(slots):
        live = window[s, lay.keep:lay.keep + 1, :]
        for kind in range(3):
            both_parts = jnp.dot(lhs[s * 3 + kind], table[kind], preferred_element_type=F32)
            spreads = both_parts[:64] + both_parts[64:]
            for side in range(2):
                face = 2 * kind + side
                keep = live * jnp.where(mask[s, face] > 0, 1.0, 0.0).astype(F32)
                for pair in range(4):
                    for block in range(4):
                        start = pair * 16 + side * SUB
                        value = spreads[start:start + SUB, block * LANES:(block + 1) * LANES] * keep
                        h, column = block // 2, block % 2
                        tile = column * 8 + h * 4 + pair if kind == 0 else h * 8 + pair * 2 + column
                        ghost[s, :, face, tile * LANES:(tile + 1) * LANES] = value[:fields]
        pltpu.make_async_copy(
            ghost.at[s, :, :, pl.ds(0, ghost_out.shape[3])], ghost_out.at[s], out_sem.at[0]
        ).start()
    out.wait()
    pltpu.make_async_copy(ghost_out, ghost_out, out_sem.at[0]).wait()


def body(n_box, n_lev, fine, coarse, owner_map, patch_count, face_mask):
    slots, fields, fine_edge, _ = fine.shape
    edge = fine_edge // 2
    block = fields * edge
    lay = Layout(fields, edge)
    offsets, reach, same = relations(n_box, n_lev)
    far = pl.BlockSpec(memory_space=pl.ANY)
    vmem = pl.BlockSpec(memory_space=pltpu.VMEM)
    flat = jax.ShapeDtypeStruct((block * edge, LANES), F32)
    places = (2 * reach + 1) * n_lev
    owner_rows = owner_map.T
    updated, window = pl.pallas_call(
        functools.partial(kernel, n_box, n_lev, slots, fields, edge),
        out_shape=(
            flat,
            jax.ShapeDtypeStruct((slots, lay.rows, LANES), F32),
        ),
        in_specs=[far] * 4,
        out_specs=(far, vmem),
        scratch_shapes=[
            pltpu.SMEM(owner_rows.shape, jnp.int32),
            pltpu.SMEM(patch_count.shape, jnp.int32),
            pltpu.VMEM((8 * slots * fields * fine_edge, LANES), F32),
            pltpu.VMEM((block * edge, LANES), F32),
            pltpu.VMEM((2 * slots * block, LANES), F32),
            pltpu.VMEM((4 * slots * block, LANES), F32),
            pltpu.VMEM((4, block, 2 * LANES), F32),
            pltpu.VMEM((4, block, 2 * LANES), F32),
            pltpu.VMEM((4, 1, LANES), F32),
            pltpu.VMEM((places, 4, 1, LANES), F32),
            pltpu.VMEM((SUB * lay.field, LANES), F32),
            pltpu.VMEM((SUB, SUB, LANES), F32),
            pltpu.VMEM((4, SUB, LANES), F32),
            pltpu.VMEM((16 * lay.side, LANES), F32),
            pltpu.VMEM((4, 4, lay.side, LANES), F32),
            pltpu.VMEM((4 * lay.z_size, LANES), F32),
            pltpu.VMEM((4, lay.z_size, LANES), F32),
            pltpu.VMEM((16, 1, LANES), F32),
            pltpu.VMEM((16, 1, LANES), F32),
            pltpu.VMEM((4, 2 * LANES, 2 * LANES), BF16),
            pltpu.SemaphoreType.DMA((3,)),
            pltpu.SemaphoreType.DMA((2,)),
            pltpu.SemaphoreType.DMA((1,)),
            pltpu.SemaphoreType.DMA((1,)),
            pltpu.SemaphoreType.DMA((2,)),
            pltpu.SemaphoreType.DMA((1,)),
            pltpu.SemaphoreType.DMA((1,)),
            pltpu.SemaphoreType.DMA((3,)),
            pltpu.SemaphoreType.DMA((3,)),
            pltpu.SemaphoreType.DMA((max(1, sum(len(v) > 1 for v in same.values())),)),
        ],
        compiler_params=pltpu.CompilerParams(
            collective_id=0, has_side_effects=True, vmem_limit_bytes=VMEM_FIRST
        ),
    )(
        owner_rows, patch_count,
        fine.reshape(slots * fields * fine_edge, fine_edge * fine_edge),
        coarse.reshape(block * edge, LANES),
    )
    ghost_shape = (slots, fields, 6, 2 * fine_edge * fine_edge)
    updated, ghost = pl.pallas_call(
        functools.partial(ghost_kernel, slots, fields, edge),
        out_shape=(flat, jax.ShapeDtypeStruct(ghost_shape, F32)),
        in_specs=[far, far, vmem],
        out_specs=(far, far),
        scratch_shapes=[
            pltpu.SMEM(face_mask.shape, jnp.int32),
            pltpu.VMEM((block * edge, LANES), F32),
            pltpu.VMEM((*ghost_shape[:3], ghost_shape[3] + LANES), F32),
            pltpu.VMEM((3, 2 * LANES, 4 * LANES), BF16),
            pltpu.VMEM((3 * slots, LANES, 2 * LANES), BF16),
            pltpu.SemaphoreType.DMA((1,)),
            pltpu.SemaphoreType.DMA((2,)),
            pltpu.SemaphoreType.DMA((1,)),
        ],
        compiler_params=pltpu.CompilerParams(vmem_limit_bytes=VMEM_SECOND),
    )(face_mask, updated, window)
    return updated.reshape(coarse.shape), ghost.transpose(0, 2, 1, 3)


def solution(mesh):
    return jax.shard_map(
        functools.partial(body, mesh.shape["box"], mesh.shape["lev"]),
        mesh=mesh,
        in_specs=(
            P(("box", "lev"), None, None, None),
            P(None, "box", "lev", None),
            P(("box", "lev"), None),
            P(("box", "lev")),
            P(("box", "lev"), None),
        ),
        out_specs=(P(None, "box", "lev", None), P(("box", "lev"), None, None, None)),
        check_vma=False,
    )
```

```python
import functools

import jax
import jax.numpy as jnp
from jax import lax
from jax.experimental import pallas as pl
from jax.experimental.pallas import tpu as pltpu
from jax.sharding import PartitionSpec as P

DELTAS = (-2, -1, 1, 2)
LANES = 128
SUB = 8
F32 = jnp.float32
BF16 = jnp.bfloat16
MESH_ID = pl.DeviceIdType.MESH
VMEM_FIRST = 56000000
VMEM_SECOND = 56000000


def iota(shape, dim):
    return lax.broadcasted_iota(jnp.int32, shape, dim)


def split(values):
    high = values.astype(BF16)
    return high, (values - high.astype(F32)).astype(BF16)


def split_lanes(values):
    return jnp.concatenate(split(values), axis=1)


def times_transposed(left, right):
    return lax.dot_general(left, right, (((1,), (1,)), ((), ())), preferred_element_type=F32)


def both(table):
    return jnp.concatenate([table, table], axis=0)


def transposed_groups(arrays, edge, bits=(4, 2, 1)):
    out = list(arrays)
    group = iota(out[0].shape, 1) // edge
    for bit in bits:
        low = (group // bit) % 2 == 0
        for i in range(8):
            if i & bit == 0:
                a, b = out[i], out[i + bit]
                out[i] = jnp.where(low, a, pltpu.roll(b, bit * edge, 1))
                out[i + bit] = jnp.where(low, pltpu.roll(a, LANES - bit * edge, 1), b)
    return out


class Layout:
    def __init__(self, fields, edge):
        self.ends = 4 * fields
        self.side = 4 * fields + 4
        self.z_size = 8 * fields
        self.z = 4 * self.side
        self.corner = self.z + self.z_size
        self.own = self.corner + 4
        self.keep = self.own + 12 * fields
        self.rows = self.keep + 1
        self.rows = self.rows + (-self.rows) % SUB
        self.field = edge * edge + SUB


DIRECTIONS = ((-1, 0), (1, 0), (0, -1), (0, 1), (-1, -1), (-1, 1), (1, -1), (1, 1))


def relations(n_box, n_lev):
    n_dev = n_box * n_lev
    offsets, same = set(), {}
    for me in range(n_dev):
        box, lev = divmod(me, n_lev)

        def add(other):
            db, dl = (other // n_lev - box) % n_box, (other % n_lev - lev) % n_lev
            offsets.add((db, dl))
            offsets.add((-db % n_box, -dl % n_lev))

        for delta in DELTAS:
            add((me + delta) % n_dev)
        for d, (dx, dy) in enumerate(DIRECTIONS):
            owner = ((box - dx) % n_box) * n_lev + (lev - dy) % n_lev
            add(owner)
            for k, delta in enumerate(DELTAS):
                target = (owner - delta) % n_dev
                add(target)
                same.setdefault((d, k), set()).add(target == me)
    offsets.discard((0, 0))
    reach = max(min(db, n_box - db) for db, _ in offsets)
    return sorted(offsets), reach, same


def kernel(
    n_box, n_lev, slots, fields, edge,
    owner_far, count_far, fine_far, coarse_far, updated, window,
    owner_of, count, fine, coarse, avg, own_got, send1, recv1, region_out, near_in,
    upd, side_table, corner_lines, corner_region, side_out, side_in, z_out, z_in, corner_out, corner_in, place_table,
    small, load, put, s1, r1, sh, rh, s3, r3, mixed,
):
    fine_edge = 2 * edge
    block = fields * edge
    plane = edge * edge
    lay = Layout(fields, edge)
    frows = fields * fine_edge
    cut = (fields + 1) // 2
    chunks = ((0, cut), (cut, fields))
    n_dev = n_box * n_lev
    offsets, reach, same = relations(n_box, n_lev)
    box = lax.axis_index("box")
    lev = lax.axis_index("lev")
    me = box * n_lev + lev

    def at(linear):
        return (lax.div(linear, n_lev), lax.rem(linear, n_lev))

    def shifted(by):
        return at(lax.rem(me + (by + n_dev), n_dev))

    def beside(dx, dy):
        return (lax.rem(box + (dx + n_box), n_box), lax.rem(lev + (dy + n_lev), n_lev))

    barrier = pltpu.get_barrier_semaphore()
    for db, dl in offsets:
        pl.semaphore_signal(barrier, inc=1, device_id=beside(db, dl), device_id_type=MESH_ID)

    small_loads = [
        pltpu.make_async_copy(src, dst, small.at[i])
        for i, (src, dst) in enumerate(((owner_far, owner_of), (count_far, count)))
    ]
    for copy in small_loads:
        copy.start()
    all_rows = slots * frows
    loads = {}
    for part, (f0, f1) in enumerate(chunks):
        for s in range(slots):
            start, size = s * frows + f0 * fine_edge, (f1 - f0) * fine_edge
            for t in range(8):
                copy = pltpu.make_async_copy(
                    fine_far.at[pl.ds(start, size), pl.ds(t * LANES, LANES)],
                    fine.at[pl.ds(t * all_rows + start, size)],
                    load.at[part],
                )
                copy.start()
        rows = fine.at[pl.ds(0, 8 * slots * (f1 - f0) * fine_edge)]
        loads[part] = pltpu.make_async_copy(rows, rows, load.at[part])
    coarse_load = pltpu.make_async_copy(coarse_far, coarse, small.at[2])
    coarse_load.start()
    q = iota((fine_edge * fine_edge, plane), 0)
    c = iota((fine_edge * fine_edge, plane), 1)
    goal = (q // (2 * fine_edge)) * edge + (q % fine_edge) // 2
    table = jnp.where(goal == c, 0.125, 0.0).astype(BF16)
    order = (1, 2, 0, 3)
    back = [shifted(-delta) for delta in DELTAS]

    def target_of(d, k):
        dx, dy = DIRECTIONS[d]
        other = beside(-dx, -dy)
        return at(lax.rem(other[0] * n_lev + other[1] + (n_dev - DELTAS[k]), n_dev))

    targets = [[target_of(d, k) for k in range(4)] for d in range(8)]

    def place_of(device):
        db = lax.rem(device[0] - box + (n_box + reach), n_box)
        return db * n_lev + lax.rem(device[1] - lev + n_lev, n_lev)

    for copy in small_loads:
        copy.wait()
    live_count = count[0]
    owner = [owner_of[0, s] for s in range(slots)]
    region_of = [owner_of[1, s] for s in range(slots)]
    chosen = [
        [(s < live_count) & (owner[s] == delta) for delta in DELTAS] for s in range(slots)
    ]
    weight = [[jnp.where(c, 1.0, 0.0).astype(F32) for c in row] for row in chosen]
    for k in range(4):
        region = jnp.int32(-1)
        for s in range(slots):
            region = jnp.where(chosen[s][k], region_of[s], region)
        region_out[k] = jnp.full((1, LANES), 1.0, F32) * region.astype(F32)

    near_in[reach * n_lev] = region_out[...]
    first = {}
    for part, (f0, f1) in enumerate(chunks):
        size = (f1 - f0) * edge
        loads[part].wait()
        columns = []
        for t in range(8):
            pieces = []
            for s in range(slots):
                start = t * all_rows + s * frows + f0 * fine_edge
                pieces.append(
                    fine[pl.ds(start, size, stride=2), :] + fine[pl.ds(start + 1, size, stride=2), :]
                )
            columns.append(jnp.concatenate(pieces, axis=0))
        high, low = split(jnp.concatenate(columns, axis=1))
        got = jnp.dot(jnp.concatenate([high, low], axis=0), table, preferred_element_type=F32)
        got = got[:slots * size] + got[slots * size:]
        to = f0 * edge
        for h in range(2):
            averaged = []
            for s in range(slots):
                mean = got[s * size:(s + 1) * size, h * LANES:(h + 1) * LANES]
                start = (h * slots + s) * block + to
                avg[start:start + size, :] = mean
                averaged.append(mean)
            for k in range(4):
                total = averaged[0] * weight[0][k]
                for s in range(1, slots):
                    total = total + averaged[s] * weight[s][k]
                send1[k, to:to + size, h * LANES:(h + 1) * LANES] = total

    pl.semaphore_wait(barrier, len(offsets))
    for db, dl in offsets:
        slot = ((reach - db) % n_box) * n_lev + (-dl) % n_lev
        pltpu.make_async_remote_copy(
            src_ref=region_out, dst_ref=near_in.at[slot], send_sem=sh.at[0], recv_sem=rh.at[0],
            device_id=beside(db, dl), device_id_type=MESH_ID,
        ).start()
    for part, (f0, f1) in enumerate(chunks):
        to, size = f0 * edge, (f1 - f0) * edge
        for k in order:
            pltpu.make_async_remote_copy(
                src_ref=send1.at[k, pl.ds(to, size)], dst_ref=recv1.at[k, pl.ds(to, size)],
                send_sem=s1.at[0], recv_sem=r1.at[part],
                device_id=shifted(DELTAS[k]), device_id_type=MESH_ID,
            ).start()
        rows = recv1.at[:, pl.ds(to, size)]
        first[part] = pltpu.make_async_copy(rows, rows, r1.at[part])

    for pair in range(4):
        row = iota((LANES, 2 * LANES), 0)
        col = iota((LANES, 2 * LANES), 1)
        hit = (row // edge == 2 * pair + col // LANES) & (row % edge == col % edge)
        place_table[pair] = both(jnp.where(hit, 1.0, 0.0).astype(BF16))

    row = iota((plane, 4 * LANES), 0)
    col = iota((plane, 4 * LANES), 1)
    kind = col // LANES
    inner = col % edge
    fixed = jnp.where(kind % 2 == 0, 0, edge - 1)
    hit = jnp.where(kind < 2, fixed * edge + inner, inner * edge + fixed) == row
    own_table = jnp.where(hit, 1.0, 0.0).astype(BF16)
    high, low = split(jnp.concatenate(
        [avg[:slots * block, :], avg[slots * block:, :]], axis=1
    ))
    got = jnp.dot(high, own_table, preferred_element_type=F32) + jnp.dot(
        low, own_table, preferred_element_type=F32
    )
    for kind in range(4):
        own_got[kind * slots * block:(kind + 1) * slots * block, :] = got[
            :, kind * LANES:(kind + 1) * LANES
        ]
    group_f = iota((fields, LANES), 1) // edge
    for s in range(slots):
        for h in range(2):
            for side in range(2):
                start = (h * slots + s) * block + side * (edge - 1)
                to = lay.own + (2 * side + h) * fields
                window[s, to:to + fields, :] = avg[pl.ds(start, fields, stride=edge), :]
            for kind in range(4):
                total = jnp.zeros((fields, LANES), F32)
                for i in range(8):
                    start = (kind * slots + s) * block + h * 8 + i
                    part = own_got[pl.ds(start, fields, stride=edge), :]
                    total = jnp.where(group_f == i, part, total)
                to = lay.own + (2 * (2 + kind) + h) * fields
                window[s, to:to + fields, :] = total

        live = jnp.where(s < live_count, 1.0, 0.0).astype(F32)
        window[s, lay.keep:lay.keep + 1, :] = jnp.full((1, LANES), 1.0, F32) * live
    corner_lines[...] = jnp.zeros_like(corner_lines)
    coarse_load.wait()
    told = near_in.at[pl.ds(0, len(offsets))]
    pltpu.make_async_copy(told, told, rh.at[0]).wait()

    lane = iota((1, LANES), 1).astype(F32)
    here_rows = [near_in[place_of(back[k]), k] for k in range(4)]
    near = [[near_in[place_of(targets[d][k]), k] for k in range(4)] for d in range(8)]

    def pick(region, place):
        t = lane - edge * region - place
        return jnp.where((t == 0.0) | (t == LANES) | (t == -LANES), 1.0, 0.0)

    z_rows = []
    for depth in range(2):
        for k in range(4):
            for place in (-1 - depth, edge + depth):
                z_rows.append(pick(here_rows[k], place))
    for d in range(2):
        for place in (-1, edge):
            for k in range(4):
                z_rows.append(pick(near[d][k], place))
    z_table = jnp.concatenate(z_rows, axis=0).astype(BF16)
    z_table = jnp.concatenate([z_table, z_table], axis=1)
    z_cell = iota((LANES, LANES), 0).astype(F32)
    out_lane = iota((1, LANES), 1)
    inside = (out_lane % edge).astype(F32)
    outside = jnp.where(out_lane % 2 == 1, -1, edge).astype(F32)
    for d in (2, 3):
        for k in range(4):
            base = z_cell - edge * near[d][k]
            found = base == inside
            t = base - outside
            past = (t == 0.0) | (t == LANES) | (t == -LANES)
            for i, hit in enumerate((found, past)):
                side_table[d - 2, i, :, k * LANES:(k + 1) * LANES] = both(
                    jnp.where(hit, 1.0, 0.0).astype(BF16)
                )
    for corner in range(4):
        for k in range(4):
            corner_region[k, corner:corner + 1, :] = near[4 + corner][k]

    def z_fields(f0, f1):
        for f in range(f0, f1):
            start = f * lay.field
            got = times_transposed(z_table, split_lanes(upd[start:start + plane, :]))
            for depth in range(2):
                for h in range(2):
                    z_out[pl.ds((2 * depth + h) * fields + f, 8, stride=4 * fields), :] = got[
                        depth * 8:(depth + 1) * 8, h * LANES:(h + 1) * LANES
                    ]
            high_end = got[16:24, LANES:]
            if f:
                high_end = pltpu.roll(high_end, LANES - f * edge, 1)
            low_end = pltpu.roll(got[24:32, :LANES], LANES - (f + 1) * edge, 1)
            end_lines[0] = jnp.where(group8 == 7 - f, high_end, end_lines[0])
            end_lines[1] = jnp.where(group8 == 7 - f, low_end, end_lines[1])

    group = (iota((1, LANES), 1) // edge).astype(F32)
    here = [group == region for region in here_rows]
    group8 = iota((SUB, LANES), 1) // edge
    end_lines = [jnp.zeros((SUB, LANES), F32) for _ in range(2)]
    for part, (f0, f1) in enumerate(chunks):
        size = (f1 - f0) * edge
        first[part].wait()
        to = f0 * edge
        for h in range(2):
            stacked = split_lanes(jnp.concatenate(
                [recv1[k, to:to + size, h * LANES:(h + 1) * LANES] for k in range(4)], axis=0
            ))
            for pair in range(4):
                spread = jnp.dot(stacked, place_table[pair], preferred_element_type=F32)
                for odd in range(2):
                    y = h * SUB + 2 * pair + odd
                    for f in range(f0, f1):
                        merged = coarse[pl.ds(f * plane + y, edge, stride=edge), :]
                        for k in range(4):
                            start = k * size + (f - f0) * edge
                            merged = jnp.where(
                                here[k],
                                spread[start:start + edge, odd * LANES:(odd + 1) * LANES],
                                merged,
                            )
                        upd[pl.ds(f * lay.field + y, edge, stride=edge), :] = merged
        for f in range(f0, f1):
            pltpu.make_async_copy(
                upd.at[pl.ds(f * lay.field, plane)], updated.at[pl.ds(f * plane, plane)], put.at[0]
            ).start()
        if part == 0:
            z_fields(f0, f1)

    clear, unclear = [0, 0, 0], []

    def send(src, dst, sem, d, k, target):
        kinds = {False} if d is None else same[d, k]
        remote = local = None
        if False in kinds:
            remote = pltpu.make_async_remote_copy(
                src_ref=src, dst_ref=dst, recv_sem=r3.at[sem], device_id=target, device_id_type=MESH_ID,
                send_sem=s3.at[sem] if len(kinds) == 1 else mixed.at[len(unclear)],
            )
        if True in kinds:
            local = pltpu.make_async_copy(src, dst, r3.at[sem])
        if local is None:
            remote.start()
            clear[sem] += 1
        elif remote is None:
            local.start()
        else:
            itself = (target[0] == box) & (target[1] == lev)
            pl.when(itself)(local.start)
            pl.when(jnp.logical_not(itself))(remote.start)
            unclear.append((remote, itself))

    z_fields(*chunks[1])
    for k in order:
        send(z_out.at[pl.ds(k * lay.z_size, lay.z_size)], z_in.at[k], 0, None, k, back[k])
    field_step = lay.field
    sublane = iota((SUB, LANES), 0)
    in_group = iota((SUB, LANES), 1) % edge
    wide_group = iota((4 * SUB, LANES), 1) // edge
    turned = (iota((SUB, LANES), 1) + 2 * sublane) % LANES
    end_place = jnp.where(
        (sublane < fields) & ((turned % edge == 0) | (turned % edge == edge - 1)), turned // edge, -1
    )
    for d in (0, 1, 2, 3):
        outer, inner = (edge, 1) if d < 2 else (1, edge)
        adjacent = edge - 1 if d % 2 == 0 else 0
        far = edge - 2 if d % 2 == 0 else 1
        lines = []
        for i in range(8):
            lines.append(jnp.concatenate([
                upd[pl.ds(level * outer + (h * 8 + i) * inner, SUB, stride=field_step), :]
                for level in (adjacent, far) for h in range(2)
            ], axis=0))
        if d < 2:
            by_region = transposed_groups(lines, edge)
            ends = []
            for g in range(8):
                before = by_region[(g + 7) % 8][:2 * SUB]
                after = by_region[(g + 1) % 8][:2 * SUB]
                ends.append(jnp.where(iota((2 * SUB, LANES), 1) % edge == 0, after, before))
        else:
            wide = split_lanes(jnp.concatenate(lines, axis=0))
            ahead = split_lanes(jnp.concatenate([v[:2 * SUB] for v in lines], axis=0))
            cells = jnp.dot(wide, side_table[d - 2, 0], preferred_element_type=F32)
            beyond = jnp.dot(ahead, side_table[d - 2, 1], preferred_element_type=F32)
        for k in range(4):
            if d < 2:
                region = near[d][k]
                total = by_region[0]
                end = ends[0]
                for g in range(1, 8):
                    hit = region == float(g)
                    total = jnp.where(hit, by_region[g], total)
                    end = jnp.where(hit, ends[g], end)
                single = []
                for h in range(2):
                    used = (sublane < fields) & ((in_group == 0) | (in_group == edge - 1))
                    one = jnp.where(used, end[h * SUB:(h + 1) * SUB, :], 0.0)
                    moved = one
                    for f in range(1, fields):
                        moved = jnp.where(sublane == f, pltpu.roll(one, LANES - 2 * f, 1), moved)
                    single.append(moved)
            else:
                cols = slice(k * LANES, (k + 1) * LANES)
                total = cells[:4 * SUB, cols]
                for i in range(1, 8):
                    total = jnp.where(wide_group == i, cells[i * 4 * SUB:(i + 1) * 4 * SUB, cols], total)
                single = []
                for h in range(2):
                    moved = jnp.zeros((SUB, LANES), F32)
                    for i in range(8):
                        start = (2 * i + h) * SUB
                        moved = jnp.where(end_place == i, beyond[start:start + SUB, cols], moved)
                    single.append(moved)
            base = (d * 4 + k) * lay.side
            for part in range(4):
                side_out[base + part * fields:base + (part + 1) * fields, :] = total[
                    part * SUB:part * SUB + fields, :
                ]
            for h in range(2):
                side_out[base + lay.ends + h:base + lay.ends + h + 1, :] = jnp.sum(
                    single[h], axis=0, keepdims=True
                )
        if d < 2:
            for e in range(2):
                side_out[pl.ds(d * 4 * lay.side + lay.ends + 2 + e, 4, stride=lay.side), :] = (
                    end_lines[d][e * 4:(e + 1) * 4, :]
                )
        else:
            for e in range(2):
                side_out[pl.ds(d * 4 * lay.side + lay.ends + 2 + e, 4, stride=lay.side), :] = (
                    jnp.zeros((4, LANES), F32)
                )

        if d == 3:
            for near_d in range(4):
                for k in order:
                    send(
                        side_out.at[pl.ds((near_d * 4 + k) * lay.side, lay.side)],
                        side_in.at[k, near_d], 1, near_d, k, targets[near_d][k],
                    )

    for f in range(fields):
        for corner in range(4):
            x = 0 if corner // 2 else edge - 1
            y = 0 if corner % 2 else edge - 1
            start = f * lay.field + x * edge + y
            corner_lines[7 - f, corner:corner + 1, :] = upd[start:start + 1, :]
    by_region = transposed_groups([corner_lines[f] for f in range(8)], edge)
    for k in range(4):
        region = corner_region[k]
        total = by_region[0]
        for g in range(1, 8):
            total = jnp.where(region == float(g), by_region[g], total)
        for corner in range(4):
            corner_out[corner * 4 + k] = total[corner:corner + 1, :]
    for corner in range(4):
        for k in order:
            send(
                corner_out.at[corner * 4 + k], corner_in.at[k * 4 + corner],
                2, 4 + corner, k, targets[4 + corner][k],
            )

    for sem, ref in enumerate((z_in, side_in, corner_in)):
        pltpu.make_async_copy(ref, ref, r3.at[sem]).wait()
    for s in range(slots):
        k = owner[s] + 2 - jnp.where(owner[s] > 0, 1, 0)
        for d in range(4):
            window[s, d * lay.side:(d + 1) * lay.side, :] = side_in[k, d]
        window[s, lay.z:lay.z + lay.z_size, :] = z_in[k]
        for corner in range(4):
            window[s, lay.corner + corner:lay.corner + corner + 1, :] = corner_in[k * 4 + corner]

    pltpu.make_async_copy(updated, updated, put.at[0]).wait()
    pltpu.make_async_copy(send1, send1, s1.at[0]).wait()
    told = near_in.at[pl.ds(0, len(offsets))]
    pltpu.make_async_copy(told, told, sh.at[0]).wait()
    for sem, (ref, size) in enumerate(((z_out, lay.z_size), (side_out, lay.side), (corner_out, 1))):
        if clear[sem]:
            rows = ref.at[pl.ds(0, clear[sem] * size)]
            pltpu.make_async_copy(rows, rows, s3.at[sem]).wait()
    for remote, itself in unclear:
        pl.when(jnp.logical_not(itself))(remote.wait_send)


def ghost_kernel(
    slots, fields, edge, mask_far, updated_in, window, updated_out, ghost_out,
    mask, passing, ghost, table, lhs, mask_sem, pass_sem, out_sem,
):
    lay = Layout(fields, edge)
    into = pltpu.make_async_copy(updated_in, passing, pass_sem.at[0])
    out = pltpu.make_async_copy(passing, updated_out, pass_sem.at[1])
    mask_load = pltpu.make_async_copy(mask_far, mask, mask_sem.at[0])
    mask_load.start()
    into.start()

    table[...] = jnp.zeros_like(table)
    cell_row = iota((edge, LANES), 0)
    col = iota((edge, LANES), 1)
    quarter = 2 * edge
    for kind in range(3):
        target = (col % 64) // 4 if kind == 2 else (col % quarter) // 2
        along = (col // quarter) % 2 if kind == 0 else col // 64
        within = (col // 2) % 2 if kind == 2 else col % 2
        step = cell_row - target
        alike = step == 0

        def signed(sign, where):
            return jnp.where(where, jnp.where(sign == 1, 0.125, -0.125), 0.0)

        centre = jnp.where(alike, 1.0, signed(within, step == 1) - signed(within, step == -1))
        ends = signed(within, step == 1 - edge) - signed(within, step == edge - 1)
        slope = signed(along, alike)
        for odd in range(2):
            for line in range(2):
                block = 2 * odd + line
                for column in range(2):
                    if kind == 0:
                        normal = jnp.where(alike, 0.125 if column else -0.125, 0.0)
                        used = col // 64 == line
                    else:
                        normal = signed(col % 2 if kind == 2 else (col // quarter) % 2, alike)
                        used = None if column == line else False
                    if used is False:
                        continue
                    for part, value in enumerate((centre, slope, normal, ends)):
                        if used is not None:
                            value = jnp.where(used, value, 0.0)
                        row = (part % 2) * LANES + (odd * 4 + (part // 2) * 2 + line) * edge
                        to = (2 * odd + column) * LANES
                        table[kind, row:row + edge, to:to + LANES] = value.astype(BF16)

    lane = iota((SUB, LANES), 1)
    in_group = lane % edge
    last_lane, first_lane = lane >= LANES - edge, lane < edge

    def gather(s):
        def rows(start, size=SUB):
            return window[s, start:start + size, :]

        def spread(start, shift, stride):
            row = jnp.broadcast_to(rows(start, 1), (SUB, LANES))
            return pltpu.roll(row, shift % LANES, 1, stride=stride, stride_axis=0)

        for kind in range(3):
            parts = [[] for _ in range(8)]
            for side in range(2):
                face = 2 * kind + side
                base = face * lay.side if kind < 2 else lay.z + side * 4 * fields
                layers = [rows(base + h * fields) for h in range(4)]
                centre, far = layers[:2], layers[2:]
                own = [rows(lay.own + (2 * face + h) * fields) for h in range(2)]
                if kind == 0:
                    lines = [lay.corner + 2 * side, lay.corner + 2 * side + 1]
                elif kind == 1:
                    lines = [lay.corner + side, lay.corner + 2 + side]
                else:
                    lines = [d * lay.side + lay.ends + 2 + side for d in range(2)]
                below = spread(lines[0], edge, edge)
                above = spread(lines[1], 0, edge)
                up = [pltpu.roll(v, LANES - edge, 1) for v in centre]
                down = [pltpu.roll(v, edge, 1) for v in centre]
                along = [
                    jnp.where(last_lane, up[1], up[0]) - jnp.where(first_lane, below, down[0]),
                    jnp.where(last_lane, above, up[1]) - jnp.where(first_lane, down[0], down[1]),
                ]
                for h in range(2):
                    if kind < 2:
                        before = after = spread(base + lay.ends + h, 0, 2)
                    else:
                        low_row, high_row = 2 * lay.side + lay.ends + h, 3 * lay.side + lay.ends + h
                        before = spread(low_row, edge - 1 if side else 0, 2)
                        after = spread(high_row, 0 if side else 1 - edge, 2)
                    end = jnp.where(in_group == edge - 1, before, jnp.where(in_group == 0, after, 0.0))
                    normal = own[h] - far[h] if side == 0 else far[h] - own[h]
                    for part, values in enumerate((centre[h], along[h], normal, end)):
                        parts[h * 4 + part].append(values)
            groups = transposed_groups([jnp.concatenate(v, axis=0) for v in parts], edge, (4, 2))
            for pair in range(4):
                high, low = split(jnp.concatenate(groups[2 * pair:2 * pair + 2], axis=1))
                lhs[s * 3 + kind, pair * 16:(pair + 1) * 16, :] = high
                lhs[s * 3 + kind, 64 + pair * 16:64 + (pair + 1) * 16, :] = low

    def finish(s):
        live = window[s, lay.keep:lay.keep + 1, :]
        for kind in range(3):
            both_parts = jnp.dot(lhs[s * 3 + kind], table[kind], preferred_element_type=F32)
            spreads = both_parts[:64] + both_parts[64:]
            for side in range(2):
                face = 2 * kind + side
                keep = live * jnp.where(mask[s, face] > 0, 1.0, 0.0).astype(F32)
                for pair in range(4):
                    for block in range(4):
                        start = pair * 16 + side * SUB
                        value = spreads[start:start + SUB, block * LANES:(block + 1) * LANES] * keep
                        h, column = block // 2, block % 2
                        tile = column * 8 + h * 4 + pair if kind == 0 else h * 8 + pair * 2 + column
                        ghost[s, :, face, tile * LANES:(tile + 1) * LANES] = value[:fields]

    def send(s):
        pltpu.make_async_copy(
            ghost.at[s, :, :, pl.ds(0, ghost_out.shape[3])], ghost_out.at[s], out_sem.at[0]
        ).start()

    gather(0)
    mask_load.wait()
    for s in range(slots):
        if s + 1 < slots:
            gather(s + 1)
        finish(s)
        send(s)
        if s == 0:
            into.wait()
            out.start()
    out.wait()
    pltpu.make_async_copy(ghost_out, ghost_out, out_sem.at[0]).wait()


def body(n_box, n_lev, fine, coarse, owner_map, patch_count, face_mask):
    slots, fields, fine_edge, _ = fine.shape
    edge = fine_edge // 2
    block = fields * edge
    lay = Layout(fields, edge)
    offsets, reach, same = relations(n_box, n_lev)
    far = pl.BlockSpec(memory_space=pl.ANY)
    vmem = pl.BlockSpec(memory_space=pltpu.VMEM)
    flat = jax.ShapeDtypeStruct((block * edge, LANES), F32)
    places = (2 * reach + 1) * n_lev
    owner_rows = owner_map.T
    updated, window = pl.pallas_call(
        functools.partial(kernel, n_box, n_lev, slots, fields, edge),
        out_shape=(
            flat,
            jax.ShapeDtypeStruct((slots, lay.rows, LANES), F32),
        ),
        in_specs=[far] * 4,
        out_specs=(far, vmem),
        scratch_shapes=[
            pltpu.SMEM(owner_rows.shape, jnp.int32),
            pltpu.SMEM(patch_count.shape, jnp.int32),
            pltpu.VMEM((8 * slots * fields * fine_edge, LANES), F32),
            pltpu.VMEM((block * edge, LANES), F32),
            pltpu.VMEM((2 * slots * block, LANES), F32),
            pltpu.VMEM((4 * slots * block, LANES), F32),
            pltpu.VMEM((4, block, 2 * LANES), F32),
            pltpu.VMEM((4, block, 2 * LANES), F32),
            pltpu.VMEM((4, 1, LANES), F32),
            pltpu.VMEM((places, 4, 1, LANES), F32),
            pltpu.VMEM((SUB * lay.field, LANES), F32),
            pltpu.VMEM((2, 2, 2 * LANES, 4 * LANES), BF16),
            pltpu.VMEM((SUB, SUB, LANES), F32),
            pltpu.VMEM((4, SUB, LANES), F32),
            pltpu.VMEM((16 * lay.side, LANES), F32),
            pltpu.VMEM((4, 4, lay.side, LANES), F32),
            pltpu.VMEM((4 * lay.z_size, LANES), F32),
            pltpu.VMEM((4, lay.z_size, LANES), F32),
            pltpu.VMEM((16, 1, LANES), F32),
            pltpu.VMEM((16, 1, LANES), F32),
            pltpu.VMEM((4, 2 * LANES, 2 * LANES), BF16),
            pltpu.SemaphoreType.DMA((3,)),
            pltpu.SemaphoreType.DMA((2,)),
            pltpu.SemaphoreType.DMA((1,)),
            pltpu.SemaphoreType.DMA((1,)),
            pltpu.SemaphoreType.DMA((2,)),
            pltpu.SemaphoreType.DMA((1,)),
            pltpu.SemaphoreType.DMA((1,)),
            pltpu.SemaphoreType.DMA((3,)),
            pltpu.SemaphoreType.DMA((3,)),
            pltpu.SemaphoreType.DMA((max(1, sum(len(v) > 1 for v in same.values())),)),
        ],
        compiler_params=pltpu.CompilerParams(
            collective_id=0, has_side_effects=True, vmem_limit_bytes=VMEM_FIRST
        ),
    )(
        owner_rows, patch_count,
        fine.reshape(slots * fields * fine_edge, fine_edge * fine_edge),
        coarse.reshape(block * edge, LANES),
    )
    ghost_shape = (slots, fields, 6, 2 * fine_edge * fine_edge)
    updated, ghost = pl.pallas_call(
        functools.partial(ghost_kernel, slots, fields, edge),
        out_shape=(flat, jax.ShapeDtypeStruct(ghost_shape, F32)),
        in_specs=[far, far, vmem],
        out_specs=(far, far),
        scratch_shapes=[
            pltpu.SMEM(face_mask.shape, jnp.int32),
            pltpu.VMEM((block * edge, LANES), F32),
            pltpu.VMEM((*ghost_shape[:3], ghost_shape[3] + LANES), F32),
            pltpu.VMEM((3, 2 * LANES, 4 * LANES), BF16),
            pltpu.VMEM((3 * slots, LANES, 2 * LANES), BF16),
            pltpu.SemaphoreType.DMA((1,)),
            pltpu.SemaphoreType.DMA((2,)),
            pltpu.SemaphoreType.DMA((1,)),
        ],
        compiler_params=pltpu.CompilerParams(vmem_limit_bytes=VMEM_SECOND),
    )(face_mask, updated, window)
    return updated.reshape(coarse.shape), ghost.transpose(0, 2, 1, 3)


def solution(mesh):
    return jax.shard_map(
        functools.partial(body, mesh.shape["box"], mesh.shape["lev"]),
        mesh=mesh,
        in_specs=(
            P(("box", "lev"), None, None, None),
            P(None, "box", "lev", None),
            P(("box", "lev"), None),
            P(("box", "lev")),
            P(("box", "lev"), None),
        ),
        out_specs=(P(None, "box", "lev", None), P(("box", "lev"), None, None, None)),
        check_vma=False,
    )
```

```python
import functools

import jax
import jax.numpy as jnp
from jax import lax
from jax.experimental import pallas as pl
from jax.experimental.pallas import tpu as pltpu
from jax.sharding import PartitionSpec as P

DELTAS = (-2, -1, 1, 2)
LANES = 128
SUB = 8
F32 = jnp.float32
BF16 = jnp.bfloat16
MESH_ID = pl.DeviceIdType.MESH
VMEM_FIRST = 56000000
VMEM_SECOND = 56000000


def iota(shape, dim):
    return lax.broadcasted_iota(jnp.int32, shape, dim)


def split(values):
    high = values.astype(BF16)
    return high, (values - high.astype(F32)).astype(BF16)


def split_lanes(values):
    return jnp.concatenate(split(values), axis=1)


def times_transposed(left, right):
    return lax.dot_general(left, right, (((1,), (1,)), ((), ())), preferred_element_type=F32)


def both(table):
    return jnp.concatenate([table, table], axis=0)


def transposed_groups(arrays, edge, bits=(4, 2, 1)):
    out = list(arrays)
    group = iota(out[0].shape, 1) // edge
    for bit in bits:
        low = (group // bit) % 2 == 0
        for i in range(8):
            if i & bit == 0:
                a, b = out[i], out[i + bit]
                out[i] = jnp.where(low, a, pltpu.roll(b, bit * edge, 1))
                out[i + bit] = jnp.where(low, pltpu.roll(a, LANES - bit * edge, 1), b)
    return out


class Layout:
    def __init__(self, fields, edge):
        self.ends = 4 * fields
        self.side = 4 * fields + 4
        self.z_size = 8 * fields
        self.z = 4 * self.side
        self.corner = self.z + self.z_size
        self.own = self.corner + 4
        self.keep = self.own + 12 * fields
        self.rows = self.keep + 1
        self.rows = self.rows + (-self.rows) % SUB
        self.field = edge * edge + SUB


DIRECTIONS = ((-1, 0), (1, 0), (0, -1), (0, 1), (-1, -1), (-1, 1), (1, -1), (1, 1))


def relations(n_box, n_lev):
    n_dev = n_box * n_lev
    offsets, same, counts = set(), {}, (set(), set())
    for me in range(n_dev):
        box, lev = divmod(me, n_lev)

        def add(other):
            db, dl = (other // n_lev - box) % n_box, (other % n_lev - lev) % n_lev
            offsets.add((db, dl))
            offsets.add((-db % n_box, -dl % n_lev))

        for delta in DELTAS:
            add((me + delta) % n_dev)
        others = [0, 0]
        for d, (dx, dy) in enumerate(DIRECTIONS):
            owner = ((box - dx) % n_box) * n_lev + (lev - dy) % n_lev
            add(owner)
            for k, delta in enumerate(DELTAS):
                target = (owner - delta) % n_dev
                add(target)
                same.setdefault((d, k), set()).add(target == me)
                others[d // 4] += target != me
        for kind in range(2):
            counts[kind].add(others[kind])
    offsets.discard((0, 0))
    reach = max(min(db, n_box - db) for db, _ in offsets)
    return sorted(offsets), reach, same, counts


def kernel(
    n_box, n_lev, slots, fields, edge,
    owner_far, count_far, fine_far, coarse_far, updated, window,
    owner_of, count, fine, coarse, avg, own_got, send1, recv1, region_out, near_in,
    upd, side_table, corner_lines, corner_region, side_out, side_in, z_out, z_in, corner_out, corner_in, place_table,
    small, load, put, s1, r1, sh, rh, s3, r3, mixed,
):
    fine_edge = 2 * edge
    block = fields * edge
    plane = edge * edge
    lay = Layout(fields, edge)
    frows = fields * fine_edge
    cut = (fields + 1) // 2
    chunks = ((0, cut), (cut, fields))
    n_dev = n_box * n_lev
    offsets, reach, same, counts = relations(n_box, n_lev)
    box = lax.axis_index("box")
    lev = lax.axis_index("lev")
    me = box * n_lev + lev

    def at(linear):
        return (lax.div(linear, n_lev), lax.rem(linear, n_lev))

    def shifted(by):
        return at(lax.rem(me + (by + n_dev), n_dev))

    def beside(dx, dy):
        return (lax.rem(box + (dx + n_box), n_box), lax.rem(lev + (dy + n_lev), n_lev))

    barrier = pltpu.get_barrier_semaphore()
    for db, dl in offsets:
        pl.semaphore_signal(barrier, inc=1, device_id=beside(db, dl), device_id_type=MESH_ID)

    small_loads = [
        pltpu.make_async_copy(src, dst, small.at[i])
        for i, (src, dst) in enumerate(((owner_far, owner_of), (count_far, count)))
    ]
    for copy in small_loads:
        copy.start()
    all_rows = slots * frows
    loads = {}
    for part, (f0, f1) in enumerate(chunks):
        for s in range(slots):
            start, size = s * frows + f0 * fine_edge, (f1 - f0) * fine_edge
            for t in range(8):
                copy = pltpu.make_async_copy(
                    fine_far.at[pl.ds(start, size), pl.ds(t * LANES, LANES)],
                    fine.at[pl.ds(t * all_rows + start, size)],
                    load.at[part],
                )
                copy.start()
        rows = fine.at[pl.ds(0, 8 * slots * (f1 - f0) * fine_edge)]
        loads[part] = pltpu.make_async_copy(rows, rows, load.at[part])
    coarse_load = pltpu.make_async_copy(coarse_far, coarse, small.at[2])
    coarse_load.start()
    q = iota((fine_edge * fine_edge, plane), 0)
    c = iota((fine_edge * fine_edge, plane), 1)
    goal = (q // (2 * fine_edge)) * edge + (q % fine_edge) // 2
    table = jnp.where(goal == c, 0.125, 0.0).astype(BF16)
    order = (1, 2, 0, 3)
    back = [shifted(-delta) for delta in DELTAS]

    def target_of(d, k):
        dx, dy = DIRECTIONS[d]
        other = beside(-dx, -dy)
        return at(lax.rem(other[0] * n_lev + other[1] + (n_dev - DELTAS[k]), n_dev))

    targets = [[target_of(d, k) for k in range(4)] for d in range(8)]

    def place_of(device):
        db = lax.rem(device[0] - box + (n_box + reach), n_box)
        return db * n_lev + lax.rem(device[1] - lev + n_lev, n_lev)

    for copy in small_loads:
        copy.wait()
    live_count = count[0]
    owner = [owner_of[0, s] for s in range(slots)]
    region_of = [owner_of[1, s] for s in range(slots)]
    chosen = [
        [(s < live_count) & (owner[s] == delta) for delta in DELTAS] for s in range(slots)
    ]
    weight = [[jnp.where(c, 1.0, 0.0).astype(F32) for c in row] for row in chosen]
    for k in range(4):
        region = jnp.int32(-1)
        for s in range(slots):
            region = jnp.where(chosen[s][k], region_of[s], region)
        region_out[k] = jnp.full((1, LANES), 1.0, F32) * region.astype(F32)

    near_in[reach * n_lev] = region_out[...]
    first = {}
    for part, (f0, f1) in enumerate(chunks):
        size = (f1 - f0) * edge
        loads[part].wait()
        columns = []
        for t in range(8):
            pieces = []
            for s in range(slots):
                start = t * all_rows + s * frows + f0 * fine_edge
                pieces.append(
                    fine[pl.ds(start, size, stride=2), :] + fine[pl.ds(start + 1, size, stride=2), :]
                )
            columns.append(jnp.concatenate(pieces, axis=0))
        high, low = split(jnp.concatenate(columns, axis=1))
        got = jnp.dot(jnp.concatenate([high, low], axis=0), table, preferred_element_type=F32)
        got = got[:slots * size] + got[slots * size:]
        to = f0 * edge
        for h in range(2):
            averaged = []
            for s in range(slots):
                mean = got[s * size:(s + 1) * size, h * LANES:(h + 1) * LANES]
                start = (h * slots + s) * block + to
                avg[start:start + size, :] = mean
                averaged.append(mean)
            for k in range(4):
                total = averaged[0] * weight[0][k]
                for s in range(1, slots):
                    total = total + averaged[s] * weight[s][k]
                send1[k, to:to + size, h * LANES:(h + 1) * LANES] = total

    pl.semaphore_wait(barrier, len(offsets))
    for db, dl in offsets:
        slot = ((reach - db) % n_box) * n_lev + (-dl) % n_lev
        pltpu.make_async_remote_copy(
            src_ref=region_out, dst_ref=near_in.at[slot], send_sem=sh.at[0], recv_sem=rh.at[0],
            device_id=beside(db, dl), device_id_type=MESH_ID,
        ).start()
    for part, (f0, f1) in enumerate(chunks):
        to, size = f0 * edge, (f1 - f0) * edge
        for k in order:
            pltpu.make_async_remote_copy(
                src_ref=send1.at[k, pl.ds(to, size)], dst_ref=recv1.at[k, pl.ds(to, size)],
                send_sem=s1.at[0], recv_sem=r1.at[part],
                device_id=shifted(DELTAS[k]), device_id_type=MESH_ID,
            ).start()
        rows = recv1.at[:, pl.ds(to, size)]
        first[part] = pltpu.make_async_copy(rows, rows, r1.at[part])

    for pair in range(4):
        row = iota((LANES, 2 * LANES), 0)
        col = iota((LANES, 2 * LANES), 1)
        hit = (row // edge == 2 * pair + col // LANES) & (row % edge == col % edge)
        place_table[pair] = both(jnp.where(hit, 1.0, 0.0).astype(BF16))

    row = iota((plane, 4 * LANES), 0)
    col = iota((plane, 4 * LANES), 1)
    kind = col // LANES
    inner = col % edge
    fixed = jnp.where(kind % 2 == 0, 0, edge - 1)
    hit = jnp.where(kind < 2, fixed * edge + inner, inner * edge + fixed) == row
    own_table = jnp.where(hit, 1.0, 0.0).astype(BF16)
    high, low = split(jnp.concatenate(
        [avg[:slots * block, :], avg[slots * block:, :]], axis=1
    ))
    got = jnp.dot(high, own_table, preferred_element_type=F32) + jnp.dot(
        low, own_table, preferred_element_type=F32
    )
    for kind in range(4):
        own_got[kind * slots * block:(kind + 1) * slots * block, :] = got[
            :, kind * LANES:(kind + 1) * LANES
        ]
    group_f = iota((fields, LANES), 1) // edge
    for s in range(slots):
        for h in range(2):
            for side in range(2):
                start = (h * slots + s) * block + side * (edge - 1)
                to = lay.own + (2 * side + h) * fields
                window[s, to:to + fields, :] = avg[pl.ds(start, fields, stride=edge), :]
            for kind in range(4):
                total = jnp.zeros((fields, LANES), F32)
                for i in range(8):
                    start = (kind * slots + s) * block + h * 8 + i
                    part = own_got[pl.ds(start, fields, stride=edge), :]
                    total = jnp.where(group_f == i, part, total)
                to = lay.own + (2 * (2 + kind) + h) * fields
                window[s, to:to + fields, :] = total

        live = jnp.where(s < live_count, 1.0, 0.0).astype(F32)
        window[s, lay.keep:lay.keep + 1, :] = jnp.full((1, LANES), 1.0, F32) * live
    corner_lines[...] = jnp.zeros_like(corner_lines)
    coarse_load.wait()
    told = near_in.at[pl.ds(0, len(offsets))]
    pltpu.make_async_copy(told, told, rh.at[0]).wait()

    lane = iota((1, LANES), 1).astype(F32)
    here_rows = [near_in[place_of(back[k]), k] for k in range(4)]
    near = [[near_in[place_of(targets[d][k]), k] for k in range(4)] for d in range(8)]

    def pick(region, place):
        t = lane - edge * region - place
        return jnp.where((t == 0.0) | (t == LANES) | (t == -LANES), 1.0, 0.0)

    z_rows = []
    for depth in range(2):
        for k in range(4):
            for place in (-1 - depth, edge + depth):
                z_rows.append(pick(here_rows[k], place))
    for d in range(2):
        for place in (-1, edge):
            for k in range(4):
                z_rows.append(pick(near[d][k], place))
    z_table = jnp.concatenate(z_rows, axis=0).astype(BF16)
    z_table = jnp.concatenate([z_table, z_table], axis=1)
    z_cell = iota((LANES, LANES), 0).astype(F32)
    out_lane = iota((1, LANES), 1)
    inside = (out_lane % edge).astype(F32)
    outside = jnp.where(out_lane % 2 == 1, -1, edge).astype(F32)
    for d in (2, 3):
        for k in range(4):
            base = z_cell - edge * near[d][k]
            found = base == inside
            t = base - outside
            past = (t == 0.0) | (t == LANES) | (t == -LANES)
            for i, hit in enumerate((found, past)):
                side_table[d - 2, i, :, k * LANES:(k + 1) * LANES] = both(
                    jnp.where(hit, 1.0, 0.0).astype(BF16)
                )
    for corner in range(4):
        for k in range(4):
            corner_region[k, corner:corner + 1, :] = near[4 + corner][k]

    def z_fields(f0, f1):
        for f in range(f0, f1):
            start = f * lay.field
            got = times_transposed(z_table, split_lanes(upd[start:start + plane, :]))
            for depth in range(2):
                for h in range(2):
                    z_out[pl.ds((2 * depth + h) * fields + f, 8, stride=4 * fields), :] = got[
                        depth * 8:(depth + 1) * 8, h * LANES:(h + 1) * LANES
                    ]
            high_end = got[16:24, LANES:]
            if f:
                high_end = pltpu.roll(high_end, LANES - f * edge, 1)
            low_end = pltpu.roll(got[24:32, :LANES], LANES - (f + 1) * edge, 1)
            end_lines[0] = jnp.where(group8 == 7 - f, high_end, end_lines[0])
            end_lines[1] = jnp.where(group8 == 7 - f, low_end, end_lines[1])

    group = (iota((1, LANES), 1) // edge).astype(F32)
    here = [group == region for region in here_rows]
    group8 = iota((SUB, LANES), 1) // edge
    end_lines = [jnp.zeros((SUB, LANES), F32) for _ in range(2)]
    for part, (f0, f1) in enumerate(chunks):
        size = (f1 - f0) * edge
        first[part].wait()
        to = f0 * edge
        for h in range(2):
            stacked = split_lanes(jnp.concatenate(
                [recv1[k, to:to + size, h * LANES:(h + 1) * LANES] for k in range(4)], axis=0
            ))
            for pair in range(4):
                spread = jnp.dot(stacked, place_table[pair], preferred_element_type=F32)
                for odd in range(2):
                    y = h * SUB + 2 * pair + odd
                    for f in range(f0, f1):
                        merged = coarse[pl.ds(f * plane + y, edge, stride=edge), :]
                        for k in range(4):
                            start = k * size + (f - f0) * edge
                            merged = jnp.where(
                                here[k],
                                spread[start:start + edge, odd * LANES:(odd + 1) * LANES],
                                merged,
                            )
                        upd[pl.ds(f * lay.field + y, edge, stride=edge), :] = merged
        for f in range(f0, f1):
            pltpu.make_async_copy(
                upd.at[pl.ds(f * lay.field, plane)], updated.at[pl.ds(f * plane, plane)], put.at[0]
            ).start()
        if part == 0:
            z_fields(f0, f1)

    clear, unclear = [0, 0, 0], []
    steady = [True] + [len(v) == 1 for v in counts]

    def send(src, dst, sem, d, k, target):
        kinds = {False} if d is None else same[d, k]
        remote = local = None
        if False in kinds:
            remote = pltpu.make_async_remote_copy(
                src_ref=src, dst_ref=dst, recv_sem=r3.at[sem], device_id=target, device_id_type=MESH_ID,
                send_sem=s3.at[sem] if len(kinds) == 1 or steady[sem] else mixed.at[len(unclear)],
            )
        if True in kinds:
            local = pltpu.make_async_copy(src, dst, r3.at[sem])
        if local is None:
            remote.start()
            clear[sem] += 1
        elif remote is None:
            local.start()
        else:
            itself = (target[0] == box) & (target[1] == lev)
            pl.when(itself)(local.start)
            pl.when(jnp.logical_not(itself))(remote.start)
            if not steady[sem]:
                unclear.append((remote, itself))

    z_fields(*chunks[1])
    for k in order:
        send(z_out.at[pl.ds(k * lay.z_size, lay.z_size)], z_in.at[k], 0, None, k, back[k])
    field_step = lay.field
    sublane = iota((SUB, LANES), 0)
    in_group = iota((SUB, LANES), 1) % edge
    wide_group = iota((4 * SUB, LANES), 1) // edge
    turned = (iota((SUB, LANES), 1) + 2 * sublane) % LANES
    end_place = jnp.where(
        (sublane < fields) & ((turned % edge == 0) | (turned % edge == edge - 1)), turned // edge, -1
    )
    for d in (0, 1, 2, 3):
        outer, inner = (edge, 1) if d < 2 else (1, edge)
        adjacent = edge - 1 if d % 2 == 0 else 0
        far = edge - 2 if d % 2 == 0 else 1
        lines = []
        for i in range(8):
            lines.append(jnp.concatenate([
                upd[pl.ds(level * outer + (h * 8 + i) * inner, SUB, stride=field_step), :]
                for level in (adjacent, far) for h in range(2)
            ], axis=0))
        if d < 2:
            by_region = transposed_groups(lines, edge)
            ends = []
            for g in range(8):
                before = by_region[(g + 7) % 8][:2 * SUB]
                after = by_region[(g + 1) % 8][:2 * SUB]
                ends.append(jnp.where(iota((2 * SUB, LANES), 1) % edge == 0, after, before))
        else:
            wide = split_lanes(jnp.concatenate(lines, axis=0))
            ahead = split_lanes(jnp.concatenate([v[:2 * SUB] for v in lines], axis=0))
            cells = jnp.dot(wide, side_table[d - 2, 0], preferred_element_type=F32)
            beyond = jnp.dot(ahead, side_table[d - 2, 1], preferred_element_type=F32)
        for k in range(4):
            if d < 2:
                region = near[d][k]
                total = by_region[0]
                end = ends[0]
                for g in range(1, 8):
                    hit = region == float(g)
                    total = jnp.where(hit, by_region[g], total)
                    end = jnp.where(hit, ends[g], end)
                single = []
                for h in range(2):
                    used = (sublane < fields) & ((in_group == 0) | (in_group == edge - 1))
                    one = jnp.where(used, end[h * SUB:(h + 1) * SUB, :], 0.0)
                    moved = one
                    for f in range(1, fields):
                        moved = jnp.where(sublane == f, pltpu.roll(one, LANES - 2 * f, 1), moved)
                    single.append(moved)
            else:
                cols = slice(k * LANES, (k + 1) * LANES)
                total = cells[:4 * SUB, cols]
                for i in range(1, 8):
                    total = jnp.where(wide_group == i, cells[i * 4 * SUB:(i + 1) * 4 * SUB, cols], total)
                single = []
                for h in range(2):
                    moved = jnp.zeros((SUB, LANES), F32)
                    for i in range(8):
                        start = (2 * i + h) * SUB
                        moved = jnp.where(end_place == i, beyond[start:start + SUB, cols], moved)
                    single.append(moved)
            base = (d * 4 + k) * lay.side
            for part in range(4):
                side_out[base + part * fields:base + (part + 1) * fields, :] = total[
                    part * SUB:part * SUB + fields, :
                ]
            for h in range(2):
                side_out[base + lay.ends + h:base + lay.ends + h + 1, :] = jnp.sum(
                    single[h], axis=0, keepdims=True
                )
        if d < 2:
            for e in range(2):
                side_out[pl.ds(d * 4 * lay.side + lay.ends + 2 + e, 4, stride=lay.side), :] = (
                    end_lines[d][e * 4:(e + 1) * 4, :]
                )
        else:
            for e in range(2):
                side_out[pl.ds(d * 4 * lay.side + lay.ends + 2 + e, 4, stride=lay.side), :] = (
                    jnp.zeros((4, LANES), F32)
                )

        if d == 3:
            for near_d in range(4):
                for k in order:
                    send(
                        side_out.at[pl.ds((near_d * 4 + k) * lay.side, lay.side)],
                        side_in.at[k, near_d], 1, near_d, k, targets[near_d][k],
                    )

    for f in range(fields):
        for corner in range(4):
            x = 0 if corner // 2 else edge - 1
            y = 0 if corner % 2 else edge - 1
            start = f * lay.field + x * edge + y
            corner_lines[7 - f, corner:corner + 1, :] = upd[start:start + 1, :]
    by_region = transposed_groups([corner_lines[f] for f in range(8)], edge)
    for k in range(4):
        region = corner_region[k]
        total = by_region[0]
        for g in range(1, 8):
            total = jnp.where(region == float(g), by_region[g], total)
        for corner in range(4):
            corner_out[corner * 4 + k] = total[corner:corner + 1, :]
    for corner in range(4):
        for k in order:
            send(
                corner_out.at[corner * 4 + k], corner_in.at[k * 4 + corner],
                2, 4 + corner, k, targets[4 + corner][k],
            )

    for sem, ref in enumerate((z_in, side_in, corner_in)):
        pltpu.make_async_copy(ref, ref, r3.at[sem]).wait()
    for s in range(slots):
        k = owner[s] + 2 - jnp.where(owner[s] > 0, 1, 0)
        for d in range(4):
            window[s, d * lay.side:(d + 1) * lay.side, :] = side_in[k, d]
        window[s, lay.z:lay.z + lay.z_size, :] = z_in[k]
        for corner in range(4):
            window[s, lay.corner + corner:lay.corner + corner + 1, :] = corner_in[k * 4 + corner]

    pltpu.make_async_copy(updated, updated, put.at[0]).wait()
    pltpu.make_async_copy(send1, send1, s1.at[0]).wait()
    told = near_in.at[pl.ds(0, len(offsets))]
    pltpu.make_async_copy(told, told, sh.at[0]).wait()
    for sem in (1, 2):
        if steady[sem]:
            clear[sem] = min(counts[sem - 1])
    for sem, (ref, size) in enumerate(((z_out, lay.z_size), (side_out, lay.side), (corner_out, 1))):
        if clear[sem]:
            rows = ref.at[pl.ds(0, clear[sem] * size)]
            pltpu.make_async_copy(rows, rows, s3.at[sem]).wait()
    for remote, itself in unclear:
        pl.when(jnp.logical_not(itself))(remote.wait_send)


def ghost_kernel(
    slots, fields, edge, mask_far, updated_in, window, updated_out, ghost_out,
    mask, passing, ghost, table, lhs, mask_sem, pass_sem, out_sem,
):
    lay = Layout(fields, edge)
    into = pltpu.make_async_copy(updated_in, passing, pass_sem.at[0])
    out = pltpu.make_async_copy(passing, updated_out, pass_sem.at[1])
    mask_load = pltpu.make_async_copy(mask_far, mask, mask_sem.at[0])
    mask_load.start()
    into.start()

    table[...] = jnp.zeros_like(table)
    cell_row = iota((edge, LANES), 0)
    col = iota((edge, LANES), 1)
    quarter = 2 * edge
    for kind in range(3):
        target = (col % 64) // 4 if kind == 2 else (col % quarter) // 2
        along = (col // quarter) % 2 if kind == 0 else col // 64
        within = (col // 2) % 2 if kind == 2 else col % 2
        step = cell_row - target
        alike = step == 0

        def signed(sign, where):
            return jnp.where(where, jnp.where(sign == 1, 0.125, -0.125), 0.0)

        centre = jnp.where(alike, 1.0, signed(within, step == 1) - signed(within, step == -1))
        ends = signed(within, step == 1 - edge) - signed(within, step == edge - 1)
        slope = signed(along, alike)
        for odd in range(2):
            for line in range(2):
                block = 2 * odd + line
                for column in range(2):
                    if kind == 0:
                        normal = jnp.where(alike, 0.125 if column else -0.125, 0.0)
                        used = col // 64 == line
                    else:
                        normal = signed(col % 2 if kind == 2 else (col // quarter) % 2, alike)
                        used = None if column == line else False
                    if used is False:
                        continue
                    for part, value in enumerate((centre, slope, normal, ends)):
                        if used is not None:
                            value = jnp.where(used, value, 0.0)
                        row = (part % 2) * LANES + (odd * 4 + (part // 2) * 2 + line) * edge
                        to = (2 * odd + column) * LANES
                        table[kind, row:row + edge, to:to + LANES] = value.astype(BF16)

    lane = iota((SUB, LANES), 1)
    in_group = lane % edge
    last_lane, first_lane = lane >= LANES - edge, lane < edge

    def gather(s):
        def rows(start, size=SUB):
            return window[s, start:start + size, :]

        def spread(start, shift, stride):
            row = jnp.broadcast_to(rows(start, 1), (SUB, LANES))
            return pltpu.roll(row, shift % LANES, 1, stride=stride, stride_axis=0)

        for kind in range(3):
            parts = [[] for _ in range(8)]
            for side in range(2):
                face = 2 * kind + side
                base = face * lay.side if kind < 2 else lay.z + side * 4 * fields
                layers = [rows(base + h * fields) for h in range(4)]
                centre, far = layers[:2], layers[2:]
                own = [rows(lay.own + (2 * face + h) * fields) for h in range(2)]
                if kind == 0:
                    lines = [lay.corner + 2 * side, lay.corner + 2 * side + 1]
                elif kind == 1:
                    lines = [lay.corner + side, lay.corner + 2 + side]
                else:
                    lines = [d * lay.side + lay.ends + 2 + side for d in range(2)]
                below = spread(lines[0], edge, edge)
                above = spread(lines[1], 0, edge)
                up = [pltpu.roll(v, LANES - edge, 1) for v in centre]
                down = [pltpu.roll(v, edge, 1) for v in centre]
                along = [
                    jnp.where(last_lane, up[1], up[0]) - jnp.where(first_lane, below, down[0]),
                    jnp.where(last_lane, above, up[1]) - jnp.where(first_lane, down[0], down[1]),
                ]
                for h in range(2):
                    if kind < 2:
                        before = after = spread(base + lay.ends + h, 0, 2)
                    else:
                        low_row, high_row = 2 * lay.side + lay.ends + h, 3 * lay.side + lay.ends + h
                        before = spread(low_row, edge - 1 if side else 0, 2)
                        after = spread(high_row, 0 if side else 1 - edge, 2)
                    end = jnp.where(in_group == edge - 1, before, jnp.where(in_group == 0, after, 0.0))
                    normal = own[h] - far[h] if side == 0 else far[h] - own[h]
                    for part, values in enumerate((centre[h], along[h], normal, end)):
                        parts[h * 4 + part].append(values)
            groups = transposed_groups([jnp.concatenate(v, axis=0) for v in parts], edge, (4, 2))
            for pair in range(4):
                high, low = split(jnp.concatenate(groups[2 * pair:2 * pair + 2], axis=1))
                lhs[s * 3 + kind, pair * 16:(pair + 1) * 16, :] = high
                lhs[s * 3 + kind, 64 + pair * 16:64 + (pair + 1) * 16, :] = low

    def finish(s):
        live = window[s, lay.keep:lay.keep + 1, :]
        for kind in range(3):
            both_parts = jnp.dot(lhs[s * 3 + kind], table[kind], preferred_element_type=F32)
            spreads = both_parts[:64] + both_parts[64:]
            for side in range(2):
                face = 2 * kind + side
                keep = live * jnp.where(mask[s, face] > 0, 1.0, 0.0).astype(F32)
                for pair in range(4):
                    for block in range(4):
                        start = pair * 16 + side * SUB
                        value = spreads[start:start + SUB, block * LANES:(block + 1) * LANES] * keep
                        h, column = block // 2, block % 2
                        tile = column * 8 + h * 4 + pair if kind == 0 else h * 8 + pair * 2 + column
                        ghost[s, :, face, tile * LANES:(tile + 1) * LANES] = value[:fields]

    def send(s):
        for f in range(fields):
            pltpu.make_async_copy(
                ghost.at[s, f, :, pl.ds(0, ghost_out.shape[3])], ghost_out.at[s, f], out_sem.at[0]
            ).start()

    gather(0)
    mask_load.wait()
    for s in range(slots):
        if s + 1 < slots:
            gather(s + 1)
        finish(s)
        send(s)
        if s == 0:
            into.wait()
            out.start()
    out.wait()
    pltpu.make_async_copy(ghost_out, ghost_out, out_sem.at[0]).wait()


def body(n_box, n_lev, fine, coarse, owner_map, patch_count, face_mask):
    slots, fields, fine_edge, _ = fine.shape
    edge = fine_edge // 2
    block = fields * edge
    lay = Layout(fields, edge)
    offsets, reach, same, counts = relations(n_box, n_lev)
    far = pl.BlockSpec(memory_space=pl.ANY)
    vmem = pl.BlockSpec(memory_space=pltpu.VMEM)
    flat = jax.ShapeDtypeStruct((block * edge, LANES), F32)
    places = (2 * reach + 1) * n_lev
    unsteady = 1 if max(len(v) for v in counts) == 1 else sum(len(v) > 1 for v in same.values())
    owner_rows = owner_map.T
    updated, window = pl.pallas_call(
        functools.partial(kernel, n_box, n_lev, slots, fields, edge),
        out_shape=(
            flat,
            jax.ShapeDtypeStruct((slots, lay.rows, LANES), F32),
        ),
        in_specs=[far] * 4,
        out_specs=(far, vmem),
        scratch_shapes=[
            pltpu.SMEM(owner_rows.shape, jnp.int32),
            pltpu.SMEM(patch_count.shape, jnp.int32),
            pltpu.VMEM((8 * slots * fields * fine_edge, LANES), F32),
            pltpu.VMEM((block * edge, LANES), F32),
            pltpu.VMEM((2 * slots * block, LANES), F32),
            pltpu.VMEM((4 * slots * block, LANES), F32),
            pltpu.VMEM((4, block, 2 * LANES), F32),
            pltpu.VMEM((4, block, 2 * LANES), F32),
            pltpu.VMEM((4, 1, LANES), F32),
            pltpu.VMEM((places, 4, 1, LANES), F32),
            pltpu.VMEM((SUB * lay.field, LANES), F32),
            pltpu.VMEM((2, 2, 2 * LANES, 4 * LANES), BF16),
            pltpu.VMEM((SUB, SUB, LANES), F32),
            pltpu.VMEM((4, SUB, LANES), F32),
            pltpu.VMEM((16 * lay.side, LANES), F32),
            pltpu.VMEM((4, 4, lay.side, LANES), F32),
            pltpu.VMEM((4 * lay.z_size, LANES), F32),
            pltpu.VMEM((4, lay.z_size, LANES), F32),
            pltpu.VMEM((16, 1, LANES), F32),
            pltpu.VMEM((16, 1, LANES), F32),
            pltpu.VMEM((4, 2 * LANES, 2 * LANES), BF16),
            pltpu.SemaphoreType.DMA((3,)),
            pltpu.SemaphoreType.DMA((2,)),
            pltpu.SemaphoreType.DMA((1,)),
            pltpu.SemaphoreType.DMA((1,)),
            pltpu.SemaphoreType.DMA((2,)),
            pltpu.SemaphoreType.DMA((1,)),
            pltpu.SemaphoreType.DMA((1,)),
            pltpu.SemaphoreType.DMA((3,)),
            pltpu.SemaphoreType.DMA((3,)),
            pltpu.SemaphoreType.DMA((unsteady,)),
        ],
        compiler_params=pltpu.CompilerParams(
            collective_id=0, has_side_effects=True, vmem_limit_bytes=VMEM_FIRST
        ),
    )(
        owner_rows, patch_count,
        fine.reshape(slots * fields * fine_edge, fine_edge * fine_edge),
        coarse.reshape(block * edge, LANES),
    )
    ghost_shape = (slots, fields, 6, 2 * fine_edge * fine_edge)
    updated, ghost = pl.pallas_call(
        functools.partial(ghost_kernel, slots, fields, edge),
        out_shape=(flat, jax.ShapeDtypeStruct(ghost_shape, F32)),
        in_specs=[far, far, vmem],
        out_specs=(far, far),
        scratch_shapes=[
            pltpu.SMEM(face_mask.shape, jnp.int32),
            pltpu.VMEM((block * edge, LANES), F32),
            pltpu.VMEM((*ghost_shape[:3], ghost_shape[3] + LANES), F32),
            pltpu.VMEM((3, 2 * LANES, 4 * LANES), BF16),
            pltpu.VMEM((3 * slots, LANES, 2 * LANES), BF16),
            pltpu.SemaphoreType.DMA((1,)),
            pltpu.SemaphoreType.DMA((2,)),
            pltpu.SemaphoreType.DMA((1,)),
        ],
        compiler_params=pltpu.CompilerParams(vmem_limit_bytes=VMEM_SECOND),
    )(face_mask, updated, window)
    return updated.reshape(coarse.shape), ghost.transpose(0, 2, 1, 3)


def solution(mesh):
    return jax.shard_map(
        functools.partial(body, mesh.shape["box"], mesh.shape["lev"]),
        mesh=mesh,
        in_specs=(
            P(("box", "lev"), None, None, None),
            P(None, "box", "lev", None),
            P(("box", "lev"), None),
            P(("box", "lev")),
            P(("box", "lev"), None),
        ),
        out_specs=(P(None, "box", "lev", None), P(("box", "lev"), None, None, None)),
        check_vma=False,
    )
```

```python
import functools

import jax
import jax.numpy as jnp
from jax import lax
from jax.experimental import pallas as pl
from jax.experimental.pallas import tpu as pltpu
from jax.sharding import PartitionSpec as P

DELTAS = (-2, -1, 1, 2)
LANES = 128
SUB = 8
F32 = jnp.float32
BF16 = jnp.bfloat16
MESH_ID = pl.DeviceIdType.MESH
VMEM_FIRST = 56000000
VMEM_SECOND = 56000000


def iota(shape, dim):
    return lax.broadcasted_iota(jnp.int32, shape, dim)


def split(values):
    high = values.astype(BF16)
    return high, (values - high.astype(F32)).astype(BF16)


def split_lanes(values):
    return jnp.concatenate(split(values), axis=1)


def times_transposed(left, right):
    return lax.dot_general(left, right, (((1,), (1,)), ((), ())), preferred_element_type=F32)


def both(table):
    return jnp.concatenate([table, table], axis=0)


def transposed_groups(arrays, edge, bits=(4, 2, 1)):
    out = list(arrays)
    group = iota(out[0].shape, 1) // edge
    for bit in bits:
        low = (group // bit) % 2 == 0
        for i in range(8):
            if i & bit == 0:
                a, b = out[i], out[i + bit]
                out[i] = jnp.where(low, a, pltpu.roll(b, bit * edge, 1))
                out[i + bit] = jnp.where(low, pltpu.roll(a, LANES - bit * edge, 1), b)
    return out


class Layout:
    def __init__(self, fields, edge):
        self.ends = 4 * fields
        self.side = 4 * fields + 4
        self.z_size = 8 * fields
        self.z = 4 * self.side
        self.corner = self.z + self.z_size
        self.own = self.corner + 4
        self.keep = self.own + 12 * fields
        self.rows = self.keep + 1
        self.rows = self.rows + (-self.rows) % SUB
        self.field = edge * edge + SUB


DIRECTIONS = ((-1, 0), (1, 0), (0, -1), (0, 1), (-1, -1), (-1, 1), (1, -1), (1, 1))


def relations(n_box, n_lev):
    n_dev = n_box * n_lev
    offsets, same, counts = set(), {}, (set(), set())
    for me in range(n_dev):
        box, lev = divmod(me, n_lev)

        def add(other):
            db, dl = (other // n_lev - box) % n_box, (other % n_lev - lev) % n_lev
            offsets.add((db, dl))
            offsets.add((-db % n_box, -dl % n_lev))

        for delta in DELTAS:
            add((me + delta) % n_dev)
        others = [0, 0]
        for d, (dx, dy) in enumerate(DIRECTIONS):
            owner = ((box - dx) % n_box) * n_lev + (lev - dy) % n_lev
            add(owner)
            for k, delta in enumerate(DELTAS):
                target = (owner - delta) % n_dev
                add(target)
                same.setdefault((d, k), set()).add(target == me)
                others[d // 4] += target != me
        for kind in range(2):
            counts[kind].add(others[kind])
    offsets.discard((0, 0))
    reach = max(min(db, n_box - db) for db, _ in offsets)
    return sorted(offsets), reach, same, counts


def kernel(
    n_box, n_lev, slots, fields, edge,
    owner_far, count_far, fine_far, coarse_far, updated, window,
    owner_of, count, fine, coarse, avg, own_got, send1, recv1, region_out, near_in,
    upd, side_table, corner_lines, corner_region, side_out, side_in, z_out, z_in, corner_out, corner_in, place_table,
    small, load, put, s1, r1, sh, rh, s3, r3, mixed,
):
    fine_edge = 2 * edge
    block = fields * edge
    plane = edge * edge
    lay = Layout(fields, edge)
    frows = fields * fine_edge
    cut = (fields + 1) // 2
    chunks = ((0, cut), (cut, fields))
    n_dev = n_box * n_lev
    offsets, reach, same, counts = relations(n_box, n_lev)
    box = lax.axis_index("box")
    lev = lax.axis_index("lev")
    me = box * n_lev + lev

    def at(linear):
        return (lax.div(linear, n_lev), lax.rem(linear, n_lev))

    def shifted(by):
        return at(lax.rem(me + (by + n_dev), n_dev))

    def beside(dx, dy):
        return (lax.rem(box + (dx + n_box), n_box), lax.rem(lev + (dy + n_lev), n_lev))

    barrier = pltpu.get_barrier_semaphore()
    for db, dl in offsets:
        pl.semaphore_signal(barrier, inc=1, device_id=beside(db, dl), device_id_type=MESH_ID)

    small_loads = [
        pltpu.make_async_copy(src, dst, small.at[i])
        for i, (src, dst) in enumerate(((owner_far, owner_of), (count_far, count)))
    ]
    for copy in small_loads:
        copy.start()
    all_rows = slots * frows
    loads = {}
    for part, (f0, f1) in enumerate(chunks):
        for s in range(slots):
            start, size = s * frows + f0 * fine_edge, (f1 - f0) * fine_edge
            for t in range(8):
                copy = pltpu.make_async_copy(
                    fine_far.at[pl.ds(start, size), pl.ds(t * LANES, LANES)],
                    fine.at[pl.ds(t * all_rows + start, size)],
                    load.at[part],
                )
                copy.start()
        rows = fine.at[pl.ds(0, 8 * slots * (f1 - f0) * fine_edge)]
        loads[part] = pltpu.make_async_copy(rows, rows, load.at[part])
    coarse_load = pltpu.make_async_copy(coarse_far, coarse, small.at[2])
    coarse_load.start()
    q = iota((fine_edge * fine_edge, plane), 0)
    c = iota((fine_edge * fine_edge, plane), 1)
    goal = (q // (2 * fine_edge)) * edge + (q % fine_edge) // 2
    table = jnp.where(goal == c, 0.125, 0.0).astype(BF16)
    order = (1, 2, 0, 3)
    back = [shifted(-delta) for delta in DELTAS]

    def target_of(d, k):
        dx, dy = DIRECTIONS[d]
        other = beside(-dx, -dy)
        return at(lax.rem(other[0] * n_lev + other[1] + (n_dev - DELTAS[k]), n_dev))

    targets = [[target_of(d, k) for k in range(4)] for d in range(8)]

    def place_of(device):
        db = lax.rem(device[0] - box + (n_box + reach), n_box)
        return db * n_lev + lax.rem(device[1] - lev + n_lev, n_lev)

    for copy in small_loads:
        copy.wait()
    live_count = count[0]
    owner = [owner_of[0, s] for s in range(slots)]
    region_of = [owner_of[1, s] for s in range(slots)]
    chosen = [
        [(s < live_count) & (owner[s] == delta) for delta in DELTAS] for s in range(slots)
    ]
    weight = [[jnp.where(c, 1.0, 0.0).astype(F32) for c in row] for row in chosen]
    for k in range(4):
        region = jnp.int32(-1)
        for s in range(slots):
            region = jnp.where(chosen[s][k], region_of[s], region)
        region_out[k] = jnp.full((1, LANES), 1.0, F32) * region.astype(F32)

    near_in[reach * n_lev] = region_out[...]
    first = {}
    for part, (f0, f1) in enumerate(chunks):
        size = (f1 - f0) * edge
        loads[part].wait()
        columns = []
        for t in range(8):
            pieces = []
            for s in range(slots):
                start = t * all_rows + s * frows + f0 * fine_edge
                pieces.append(
                    fine[pl.ds(start, size, stride=2), :] + fine[pl.ds(start + 1, size, stride=2), :]
                )
            columns.append(jnp.concatenate(pieces, axis=0))
        high, low = split(jnp.concatenate(columns, axis=1))
        got = jnp.dot(jnp.concatenate([high, low], axis=0), table, preferred_element_type=F32)
        got = got[:slots * size] + got[slots * size:]
        to = f0 * edge
        for h in range(2):
            averaged = []
            for s in range(slots):
                mean = got[s * size:(s + 1) * size, h * LANES:(h + 1) * LANES]
                start = (h * slots + s) * block + to
                avg[start:start + size, :] = mean
                averaged.append(mean)
            for k in range(4):
                total = averaged[0] * weight[0][k]
                for s in range(1, slots):
                    total = total + averaged[s] * weight[s][k]
                send1[k, to:to + size, h * LANES:(h + 1) * LANES] = total

    pl.semaphore_wait(barrier, len(offsets))
    for db, dl in offsets:
        slot = ((reach - db) % n_box) * n_lev + (-dl) % n_lev
        pltpu.make_async_remote_copy(
            src_ref=region_out, dst_ref=near_in.at[slot], send_sem=sh.at[0], recv_sem=rh.at[0],
            device_id=beside(db, dl), device_id_type=MESH_ID,
        ).start()
    for part, (f0, f1) in enumerate(chunks):
        to, size = f0 * edge, (f1 - f0) * edge
        for k in order:
            pltpu.make_async_remote_copy(
                src_ref=send1.at[k, pl.ds(to, size)], dst_ref=recv1.at[k, pl.ds(to, size)],
                send_sem=s1.at[0], recv_sem=r1.at[part],
                device_id=shifted(DELTAS[k]), device_id_type=MESH_ID,
            ).start()
        rows = recv1.at[:, pl.ds(to, size)]
        first[part] = pltpu.make_async_copy(rows, rows, r1.at[part])

    for pair in range(4):
        row = iota((LANES, 2 * LANES), 0)
        col = iota((LANES, 2 * LANES), 1)
        hit = (row // edge == 2 * pair + col // LANES) & (row % edge == col % edge)
        place_table[pair] = both(jnp.where(hit, 1.0, 0.0).astype(BF16))

    row = iota((plane, 4 * LANES), 0)
    col = iota((plane, 4 * LANES), 1)
    kind = col // LANES
    inner = col % edge
    fixed = jnp.where(kind % 2 == 0, 0, edge - 1)
    hit = jnp.where(kind < 2, fixed * edge + inner, inner * edge + fixed) == row
    own_table = jnp.where(hit, 1.0, 0.0).astype(BF16)
    high, low = split(jnp.concatenate(
        [avg[:slots * block, :], avg[slots * block:, :]], axis=1
    ))
    got = jnp.dot(high, own_table, preferred_element_type=F32) + jnp.dot(
        low, own_table, preferred_element_type=F32
    )
    for kind in range(4):
        own_got[kind * slots * block:(kind + 1) * slots * block, :] = got[
            :, kind * LANES:(kind + 1) * LANES
        ]
    group_f = iota((fields, LANES), 1) // edge
    for s in range(slots):
        for h in range(2):
            for side in range(2):
                start = (h * slots + s) * block + side * (edge - 1)
                to = lay.own + (2 * side + h) * fields
                window[s, to:to + fields, :] = avg[pl.ds(start, fields, stride=edge), :]
            for kind in range(4):
                total = jnp.zeros((fields, LANES), F32)
                for i in range(8):
                    start = (kind * slots + s) * block + h * 8 + i
                    part = own_got[pl.ds(start, fields, stride=edge), :]
                    total = jnp.where(group_f == i, part, total)
                to = lay.own + (2 * (2 + kind) + h) * fields
                window[s, to:to + fields, :] = total

        live = jnp.where(s < live_count, 1.0, 0.0).astype(F32)
        window[s, lay.keep:lay.keep + 1, :] = jnp.full((1, LANES), 1.0, F32) * live
    corner_lines[...] = jnp.zeros_like(corner_lines)
    coarse_load.wait()
    told = near_in.at[pl.ds(0, len(offsets))]
    pltpu.make_async_copy(told, told, rh.at[0]).wait()

    lane = iota((1, LANES), 1).astype(F32)
    here_rows = [near_in[place_of(back[k]), k] for k in range(4)]
    near = [[near_in[place_of(targets[d][k]), k] for k in range(4)] for d in range(8)]

    def pick(region, place):
        t = lane - edge * region - place
        return jnp.where((t == 0.0) | (t == LANES) | (t == -LANES), 1.0, 0.0)

    z_rows = []
    for depth in range(2):
        for k in range(4):
            for place in (-1 - depth, edge + depth):
                z_rows.append(pick(here_rows[k], place))
    for d in range(2):
        for place in (-1, edge):
            for k in range(4):
                z_rows.append(pick(near[d][k], place))
    z_table = jnp.concatenate(z_rows, axis=0).astype(BF16)
    z_table = jnp.concatenate([z_table, z_table], axis=1)
    for corner in range(4):
        for k in range(4):
            corner_region[k, corner:corner + 1, :] = near[4 + corner][k]

    def z_fields(f0, f1):
        for f in range(f0, f1):
            start = f * lay.field
            got = times_transposed(z_table, split_lanes(upd[start:start + plane, :]))
            for depth in range(2):
                for h in range(2):
                    z_out[pl.ds((2 * depth + h) * fields + f, 8, stride=4 * fields), :] = got[
                        depth * 8:(depth + 1) * 8, h * LANES:(h + 1) * LANES
                    ]
            high_end = got[16:24, LANES:]
            if f:
                high_end = pltpu.roll(high_end, LANES - f * edge, 1)
            low_end = pltpu.roll(got[24:32, :LANES], LANES - (f + 1) * edge, 1)
            end_lines[0] = jnp.where(group8 == 7 - f, high_end, end_lines[0])
            end_lines[1] = jnp.where(group8 == 7 - f, low_end, end_lines[1])

    group = (iota((1, LANES), 1) // edge).astype(F32)
    here = [group == region for region in here_rows]
    group8 = iota((SUB, LANES), 1) // edge
    end_lines = [jnp.zeros((SUB, LANES), F32) for _ in range(2)]
    for part, (f0, f1) in enumerate(chunks):
        size = (f1 - f0) * edge
        first[part].wait()
        to = f0 * edge
        for h in range(2):
            stacked = split_lanes(jnp.concatenate(
                [recv1[k, to:to + size, h * LANES:(h + 1) * LANES] for k in range(4)], axis=0
            ))
            for pair in range(4):
                spread = jnp.dot(stacked, place_table[pair], preferred_element_type=F32)
                for odd in range(2):
                    y = h * SUB + 2 * pair + odd
                    for f in range(f0, f1):
                        merged = coarse[pl.ds(f * plane + y, edge, stride=edge), :]
                        for k in range(4):
                            start = k * size + (f - f0) * edge
                            merged = jnp.where(
                                here[k],
                                spread[start:start + edge, odd * LANES:(odd + 1) * LANES],
                                merged,
                            )
                        upd[pl.ds(f * lay.field + y, edge, stride=edge), :] = merged
        for f in range(f0, f1):
            pltpu.make_async_copy(
                upd.at[pl.ds(f * lay.field, plane)], updated.at[pl.ds(f * plane, plane)], put.at[0]
            ).start()
        if part == 0:
            z_fields(f0, f1)
            z_cell = iota((LANES, LANES), 0).astype(F32)
            out_lane = iota((1, LANES), 1)
            inside = (out_lane % edge).astype(F32)
            outside = jnp.where(out_lane % 2 == 1, -1, edge).astype(F32)
            for d in (2, 3):
                for k in range(4):
                    base = z_cell - edge * near[d][k]
                    found = base == inside
                    t = base - outside
                    past = (t == 0.0) | (t == LANES) | (t == -LANES)
                    for i, hit in enumerate((found, past)):
                        side_table[d - 2, i, :, k * LANES:(k + 1) * LANES] = both(
                            jnp.where(hit, 1.0, 0.0).astype(BF16)
                        )

    clear, unclear = [0, 0, 0], []
    steady = [True] + [len(v) == 1 for v in counts]

    def send(src, dst, sem, d, k, target):
        kinds = {False} if d is None else same[d, k]
        remote = local = None
        if False in kinds:
            remote = pltpu.make_async_remote_copy(
                src_ref=src, dst_ref=dst, recv_sem=r3.at[sem], device_id=target, device_id_type=MESH_ID,
                send_sem=s3.at[sem] if len(kinds) == 1 or steady[sem] else mixed.at[len(unclear)],
            )
        if True in kinds:
            local = pltpu.make_async_copy(src, dst, r3.at[sem])
        if local is None:
            remote.start()
            clear[sem] += 1
        elif remote is None:
            local.start()
        else:
            itself = (target[0] == box) & (target[1] == lev)
            pl.when(itself)(local.start)
            pl.when(jnp.logical_not(itself))(remote.start)
            if not steady[sem]:
                unclear.append((remote, itself))

    z_fields(*chunks[1])
    for k in order:
        send(z_out.at[pl.ds(k * lay.z_size, lay.z_size)], z_in.at[k], 0, None, k, back[k])
    field_step = lay.field
    sublane = iota((SUB, LANES), 0)
    in_group = iota((SUB, LANES), 1) % edge
    wide_group = iota((4 * SUB, LANES), 1) // edge
    turned = (iota((SUB, LANES), 1) + 2 * sublane) % LANES
    end_place = jnp.where(
        (sublane < fields) & ((turned % edge == 0) | (turned % edge == edge - 1)), turned // edge, -1
    )
    for d in (0, 1, 2, 3):
        outer, inner = (edge, 1) if d < 2 else (1, edge)
        adjacent = edge - 1 if d % 2 == 0 else 0
        far = edge - 2 if d % 2 == 0 else 1
        lines = []
        for i in range(8):
            lines.append(jnp.concatenate([
                upd[pl.ds(level * outer + (h * 8 + i) * inner, SUB, stride=field_step), :]
                for level in (adjacent, far) for h in range(2)
            ], axis=0))
        if d < 2:
            by_region = transposed_groups(lines, edge)
            ends = []
            for g in range(8):
                before = by_region[(g + 7) % 8][:2 * SUB]
                after = by_region[(g + 1) % 8][:2 * SUB]
                ends.append(jnp.where(iota((2 * SUB, LANES), 1) % edge == 0, after, before))
        else:
            wide = split_lanes(jnp.concatenate(lines, axis=0))
            ahead = split_lanes(jnp.concatenate([v[:2 * SUB] for v in lines], axis=0))
            cells = jnp.dot(wide, side_table[d - 2, 0], preferred_element_type=F32)
            beyond = jnp.dot(ahead, side_table[d - 2, 1], preferred_element_type=F32)
        for k in range(4):
            if d < 2:
                region = near[d][k]
                total = by_region[0]
                end = ends[0]
                for g in range(1, 8):
                    hit = region == float(g)
                    total = jnp.where(hit, by_region[g], total)
                    end = jnp.where(hit, ends[g], end)
                single = []
                for h in range(2):
                    used = (sublane < fields) & ((in_group == 0) | (in_group == edge - 1))
                    one = jnp.where(used, end[h * SUB:(h + 1) * SUB, :], 0.0)
                    moved = one
                    for f in range(1, fields):
                        moved = jnp.where(sublane == f, pltpu.roll(one, LANES - 2 * f, 1), moved)
                    single.append(moved)
            else:
                cols = slice(k * LANES, (k + 1) * LANES)
                total = cells[:4 * SUB, cols]
                for i in range(1, 8):
                    total = jnp.where(wide_group == i, cells[i * 4 * SUB:(i + 1) * 4 * SUB, cols], total)
                single = []
                for h in range(2):
                    moved = jnp.zeros((SUB, LANES), F32)
                    for i in range(8):
                        start = (2 * i + h) * SUB
                        moved = jnp.where(end_place == i, beyond[start:start + SUB, cols], moved)
                    single.append(moved)
            base = (d * 4 + k) * lay.side
            for part in range(4):
                side_out[base + part * fields:base + (part + 1) * fields, :] = total[
                    part * SUB:part * SUB + fields, :
                ]
            for h in range(2):
                side_out[base + lay.ends + h:base + lay.ends + h + 1, :] = jnp.sum(
                    single[h], axis=0, keepdims=True
                )
        if d < 2:
            for e in range(2):
                side_out[pl.ds(d * 4 * lay.side + lay.ends + 2 + e, 4, stride=lay.side), :] = (
                    end_lines[d][e * 4:(e + 1) * 4, :]
                )
        else:
            for e in range(2):
                side_out[pl.ds(d * 4 * lay.side + lay.ends + 2 + e, 4, stride=lay.side), :] = (
                    jnp.zeros((4, LANES), F32)
                )

        if d == 3:
            for near_d in range(4):
                for k in order:
                    send(
                        side_out.at[pl.ds((near_d * 4 + k) * lay.side, lay.side)],
                        side_in.at[k, near_d], 1, near_d, k, targets[near_d][k],
                    )

    for f in range(fields):
        for corner in range(4):
            x = 0 if corner // 2 else edge - 1
            y = 0 if corner % 2 else edge - 1
            start = f * lay.field + x * edge + y
            corner_lines[7 - f, corner:corner + 1, :] = upd[start:start + 1, :]
    by_region = transposed_groups([corner_lines[f] for f in range(8)], edge)
    for k in range(4):
        region = corner_region[k]
        total = by_region[0]
        for g in range(1, 8):
            total = jnp.where(region == float(g), by_region[g], total)
        for corner in range(4):
            corner_out[corner * 4 + k] = total[corner:corner + 1, :]
    for corner in range(4):
        for k in order:
            send(
                corner_out.at[corner * 4 + k], corner_in.at[k * 4 + corner],
                2, 4 + corner, k, targets[4 + corner][k],
            )

    for sem, ref in enumerate((z_in, side_in, corner_in)):
        pltpu.make_async_copy(ref, ref, r3.at[sem]).wait()
    for s in range(slots):
        k = owner[s] + 2 - jnp.where(owner[s] > 0, 1, 0)
        for d in range(4):
            window[s, d * lay.side:(d + 1) * lay.side, :] = side_in[k, d]
        window[s, lay.z:lay.z + lay.z_size, :] = z_in[k]
        for corner in range(4):
            window[s, lay.corner + corner:lay.corner + corner + 1, :] = corner_in[k * 4 + corner]

    pltpu.make_async_copy(updated, updated, put.at[0]).wait()
    pltpu.make_async_copy(send1, send1, s1.at[0]).wait()
    told = near_in.at[pl.ds(0, len(offsets))]
    pltpu.make_async_copy(told, told, sh.at[0]).wait()
    for sem in (1, 2):
        if steady[sem]:
            clear[sem] = min(counts[sem - 1])
    for sem, (ref, size) in enumerate(((z_out, lay.z_size), (side_out, lay.side), (corner_out, 1))):
        if clear[sem]:
            rows = ref.at[pl.ds(0, clear[sem] * size)]
            pltpu.make_async_copy(rows, rows, s3.at[sem]).wait()
    for remote, itself in unclear:
        pl.when(jnp.logical_not(itself))(remote.wait_send)


def ghost_kernel(
    slots, fields, edge, mask_far, updated_in, window, updated_out, ghost_out,
    mask, passing, ghost, table, lhs, mask_sem, pass_sem, out_sem,
):
    lay = Layout(fields, edge)
    into = pltpu.make_async_copy(updated_in, passing, pass_sem.at[0])
    out = pltpu.make_async_copy(passing, updated_out, pass_sem.at[1])
    mask_load = pltpu.make_async_copy(mask_far, mask, mask_sem.at[0])
    mask_load.start()
    into.start()

    table[...] = jnp.zeros_like(table)
    cell_row = iota((edge, LANES), 0)
    col = iota((edge, LANES), 1)
    quarter = 2 * edge
    for kind in range(3):
        target = (col % 64) // 4 if kind == 2 else (col % quarter) // 2
        along = (col // quarter) % 2 if kind == 0 else col // 64
        within = (col // 2) % 2 if kind == 2 else col % 2
        step = cell_row - target
        alike = step == 0

        def signed(sign, where):
            return jnp.where(where, jnp.where(sign == 1, 0.125, -0.125), 0.0)

        centre = jnp.where(alike, 1.0, signed(within, step == 1) - signed(within, step == -1))
        ends = signed(within, step == 1 - edge) - signed(within, step == edge - 1)
        slope = signed(along, alike)
        for odd in range(2):
            for line in range(2):
                block = 2 * odd + line
                for column in range(2):
                    if kind == 0:
                        normal = jnp.where(alike, 0.125 if column else -0.125, 0.0)
                        used = col // 64 == line
                    else:
                        normal = signed(col % 2 if kind == 2 else (col // quarter) % 2, alike)
                        used = None if column == line else False
                    if used is False:
                        continue
                    for part, value in enumerate((centre, slope, normal, ends)):
                        if used is not None:
                            value = jnp.where(used, value, 0.0)
                        row = (part % 2) * LANES + (odd * 4 + (part // 2) * 2 + line) * edge
                        to = (2 * odd + column) * LANES
                        table[kind, row:row + edge, to:to + LANES] = value.astype(BF16)

    lane = iota((SUB, LANES), 1)
    in_group = lane % edge
    last_lane, first_lane = lane >= LANES - edge, lane < edge

    def gather(s):
        def rows(start, size=SUB):
            return window[s, start:start + size, :]

        def spread(start, shift, stride):
            row = jnp.broadcast_to(rows(start, 1), (SUB, LANES))
            return pltpu.roll(row, shift % LANES, 1, stride=stride, stride_axis=0)

        for kind in range(3):
            parts = [[] for _ in range(8)]
            for side in range(2):
                face = 2 * kind + side
                base = face * lay.side if kind < 2 else lay.z + side * 4 * fields
                layers = [rows(base + h * fields) for h in range(4)]
                centre, far = layers[:2], layers[2:]
                own = [rows(lay.own + (2 * face + h) * fields) for h in range(2)]
                if kind == 0:
                    lines = [lay.corner + 2 * side, lay.corner + 2 * side + 1]
                elif kind == 1:
                    lines = [lay.corner + side, lay.corner + 2 + side]
                else:
                    lines = [d * lay.side + lay.ends + 2 + side for d in range(2)]
                below = spread(lines[0], edge, edge)
                above = spread(lines[1], 0, edge)
                up = [pltpu.roll(v, LANES - edge, 1) for v in centre]
                down = [pltpu.roll(v, edge, 1) for v in centre]
                along = [
                    jnp.where(last_lane, up[1], up[0]) - jnp.where(first_lane, below, down[0]),
                    jnp.where(last_lane, above, up[1]) - jnp.where(first_lane, down[0], down[1]),
                ]
                for h in range(2):
                    if kind < 2:
                        before = after = spread(base + lay.ends + h, 0, 2)
                    else:
                        low_row, high_row = 2 * lay.side + lay.ends + h, 3 * lay.side + lay.ends + h
                        before = spread(low_row, edge - 1 if side else 0, 2)
                        after = spread(high_row, 0 if side else 1 - edge, 2)
                    end = jnp.where(in_group == edge - 1, before, jnp.where(in_group == 0, after, 0.0))
                    normal = own[h] - far[h] if side == 0 else far[h] - own[h]
                    for part, values in enumerate((centre[h], along[h], normal, end)):
                        parts[h * 4 + part].append(values)
            groups = transposed_groups([jnp.concatenate(v, axis=0) for v in parts], edge, (4, 2))
            for pair in range(4):
                high, low = split(jnp.concatenate(groups[2 * pair:2 * pair + 2], axis=1))
                lhs[s * 3 + kind, pair * 16:(pair + 1) * 16, :] = high
                lhs[s * 3 + kind, 64 + pair * 16:64 + (pair + 1) * 16, :] = low

    def finish(s):
        live = window[s, lay.keep:lay.keep + 1, :]
        for kind in range(3):
            both_parts = jnp.dot(lhs[s * 3 + kind], table[kind], preferred_element_type=F32)
            spreads = both_parts[:64] + both_parts[64:]
            for side in range(2):
                face = 2 * kind + side
                keep = live * jnp.where(mask[s, face] > 0, 1.0, 0.0).astype(F32)
                for pair in range(4):
                    for block in range(4):
                        start = pair * 16 + side * SUB
                        value = spreads[start:start + SUB, block * LANES:(block + 1) * LANES] * keep
                        h, column = block // 2, block % 2
                        tile = column * 8 + h * 4 + pair if kind == 0 else h * 8 + pair * 2 + column
                        ghost[s, :, face, tile * LANES:(tile + 1) * LANES] = value[:fields]

    def send(s):
        for f in range(fields):
            pltpu.make_async_copy(
                ghost.at[s, f, :, pl.ds(0, ghost_out.shape[3])], ghost_out.at[s, f], out_sem.at[0]
            ).start()

    gather(0)
    mask_load.wait()
    for s in range(slots):
        if s + 1 < slots:
            gather(s + 1)
        finish(s)
        send(s)
        if s == 0:
            into.wait()
            out.start()
    out.wait()
    pltpu.make_async_copy(ghost_out, ghost_out, out_sem.at[0]).wait()


def body(n_box, n_lev, fine, coarse, owner_map, patch_count, face_mask):
    slots, fields, fine_edge, _ = fine.shape
    edge = fine_edge // 2
    block = fields * edge
    lay = Layout(fields, edge)
    offsets, reach, same, counts = relations(n_box, n_lev)
    far = pl.BlockSpec(memory_space=pl.ANY)
    vmem = pl.BlockSpec(memory_space=pltpu.VMEM)
    flat = jax.ShapeDtypeStruct((block * edge, LANES), F32)
    places = (2 * reach + 1) * n_lev
    unsteady = 1 if max(len(v) for v in counts) == 1 else sum(len(v) > 1 for v in same.values())
    owner_rows = owner_map.T
    updated, window = pl.pallas_call(
        functools.partial(kernel, n_box, n_lev, slots, fields, edge),
        out_shape=(
            flat,
            jax.ShapeDtypeStruct((slots, lay.rows, LANES), F32),
        ),
        in_specs=[far] * 4,
        out_specs=(far, vmem),
        scratch_shapes=[
            pltpu.SMEM(owner_rows.shape, jnp.int32),
            pltpu.SMEM(patch_count.shape, jnp.int32),
            pltpu.VMEM((8 * slots * fields * fine_edge, LANES), F32),
            pltpu.VMEM((block * edge, LANES), F32),
            pltpu.VMEM((2 * slots * block, LANES), F32),
            pltpu.VMEM((4 * slots * block, LANES), F32),
            pltpu.VMEM((4, block, 2 * LANES), F32),
            pltpu.VMEM((4, block, 2 * LANES), F32),
            pltpu.VMEM((4, 1, LANES), F32),
            pltpu.VMEM((places, 4, 1, LANES), F32),
            pltpu.VMEM((SUB * lay.field, LANES), F32),
            pltpu.VMEM((2, 2, 2 * LANES, 4 * LANES), BF16),
            pltpu.VMEM((SUB, SUB, LANES), F32),
            pltpu.VMEM((4, SUB, LANES), F32),
            pltpu.VMEM((16 * lay.side, LANES), F32),
            pltpu.VMEM((4, 4, lay.side, LANES), F32),
            pltpu.VMEM((4 * lay.z_size, LANES), F32),
            pltpu.VMEM((4, lay.z_size, LANES), F32),
            pltpu.VMEM((16, 1, LANES), F32),
            pltpu.VMEM((16, 1, LANES), F32),
            pltpu.VMEM((4, 2 * LANES, 2 * LANES), BF16),
            pltpu.SemaphoreType.DMA((3,)),
            pltpu.SemaphoreType.DMA((2,)),
            pltpu.SemaphoreType.DMA((1,)),
            pltpu.SemaphoreType.DMA((1,)),
            pltpu.SemaphoreType.DMA((2,)),
            pltpu.SemaphoreType.DMA((1,)),
            pltpu.SemaphoreType.DMA((1,)),
            pltpu.SemaphoreType.DMA((3,)),
            pltpu.SemaphoreType.DMA((3,)),
            pltpu.SemaphoreType.DMA((unsteady,)),
        ],
        compiler_params=pltpu.CompilerParams(
            collective_id=0, has_side_effects=True, vmem_limit_bytes=VMEM_FIRST
        ),
    )(
        owner_rows, patch_count,
        fine.reshape(slots * fields * fine_edge, fine_edge * fine_edge),
        coarse.reshape(block * edge, LANES),
    )
    ghost_shape = (slots, fields, 6, 2 * fine_edge * fine_edge)
    updated, ghost = pl.pallas_call(
        functools.partial(ghost_kernel, slots, fields, edge),
        out_shape=(flat, jax.ShapeDtypeStruct(ghost_shape, F32)),
        in_specs=[far, far, vmem],
        out_specs=(far, far),
        scratch_shapes=[
            pltpu.SMEM(face_mask.shape, jnp.int32),
            pltpu.VMEM((block * edge, LANES), F32),
            pltpu.VMEM((*ghost_shape[:3], ghost_shape[3] + LANES), F32),
            pltpu.VMEM((3, 2 * LANES, 4 * LANES), BF16),
            pltpu.VMEM((3 * slots, LANES, 2 * LANES), BF16),
            pltpu.SemaphoreType.DMA((1,)),
            pltpu.SemaphoreType.DMA((2,)),
            pltpu.SemaphoreType.DMA((1,)),
        ],
        compiler_params=pltpu.CompilerParams(vmem_limit_bytes=VMEM_SECOND),
    )(face_mask, updated, window)
    return updated.reshape(coarse.shape), ghost.transpose(0, 2, 1, 3)


def solution(mesh):
    return jax.shard_map(
        functools.partial(body, mesh.shape["box"], mesh.shape["lev"]),
        mesh=mesh,
        in_specs=(
            P(("box", "lev"), None, None, None),
            P(None, "box", "lev", None),
            P(("box", "lev"), None),
            P(("box", "lev")),
            P(("box", "lev"), None),
        ),
        out_specs=(P(None, "box", "lev", None), P(("box", "lev"), None, None, None)),
        check_vma=False,
    )
```
